16 devices in a mesh: pp: 2 (over z), ep: 8 (over y, x, core).
Axes of the slice: x: 2, y: 2, z: 2, core: 2. Of those that a mesh axis runs over, the one named last changes fastest.
Arguments:
- x_fwd: bfloat16 [2, 8192, 512], P('pp', 'ep')
- ids_fwd: int32 [2, 8192, 8], P('pp', 'ep')
- slots_fwd: int32 [2, 8192, 8], P('pp', 'ep')
- gates_fwd: bfloat16 [2, 8192, 8], P('pp', 'ep')
- x_saved: bfloat16 [2, 8192, 512], P('pp', 'ep')
- grad_in: bfloat16 [2, 8192, 512], P('pp', 'ep')
- ids_bwd: int32 [2, 8192, 8], P('pp', 'ep')
- slots_bwd: int32 [2, 8192, 8], P('pp', 'ep')
- gates_bwd: bfloat16 [2, 8192, 8], P('pp', 'ep')
- w_one: bfloat16 [2, 512, 1536], P('pp')
- w_two: bfloat16 [2, 1536, 512], P('pp')
- w_gate: bfloat16 [2, 128, 512, 384], P('pp', 'ep')
- w_up: bfloat16 [2, 128, 512, 384], P('pp', 'ep')
- w_down: bfloat16 [2, 128, 384, 512], P('pp', 'ep')
Outputs:
- output 1: bfloat16 [2, 8192, 512], P('pp', 'ep')
- output 2: bfloat16 [2, 8192, 512], P('pp', 'ep')
- output 3: float32 [2, 128, 512, 384], P('pp', 'ep')
- output 4: float32 [2, 128, 512, 384], P('pp', 'ep')
- output 5: float32 [2, 128, 384, 512], P('pp', 'ep')
All inputs are finite; a program needn't handle non-finite values.
Results may differ from the reference program's by a relative error of at most 0.0104412.
Values are sent between devices in bfloat16 or wider.
A program may use at most 1 GiB of HBM per device.

```python
import jax
import jax.numpy as jnp
from jax import lax

STAGES = 2
EP_SIZE = 8
TOKENS_DEV = 1024
HIDDEN = 512
FF_DENSE = 1536
FF_EXPERT = 384
EXPERTS = 128
TOP = 8

NORM_EPS = 1e-6
CAP_ROWS = 8 * ((2 * TOKENS_DEV * TOP + 8 * EXPERTS - 1) // (8 * EXPERTS))
TOKENS = EP_SIZE * TOKENS_DEV
BUF_ROWS = EXPERTS * EP_SIZE * CAP_ROWS


def route_ranks(row_ids):
    sort_order = jnp.argsort(row_ids, stable=True)
    sorted_ids = row_ids[sort_order]
    group_start = jnp.searchsorted(sorted_ids, sorted_ids, side="left")
    rank_sorted = (jnp.arange(row_ids.shape[0]) - group_start).astype(jnp.int32)
    return jnp.zeros(row_ids.shape, jnp.int32).at[sort_order].set(rank_sorted)


def draw_routes(route_key):
    key_base, key_mult, key_hot, key_step = jax.random.split(route_key, 4)
    block_shape = (STAGES, EP_SIZE, TOKENS_DEV)
    base_ids = jax.random.randint(key_base, block_shape, 0, EXPERTS, dtype=jnp.int32)
    base_ids = base_ids * jax.random.randint(key_mult, block_shape, 1, 4, dtype=jnp.int32) // 3
    hot_ids = jax.random.randint(key_hot, (STAGES, EP_SIZE, 1), 0, EXPERTS, dtype=jnp.int32)
    base_ids = jnp.where(jnp.arange(TOKENS_DEV) % 2 == 0, hot_ids, base_ids)
    step_ids = jax.random.randint(key_step, (STAGES, EP_SIZE, TOKENS_DEV, TOP), 1, EXPERTS // TOP + 1, dtype=jnp.int32)
    step_ids = jnp.where(jnp.arange(TOP) == 0, 0, step_ids)
    expert_ids = ((base_ids[..., None] + jnp.cumsum(step_ids, axis=-1)) % EXPERTS).astype(jnp.int32)
    route_rank = jax.vmap(route_ranks)(expert_ids.reshape(STAGES * EP_SIZE, TOKENS_DEV * TOP))
    slot_ids = jnp.where(route_rank < CAP_ROWS, route_rank, -1).astype(jnp.int32)
    return expert_ids.reshape(STAGES, TOKENS, TOP), slot_ids.reshape(STAGES, TOKENS, TOP)


def setup_inputs(seed: int = 0) -> dict:
    key_list = jax.random.split(jax.random.key(seed), 14)
    tok_shape = (STAGES, TOKENS, HIDDEN)
    gate_shape = (STAGES, TOKENS, TOP)
    ids_fwd, slots_fwd = draw_routes(key_list[0])
    ids_bwd, slots_bwd = draw_routes(key_list[1])
    return {
        "x_fwd": jax.random.normal(key_list[2], tok_shape, jnp.float32).astype(jnp.bfloat16),
        "ids_fwd": ids_fwd,
        "slots_fwd": slots_fwd,
        "gates_fwd": (jax.random.uniform(key_list[3], gate_shape, jnp.float32, 0.5, 1.5) * TOP ** -0.5).astype(jnp.bfloat16),
        "x_saved": jax.random.normal(key_list[4], tok_shape, jnp.float32).astype(jnp.bfloat16),
        "grad_in": jax.random.normal(key_list[5], tok_shape, jnp.float32).astype(jnp.bfloat16),
        "ids_bwd": ids_bwd,
        "slots_bwd": slots_bwd,
        "gates_bwd": (jax.random.uniform(key_list[6], gate_shape, jnp.float32, 0.5, 1.5) * TOP ** -0.5).astype(jnp.bfloat16),
        "w_one": (jax.random.normal(key_list[7], (STAGES, HIDDEN, FF_DENSE), jnp.float32) * HIDDEN ** -0.5).astype(jnp.bfloat16),
        "w_two": (jax.random.normal(key_list[8], (STAGES, FF_DENSE, HIDDEN), jnp.float32) * FF_DENSE ** -0.5).astype(jnp.bfloat16),
        "w_gate": (jax.random.normal(key_list[9], (STAGES, EXPERTS, HIDDEN, FF_EXPERT), jnp.float32) * HIDDEN ** -0.5).astype(jnp.bfloat16),
        "w_up": (jax.random.normal(key_list[10], (STAGES, EXPERTS, HIDDEN, FF_EXPERT), jnp.float32) * HIDDEN ** -0.5).astype(jnp.bfloat16),
        "w_down": (jax.random.normal(key_list[11], (STAGES, EXPERTS, FF_EXPERT, HIDDEN), jnp.float32) * FF_EXPERT ** -0.5).astype(jnp.bfloat16),
    }


def rms_norm(values):
    return values * lax.rsqrt(jnp.mean(values * values, axis=-1, keepdims=True) + NORM_EPS)


def silu_grad(values):
    sigmoid_vals = jax.nn.sigmoid(values)
    return sigmoid_vals * (1.0 + values * (1.0 - sigmoid_vals))


def dense_forward(x_rows, w_one, w_two):
    normed = rms_norm(x_rows.astype(jnp.float32)).astype(jnp.bfloat16)
    hidden_pre = jnp.dot(normed, w_one, preferred_element_type=jnp.float32)
    dense_act = jax.nn.silu(hidden_pre).astype(jnp.bfloat16)
    dense_out = jnp.dot(dense_act, w_two, preferred_element_type=jnp.float32)
    return (x_rows.astype(jnp.float32) + dense_out).astype(jnp.bfloat16), hidden_pre


def dense_backward(x_rows, hidden_pre, w_one, w_two, grad_h):
    _, norm_vjp = jax.vjp(rms_norm, x_rows.astype(jnp.float32))
    grad_act = jnp.dot(grad_h.astype(jnp.bfloat16), w_two.T, preferred_element_type=jnp.float32)
    grad_pre = (grad_act * silu_grad(hidden_pre)).astype(jnp.bfloat16)
    grad_norm = jnp.dot(grad_pre, w_one.T, preferred_element_type=jnp.float32)
    return grad_h + norm_vjp(grad_norm)[0]


def route_maps(expert_ids, slot_ids):
    source = (jnp.arange(TOKENS, dtype=jnp.int32) // TOKENS_DEV)[:, None]
    row_index = jnp.where(slot_ids >= 0, expert_ids * (EP_SIZE * CAP_ROWS) + source * CAP_ROWS + slot_ids, BUF_ROWS)
    token_ids = jnp.broadcast_to(jnp.arange(TOKENS, dtype=jnp.int32)[:, None], expert_ids.shape)
    token_of_row = jnp.full((BUF_ROWS,), TOKENS, jnp.int32).at[row_index.reshape(-1)].set(token_ids.reshape(-1), mode="drop")
    return row_index, token_of_row


def expert_pass(operands):
    rows_fwd, rows_bwd, grad_out, w_gate, w_up, w_down = operands
    pre_gate = jnp.dot(rows_fwd, w_gate, preferred_element_type=jnp.float32)
    pre_up = jnp.dot(rows_fwd, w_up, preferred_element_type=jnp.float32)
    act_fwd = (jax.nn.silu(pre_gate) * pre_up).astype(jnp.bfloat16)
    out_fwd = jnp.dot(act_fwd, w_down, preferred_element_type=jnp.float32).astype(jnp.bfloat16)
    gate_bwd = jnp.dot(rows_bwd, w_gate, preferred_element_type=jnp.float32)
    up_bwd = jnp.dot(rows_bwd, w_up, preferred_element_type=jnp.float32)
    silu_gate = jax.nn.silu(gate_bwd)
    act_bwd = (silu_gate * up_bwd).astype(jnp.bfloat16)
    dw_down = jnp.dot(act_bwd.T, grad_out, preferred_element_type=jnp.float32)
    grad_act = jnp.dot(grad_out, w_down.T, preferred_element_type=jnp.float32).astype(jnp.bfloat16).astype(jnp.float32)
    grad_gate = (grad_act * up_bwd * silu_grad(gate_bwd)).astype(jnp.bfloat16)
    grad_up = (grad_act * silu_gate).astype(jnp.bfloat16)
    dw_gate = jnp.dot(rows_bwd.T, grad_gate, preferred_element_type=jnp.float32)
    dw_up = jnp.dot(rows_bwd.T, grad_up, preferred_element_type=jnp.float32)
    grad_rows = (jnp.dot(grad_gate, w_gate.T, preferred_element_type=jnp.float32) + jnp.dot(grad_up, w_up.T, preferred_element_type=jnp.float32)).astype(jnp.bfloat16)
    return out_fwd, grad_rows, dw_gate, dw_up, dw_down


def stage_pass(operands):
    (x_fwd, ids_fwd, slots_fwd, gates_fwd, x_saved, grad_in, ids_bwd, slots_bwd, gates_bwd, w_one, w_two, w_gate, w_up, w_down) = operands
    h_fwd, _ = dense_forward(x_fwd, w_one, w_two)
    xn_fwd = rms_norm(h_fwd.astype(jnp.float32)).astype(jnp.bfloat16)
    row_fwd, tok_fwd = route_maps(ids_fwd, slots_fwd)
    rows_fwd = jnp.take(xn_fwd, tok_fwd, axis=0, mode="fill", fill_value=0).reshape(EXPERTS, EP_SIZE * CAP_ROWS, HIDDEN)
    h_bwd, hidden_pre = dense_forward(x_saved, w_one, w_two)
    xn_bwd = rms_norm(h_bwd.astype(jnp.float32)).astype(jnp.bfloat16)
    row_bwd, tok_bwd = route_maps(ids_bwd, slots_bwd)
    rows_bwd = jnp.take(xn_bwd, tok_bwd, axis=0, mode="fill", fill_value=0).reshape(EXPERTS, EP_SIZE * CAP_ROWS, HIDDEN)
    gate_of_row = jnp.zeros((BUF_ROWS,), jnp.float32).at[row_bwd.reshape(-1)].set(gates_bwd.reshape(-1).astype(jnp.float32), mode="drop")
    grad_out = (jnp.take(grad_in, tok_bwd, axis=0, mode="fill", fill_value=0).astype(jnp.float32) * gate_of_row[:, None]).astype(jnp.bfloat16)
    grad_out = grad_out.reshape(EXPERTS, EP_SIZE * CAP_ROWS, HIDDEN)
    out_fwd, grad_rows, dw_gate, dw_up, dw_down = lax.map(expert_pass, (rows_fwd, rows_bwd, grad_out, w_gate, w_up, w_down))
    out_flat = out_fwd.reshape(BUF_ROWS, HIDDEN)
    grad_flat = grad_rows.reshape(BUF_ROWS, HIDDEN)
    mix_sum = jnp.zeros((TOKENS, HIDDEN), jnp.float32)
    grad_xn = jnp.zeros((TOKENS, HIDDEN), jnp.float32)
    for route_idx in range(TOP):
        routed = jnp.take(out_flat, row_fwd[:, route_idx], axis=0, mode="fill", fill_value=0).astype(jnp.float32)
        mix_sum = mix_sum + gates_fwd[:, route_idx].astype(jnp.float32)[:, None] * routed
        grad_xn = grad_xn + jnp.take(grad_flat, row_bwd[:, route_idx], axis=0, mode="fill", fill_value=0).astype(jnp.float32)
    y_out = (h_fwd.astype(jnp.float32) + mix_sum).astype(jnp.bfloat16)
    _, rms_vjp = jax.vjp(rms_norm, h_bwd.astype(jnp.float32))
    grad_h = grad_in.astype(jnp.float32) + rms_vjp(grad_xn)[0]
    grad_x = dense_backward(x_saved, hidden_pre, w_one, w_two, grad_h).astype(jnp.bfloat16)
    return y_out, grad_x, dw_gate, dw_up, dw_down


def reference(x_fwd, ids_fwd, slots_fwd, gates_fwd, x_saved, grad_in, ids_bwd, slots_bwd, gates_bwd, w_one, w_two, w_gate, w_up, w_down):
    y_out, dx_out, dw_gate, dw_up, dw_down = lax.map(stage_pass, (x_fwd, ids_fwd, slots_fwd, gates_fwd, x_saved, grad_in, ids_bwd, slots_bwd, gates_bwd, w_one, w_two, w_gate, w_up, w_down))
    return jnp.roll(y_out, 1, axis=0), jnp.roll(dx_out, -1, axis=0), dw_gate, dw_up, dw_down
```

```python
import functools

import jax
import jax.numpy as jnp
from jax import lax
from jax.experimental import pallas as pl
from jax.experimental.pallas import tpu as pltpu
from jax.sharding import PartitionSpec as P

NORM_EPS = 1e-6
CHUNK = 16
ROW_TILE = 256
VMEM_BYTES = 66_500_000
BF16 = jnp.bfloat16
F32 = jnp.float32


def rms_norm(values):
    return values * lax.rsqrt(jnp.mean(values * values, axis=-1, keepdims=True) + NORM_EPS)


def silu_grad(values):
    sigmoid_vals = jax.nn.sigmoid(values)
    return sigmoid_vals * (1.0 + values * (1.0 - sigmoid_vals))


def dense_forward(x_rows, w_one, w_two):
    normed = rms_norm(x_rows.astype(F32)).astype(BF16)
    hidden_pre = jnp.dot(normed, w_one, preferred_element_type=F32)
    dense_act = jax.nn.silu(hidden_pre).astype(BF16)
    dense_out = jnp.dot(dense_act, w_two, preferred_element_type=F32)
    return (x_rows.astype(F32) + dense_out).astype(BF16), hidden_pre


def dense_backward(x_rows, hidden_pre, w_one, w_two, grad_h):
    _, norm_vjp = jax.vjp(rms_norm, x_rows.astype(F32))
    grad_act = jnp.einsum("th,fh->tf", grad_h.astype(BF16), w_two, preferred_element_type=F32)
    grad_pre = (grad_act * silu_grad(hidden_pre)).astype(BF16)
    grad_norm = jnp.einsum("tf,hf->th", grad_pre, w_one, preferred_element_type=F32)
    return grad_h + norm_vjp(grad_norm)[0]


def dot_nn(lhs, rhs):
    return jnp.dot(lhs, rhs, preferred_element_type=F32)


def dot_nt(lhs, rhs):
    return lax.dot_general(lhs, rhs, (((1,), (1,)), ((), ())), preferred_element_type=F32)


def dot_tn(lhs, rhs):
    return lax.dot_general(lhs, rhs, (((0,), (0,)), ((), ())), preferred_element_type=F32)


def rows_at(index, count):
    return pl.ds(pl.multiple_of(index, CHUNK), count)


def fill_onehot(hot_ref, pos_ref, gate_ref, chunks_ref, src, n_local):
    tok_rows = pos_ref.shape[2]
    iota = lax.broadcasted_iota(jnp.int32, (CHUNK, tok_rows), 0)
    start = jnp.int32(0)
    for expert in range(n_local):
        pos_row = pos_ref[src, pl.ds(expert, 1), :]
        value = 1.0 if gate_ref is None else gate_ref[src, pl.ds(expert, 1), :]
        n_chunks = chunks_ref[src, expert]

        def body(c, carry, pos_row=pos_row, value=value, start=start):
            hot = jnp.where(iota + c * CHUNK == pos_row, value, 0.0)
            hot_ref[rows_at(start + c * CHUNK, CHUNK), :] = hot.astype(BF16)
            return carry

        lax.fori_loop(0, n_chunks, body, 0)
        start = start + n_chunks * CHUNK
    return start


def zero_tail(ref, offset, length, tile):
    n_tiles = (length + tile - 1) // tile

    def body(c, carry):
        ref[rows_at(offset + c * CHUNK, CHUNK), :] = jnp.zeros((CHUNK, ref.shape[1]), ref.dtype)
        return carry

    lax.fori_loop(length // CHUNK, n_tiles * (tile // CHUNK), body, 0)
    return n_tiles


def move_segments(pack_ref, wide_ref, base_ref, chunks_ref, src, n_local, cap, to_wide):
    start = jnp.int32(0)
    for expert in range(n_local):
        n_chunks = chunks_ref[src, expert]
        base = expert * cap + base_ref[src, expert]

        def body(c, carry, start=start, base=base):
            pack_rows = rows_at(start + c * CHUNK, CHUNK)
            wide_rows = rows_at(base + c * CHUNK, CHUNK)
            if to_wide:
                wide_ref[wide_rows, :] = pack_ref[pack_rows, :]
            else:
                pack_ref[pack_rows, :] = wide_ref[wide_rows, :]
            return carry

        lax.fori_loop(0, n_chunks, body, 0)
        start = start + n_chunks * CHUNK


def expert_bases(base_ref, total_ref, chunks_ref, n_src, n_local):
    for expert in range(n_local):
        total_ref[expert] = 0

    def body(src, carry):
        for expert in range(n_local):
            base_ref[src, expert] = total_ref[expert]
            total_ref[expert] = total_ref[expert] + chunks_ref[src, expert] * CHUNK
        return carry

    lax.fori_loop(0, n_src, body, 0)


def dispatch(pack_ref, hot_ref, table_ref, wide_ref, base_ref, chunks_ref, src, n_local, cap, length):
    def body(tile, carry):
        rows = rows_at(tile * ROW_TILE, ROW_TILE)
        pack_ref[rows, :] = dot_nn(hot_ref[rows, :], table_ref[...]).astype(BF16)
        return carry

    lax.fori_loop(0, (length + ROW_TILE - 1) // ROW_TILE, body, 0)
    move_segments(pack_ref, wide_ref, base_ref, chunks_ref, src, n_local, cap, True)


def combine(out_ref, pack_ref, hot_ref, wide_ref, base_ref, chunks_ref, src, n_local, cap, length, tile):
    move_segments(pack_ref, wide_ref, base_ref, chunks_ref, src, n_local, cap, False)
    n_tiles = zero_tail(pack_ref, 0, length, tile)
    zero_tail(hot_ref, 0, length, tile)
    out_ref[...] = jnp.zeros_like(out_ref)

    def body(step, carry):
        rows = rows_at(step * tile, tile)
        out_ref[...] += dot_tn(hot_ref[rows, :], pack_ref[rows, :])
        return carry

    lax.fori_loop(0, n_tiles, body, 0)


def weight_copies(expert, slot, wg_ref, wu_ref, wd_ref, gu_buf, dn_buf, sems):
    ff = wg_ref.shape[2]
    return (
        pltpu.make_async_copy(wg_ref.at[expert], gu_buf.at[slot, :, pl.ds(0, ff)], sems.at[slot, 0]),
        pltpu.make_async_copy(wu_ref.at[expert], gu_buf.at[slot, :, pl.ds(ff, ff)], sems.at[slot, 1]),
        pltpu.make_async_copy(wd_ref.at[expert], dn_buf.at[slot], sems.at[slot, 2]),
    )


def next_weights(expert, n_local, *refs):
    slot = lax.rem(expert, 2)

    @pl.when(expert + 1 < n_local)
    def _():
        for copy in weight_copies(expert + 1, lax.rem(expert + 1, 2), *refs):
            copy.start()

    for copy in weight_copies(expert, slot, *refs):
        copy.wait()
    return slot


def forward_kernel(n_src, n_local, cap, chunks_ref, tok_ref, pos_ref, gate_ref, wg_ref, wu_ref, wd_ref, out_ref,
                   wide, hot, pack, gu_buf, dn_buf, base, total, sems):
    step = pl.program_id(0)
    ff = wg_ref.shape[2]
    w_refs = (wg_ref, wu_ref, wd_ref, gu_buf, dn_buf, sems)

    @pl.when(step == 0)
    def _():
        for copy in weight_copies(0, 0, *w_refs):
            copy.start()
        expert_bases(base, total, chunks_ref, n_src, n_local)

    @pl.when(step < n_src)
    def _():
        length = fill_onehot(hot, pos_ref, None, chunks_ref, step, n_local)
        dispatch(pack, hot, tok_ref, wide, base, chunks_ref, step, n_local, cap, length)

    @pl.when((step >= n_src) & (step < n_src + n_local))
    def _():
        expert = step - n_src
        slot = next_weights(expert, n_local, *w_refs)

        def body(tile, carry):
            rows = rows_at(expert * cap + tile * ROW_TILE, ROW_TILE)
            pre = dot_nn(wide[rows, :], gu_buf[slot])
            gate = pre[:, :ff]
            act = (gate * jax.nn.sigmoid(gate) * pre[:, ff:]).astype(BF16)
            wide[rows, :] = dot_nn(act, dn_buf[slot]).astype(BF16)
            return carry

        lax.fori_loop(0, (total[expert] + ROW_TILE - 1) // ROW_TILE, body, 0)

    @pl.when(step >= n_src + n_local)
    def _():
        src = step - n_src - n_local
        length = fill_onehot(hot, pos_ref, gate_ref, chunks_ref, src, n_local)
        combine(out_ref, pack, hot, wide, base, chunks_ref, src, n_local, cap, length, 2 * ROW_TILE)


def backward_kernel(n_src, n_local, cap, chunks_ref, tok_ref, grad_ref, pos_ref, gate_ref, wg_ref, wu_ref, wd_ref,
                    out_ref, dwg_ref, dwu_ref, dwd_ref,
                    wide_x, wide_q, hot, pack, gu_buf, dn_buf, base, total, sems):
    step = pl.program_id(0)
    ff = wg_ref.shape[2]
    w_refs = (wg_ref, wu_ref, wd_ref, gu_buf, dn_buf, sems)

    @pl.when(step == 0)
    def _():
        for copy in weight_copies(0, 0, *w_refs):
            copy.start()
        expert_bases(base, total, chunks_ref, n_src, n_local)

    @pl.when(step < n_src)
    def _():
        length = fill_onehot(hot, pos_ref, None, chunks_ref, step, n_local)
        dispatch(pack, hot, tok_ref, wide_x, base, chunks_ref, step, n_local, cap, length)
        fill_onehot(hot, pos_ref, gate_ref, chunks_ref, step, n_local)
        dispatch(pack, hot, grad_ref, wide_q, base, chunks_ref, step, n_local, cap, length)

    @pl.when((step >= n_src) & (step < n_src + n_local))
    def _():
        expert = step - n_src
        slot = next_weights(expert, n_local, *w_refs)
        n_tiles = zero_tail(wide_x, expert * cap, total[expert], ROW_TILE)
        zero_tail(wide_q, expert * cap, total[expert], ROW_TILE)
        dwg_ref[...] = jnp.zeros_like(dwg_ref)
        dwu_ref[...] = jnp.zeros_like(dwu_ref)
        dwd_ref[...] = jnp.zeros_like(dwd_ref)

        def body(tile, carry):
            rows = rows_at(expert * cap + tile * ROW_TILE, ROW_TILE)
            x_rows = wide_x[rows, :]
            q_rows = wide_q[rows, :]
            pre = dot_nn(x_rows, gu_buf[slot])
            gate, up = pre[:, :ff], pre[:, ff:]
            sig = jax.nn.sigmoid(gate)
            silu = gate * sig
            act = (silu * up).astype(BF16)
            grad_act = dot_nt(q_rows, dn_buf[slot]).astype(BF16).astype(F32)
            grad_gate = (grad_act * up * (sig * (1.0 + gate * (1.0 - sig)))).astype(BF16)
            grad_up = (grad_act * silu).astype(BF16)
            grad_pre = jnp.concatenate([grad_gate, grad_up], axis=1)
            dwd_ref[0] += dot_tn(act, q_rows)
            dw_pre = dot_tn(x_rows, grad_pre)
            dwg_ref[0] += dw_pre[:, :ff]
            dwu_ref[0] += dw_pre[:, ff:]
            wide_x[rows, :] = dot_nt(grad_pre, gu_buf[slot]).astype(BF16)
            return carry

        lax.fori_loop(0, n_tiles, body, 0)

    @pl.when(step >= n_src + n_local)
    def _():
        src = step - n_src - n_local
        length = fill_onehot(hot, pos_ref, None, chunks_ref, src, n_local)
        combine(out_ref, pack, hot, wide_x, base, chunks_ref, src, n_local, cap, length, 2 * ROW_TILE)


def expert_call(backward, chunks, tables, pos, gate, w_gate, w_up, w_down):
    n_src, n_local, tok_rows = pos.shape
    hidden, ff = w_gate.shape[1:]
    cap = n_src * 128
    pack_rows = n_local * 128
    steps = 2 * n_src + n_local

    def src_in(i, *_):
        return (jnp.minimum(i, n_src - 1), 0)

    def src_out(i, *_):
        return (jnp.clip(i - n_src - n_local, 0, n_src - 1), 0)

    def weight_out(i, *_):
        return (jnp.clip(i - n_src, 0, n_local - 1), 0, 0)

    table_spec = pl.BlockSpec((tok_rows, hidden), src_in)
    whole = pl.BlockSpec(pos.shape, lambda i, *_: (0, 0, 0), pipeline_mode=pl.Buffered(1))
    raw = pl.BlockSpec(memory_space=pl.ANY)
    out_shape = [jax.ShapeDtypeStruct((n_src * tok_rows, hidden), F32)]
    out_specs = [pl.BlockSpec((tok_rows, hidden), src_out)]
    wide = pltpu.VMEM((n_local * cap, hidden), BF16)
    scratch = [wide]
    if backward:
        out_shape += [jax.ShapeDtypeStruct(w.shape, F32) for w in (w_gate, w_up, w_down)]
        out_specs += [pl.BlockSpec((1,) + w.shape[1:], weight_out) for w in (w_gate, w_up, w_down)]
        scratch += [wide]
    scratch += [
        pltpu.VMEM((pack_rows, tok_rows), BF16),
        pltpu.VMEM((pack_rows, hidden), BF16),
        pltpu.VMEM((2, hidden, 2 * ff), BF16),
        pltpu.VMEM((2, ff, hidden), BF16),
        pltpu.SMEM((n_src, n_local), jnp.int32),
        pltpu.SMEM((n_local,), jnp.int32),
        pltpu.SemaphoreType.DMA((2, 3)),
    ]
    body = backward_kernel if backward else forward_kernel
    flops = (100 if backward else 60) * 10 ** 9
    return pl.pallas_call(
        functools.partial(body, n_src, n_local, cap),
        grid_spec=pltpu.PrefetchScalarGridSpec(
            num_scalar_prefetch=1,
            grid=(steps,),
            in_specs=[table_spec] * len(tables) + [whole, whole, raw, raw, raw],
            out_specs=out_specs,
            scratch_shapes=scratch,
        ),
        out_shape=out_shape,
        compiler_params=pltpu.CompilerParams(dimension_semantics=("arbitrary",), vmem_limit_bytes=VMEM_BYTES),
        cost_estimate=pl.CostEstimate(flops=flops, bytes_accessed=60 * 10 ** 6, transcendentals=0),
        name="expert_backward" if backward else "expert_forward",
    )(chunks, *tables, pos, gate, w_gate, w_up, w_down)


def route_tables(ids, gates, first, n_local):
    tok_rows = ids.shape[2]
    experts = (first + jnp.arange(n_local)).astype(F32)
    match = ids[:, None] == experts[None, :, None, None]
    kept = jnp.any(match, axis=2)
    gate = jnp.sum(jnp.where(match, gates[:, None], 0.0), axis=2)
    upper = (jnp.arange(tok_rows)[:, None] <= jnp.arange(tok_rows)[None, :]).astype(BF16)
    rank = jnp.einsum("set,tu->seu", kept.astype(BF16), upper, preferred_element_type=F32)
    pos = jnp.where(kept, rank - 1.0, -1.0).astype(jnp.int32)
    chunks = (rank[:, :, -1].astype(jnp.int32) + CHUNK - 1) // CHUNK
    return pos, gate, chunks


def solution(mesh):
    stages = mesh.shape["pp"]
    ep_size = mesh.shape["ep"]
    next_perm = [(stage_idx, (stage_idx + 1) % stages) for stage_idx in range(stages)]
    prev_perm = [(stage_idx, (stage_idx - 1) % stages) for stage_idx in range(stages)]
    tok_spec = P("pp", "ep", None)
    dense_spec = P("pp", None, None)
    expert_spec = P("pp", "ep", None, None)

    def device_step(x_fwd, ids_fwd, slots_fwd, gates_fwd, x_saved, grad_in, ids_bwd, slots_bwd, gates_bwd, w_one, w_two, w_gate, w_up, w_down):
        x_fwd, ids_fwd, slots_fwd, gates_fwd = x_fwd[0], ids_fwd[0], slots_fwd[0], gates_fwd[0]
        x_saved, grad_in, ids_bwd, slots_bwd, gates_bwd = x_saved[0], grad_in[0], ids_bwd[0], slots_bwd[0], gates_bwd[0]
        w_one, w_two, w_gate, w_up, w_down = w_one[0], w_two[0], w_gate[0], w_up[0], w_down[0]
        top_k = ids_fwd.shape[1]
        n_local = w_gate.shape[0]
        first = lax.axis_index("ep") * n_local

        routes = jnp.concatenate([
            jnp.where(slots_fwd >= 0, ids_fwd, -1).astype(F32), gates_fwd.astype(F32),
            jnp.where(slots_bwd >= 0, ids_bwd, -1).astype(F32), gates_bwd.astype(F32),
        ], axis=1).T
        routes = lax.all_gather(routes, "ep", axis=0, tiled=False)
        id_f, gate_f, id_b, gate_b = (routes[:, i * top_k:(i + 1) * top_k] for i in range(4))
        pos_f, gate_f, chunks_f = route_tables(id_f, gate_f, first, n_local)
        pos_b, gate_b, chunks_b = route_tables(id_b, gate_b, first, n_local)

        h_fwd, _ = dense_forward(x_fwd, w_one, w_two)
        xn_fwd = rms_norm(h_fwd.astype(F32)).astype(BF16)
        all_fwd = lax.all_gather(xn_fwd, "ep", axis=0, tiled=True)
        all_grad = lax.all_gather(grad_in, "ep", axis=0, tiled=True)
        h_bwd, hidden_pre = dense_forward(x_saved, w_one, w_two)
        xn_bwd = rms_norm(h_bwd.astype(F32)).astype(BF16)
        all_bwd = lax.all_gather(xn_bwd, "ep", axis=0, tiled=True)

        (part_fwd,) = expert_call(False, chunks_f, (all_fwd,), pos_f, gate_f, w_gate, w_up, w_down)
        mix_sum = lax.psum_scatter(part_fwd, "ep", scatter_dimension=0, tiled=True)
        y_out = (h_fwd.astype(F32) + mix_sum).astype(BF16)

        part_bwd, dw_gate, dw_up, dw_down = expert_call(True, chunks_b, (all_bwd, all_grad), pos_b, gate_b, w_gate, w_up, w_down)
        grad_xn = lax.psum_scatter(part_bwd, "ep", scatter_dimension=0, tiled=True)
        _, rms_vjp = jax.vjp(rms_norm, h_bwd.astype(F32))
        grad_h = grad_in.astype(F32) + rms_vjp(grad_xn)[0]
        grad_x = dense_backward(x_saved, hidden_pre, w_one, w_two, grad_h).astype(BF16)

        y_next = lax.ppermute(y_out, "pp", next_perm)
        dx_prev = lax.ppermute(grad_x, "pp", prev_perm)
        return y_next[None], dx_prev[None], dw_gate[None], dw_up[None], dw_down[None]

    in_specs = (tok_spec,) * 9 + (dense_spec, dense_spec, expert_spec, expert_spec, expert_spec)
    out_specs = (tok_spec, tok_spec, expert_spec, expert_spec, expert_spec)
    return jax.shard_map(device_step, mesh=mesh, in_specs=in_specs, out_specs=out_specs, check_vma=False)
```

```python
import functools

import jax
import jax.numpy as jnp
from jax import lax
from jax.experimental import pallas as pl
from jax.experimental.pallas import tpu as pltpu
from jax.sharding import PartitionSpec as P

NORM_EPS = 1e-6
CHUNK = 16
BLOCK = 64
ROW_TILE = 512
BIG_TILE = 512
SMALL_TILE = 256
VMEM_BYTES = 66_500_000
BF16 = jnp.bfloat16
F32 = jnp.float32


def rms_norm(values):
    return values * lax.rsqrt(jnp.mean(values * values, axis=-1, keepdims=True) + NORM_EPS)


def silu_grad(values):
    sigmoid_vals = jax.nn.sigmoid(values)
    return sigmoid_vals * (1.0 + values * (1.0 - sigmoid_vals))


def dense_forward(x_rows, w_one, w_two):
    normed = rms_norm(x_rows.astype(F32)).astype(BF16)
    hidden_pre = jnp.dot(normed, w_one, preferred_element_type=F32)
    dense_act = jax.nn.silu(hidden_pre).astype(BF16)
    dense_out = jnp.dot(dense_act, w_two, preferred_element_type=F32)
    return (x_rows.astype(F32) + dense_out).astype(BF16), hidden_pre


def dense_backward(x_rows, hidden_pre, w_one, w_two, grad_h):
    _, norm_vjp = jax.vjp(rms_norm, x_rows.astype(F32))
    grad_act = jnp.einsum("th,fh->tf", grad_h.astype(BF16), w_two, preferred_element_type=F32)
    grad_pre = (grad_act * silu_grad(hidden_pre)).astype(BF16)
    grad_norm = jnp.einsum("tf,hf->th", grad_pre, w_one, preferred_element_type=F32)
    return grad_h + norm_vjp(grad_norm)[0]


def dot_nn(lhs, rhs):
    return jnp.dot(lhs, rhs, preferred_element_type=F32)


def dot_nt(lhs, rhs):
    return lax.dot_general(lhs, rhs, (((1,), (1,)), ((), ())), preferred_element_type=F32)


def dot_tn(lhs, rhs):
    return lax.dot_general(lhs, rhs, (((0,), (0,)), ((), ())), preferred_element_type=F32)


def rows_at(index, count):
    return pl.ds(pl.multiple_of(index, CHUNK), count)


def fill_onehot(hot_ref, pos_ref, gate_ref, chunks_ref, src, n_local):
    tok_rows = pos_ref.shape[3]
    iota = lax.broadcasted_iota(jnp.int32, (CHUNK, tok_rows), 0).astype(F32).astype(BF16)

    def body(expert, start):
        n_chunks = chunks_ref[src, expert]

        def block(first):
            pos_rows = pos_ref[0, expert]
            value = jnp.ones((CHUNK, tok_rows), BF16) if gate_ref is None else gate_ref[0, expert]
            for c in range(first, first + BLOCK // CHUNK):
                hot = jnp.where(iota + jnp.bfloat16(c * CHUNK) == pos_rows, value, jnp.zeros_like(value))
                hot_ref[rows_at(start + c * CHUNK, CHUNK), :] = hot

        block(0)
        pl.when(n_chunks > BLOCK // CHUNK)(functools.partial(block, BLOCK // CHUNK))
        return start + n_chunks * CHUNK

    return lax.fori_loop(0, n_local, body, jnp.int32(0))


def zero_tail(ref, offset, length, tile):
    n_tiles = (length + tile - 1) // tile

    def body(c, carry):
        ref[rows_at(offset + c * CHUNK, CHUNK), :] = jnp.zeros((CHUNK, ref.shape[1]), ref.dtype)
        return carry

    lax.fori_loop(length // CHUNK, n_tiles * (tile // CHUNK), body, 0)
    return n_tiles


def move_segments(pack_ref, wide_ref, base_ref, chunks_ref, src, n_local, cap, to_wide):
    def body(expert, start):
        n_chunks = chunks_ref[src, expert]
        base = expert * cap + base_ref[src, expert]

        def block(first):
            pack_rows = rows_at(start + first, BLOCK)
            wide_rows = rows_at(base + first, BLOCK)
            if to_wide:
                wide_ref[wide_rows, :] = pack_ref[pack_rows, :]
            else:
                pack_ref[pack_rows, :] = wide_ref[wide_rows, :]

        block(0)
        pl.when(n_chunks > BLOCK // CHUNK)(functools.partial(block, BLOCK))
        return start + n_chunks * CHUNK

    lax.fori_loop(0, n_local, body, jnp.int32(0))


def expert_bases(base_ref, total_ref, chunks_ref, n_src, n_local):
    for expert in range(n_local):
        total_ref[expert] = 0

    def body(src, carry):
        for expert in range(n_local):
            base_ref[src, expert] = total_ref[expert]
            total_ref[expert] = total_ref[expert] + chunks_ref[src, expert] * CHUNK
        return carry

    lax.fori_loop(0, n_src, body, 0)


def dispatch(pack_ref, hot_ref, table_ref, wide_ref, base_ref, chunks_ref, src, n_local, cap, length):
    def body(tile, carry):
        rows = rows_at(tile * ROW_TILE, ROW_TILE)
        pack_ref[rows, :] = dot_nn(hot_ref[rows, :], table_ref[...]).astype(BF16)
        return carry

    lax.fori_loop(0, (length + ROW_TILE - 1) // ROW_TILE, body, 0)
    move_segments(pack_ref, wide_ref, base_ref, chunks_ref, src, n_local, cap, True)


def combine(out_ref, pack_ref, hot_ref, wide_ref, base_ref, chunks_ref, src, n_local, cap, length, tile):
    move_segments(pack_ref, wide_ref, base_ref, chunks_ref, src, n_local, cap, False)
    n_tiles = zero_tail(pack_ref, 0, length, tile)
    zero_tail(hot_ref, 0, length, tile)
    out_ref[...] = jnp.zeros_like(out_ref)

    def body(step, carry):
        rows = rows_at(step * tile, tile)
        out_ref[...] += dot_tn(hot_ref[rows, :], pack_ref[rows, :])
        return carry

    lax.fori_loop(0, n_tiles, body, 0)


def tiled_rows(first, count, step):
    n_small = (count + SMALL_TILE - 1) // SMALL_TILE
    per_big = BIG_TILE // SMALL_TILE
    n_big = n_small // per_big

    def big(tile, carry):
        step(rows_at(first + tile * BIG_TILE, BIG_TILE))
        return carry

    def small(tile, carry):
        step(rows_at(first + n_big * BIG_TILE + tile * SMALL_TILE, SMALL_TILE))
        return carry

    lax.fori_loop(0, n_big, big, 0)
    if per_big > 1:
        lax.fori_loop(0, n_small - n_big * per_big, small, 0)


def weight_copies(expert, slot, wg_ref, wu_ref, wd_ref, gu_buf, dn_buf, sems):
    ff = wg_ref.shape[2]
    return (
        pltpu.make_async_copy(wg_ref.at[expert], gu_buf.at[slot, :, pl.ds(0, ff)], sems.at[slot, 0]),
        pltpu.make_async_copy(wu_ref.at[expert], gu_buf.at[slot, :, pl.ds(ff, ff)], sems.at[slot, 1]),
        pltpu.make_async_copy(wd_ref.at[expert], dn_buf.at[slot], sems.at[slot, 2]),
    )


def next_weights(expert, n_local, *refs):
    slot = lax.rem(expert, 2)

    @pl.when(expert + 1 < n_local)
    def _():
        for copy in weight_copies(expert + 1, lax.rem(expert + 1, 2), *refs):
            copy.start()

    for copy in weight_copies(expert, slot, *refs):
        copy.wait()
    return slot


def forward_kernel(n_src, n_local, cap, chunks_ref, tok_ref, pos_ref, gate_ref, wg_ref, wu_ref, wd_ref, out_ref,
                   wide, hot, pack, gu_buf, dn_buf, base, total, sems):
    step = pl.program_id(0)
    ff = wg_ref.shape[2]
    w_refs = (wg_ref, wu_ref, wd_ref, gu_buf, dn_buf, sems)

    @pl.when(step == 0)
    def _():
        for copy in weight_copies(0, 0, *w_refs):
            copy.start()
        expert_bases(base, total, chunks_ref, n_src, n_local)

    @pl.when(step < n_src)
    def _():
        length = fill_onehot(hot, pos_ref, None, chunks_ref, step, n_local)
        dispatch(pack, hot, tok_ref, wide, base, chunks_ref, step, n_local, cap, length)

    @pl.when((step >= n_src) & (step < n_src + n_local))
    def _():
        expert = step - n_src
        slot = next_weights(expert, n_local, *w_refs)

        def rows_step(rows):
            pre = dot_nn(wide[rows, :], gu_buf[slot])
            gate = pre[:, :ff]
            act = (gate * jax.nn.sigmoid(gate) * pre[:, ff:]).astype(BF16)
            wide[rows, :] = dot_nn(act, dn_buf[slot]).astype(BF16)

        tiled_rows(expert * cap, total[expert], rows_step)

    @pl.when(step >= n_src + n_local)
    def _():
        src = step - n_src - n_local
        length = fill_onehot(hot, pos_ref, gate_ref, chunks_ref, src, n_local)
        combine(out_ref, pack, hot, wide, base, chunks_ref, src, n_local, cap, length, ROW_TILE)


def backward_kernel(n_src, n_local, cap, chunks_ref, tok_ref, grad_ref, pos_ref, gate_ref, wg_ref, wu_ref, wd_ref,
                    out_ref, dwg_ref, dwu_ref, dwd_ref,
                    wide_x, wide_q, hot, pack, gu_buf, dn_buf, base, total, sems):
    step = pl.program_id(0)
    ff = wg_ref.shape[2]
    w_refs = (wg_ref, wu_ref, wd_ref, gu_buf, dn_buf, sems)

    @pl.when(step == 0)
    def _():
        for copy in weight_copies(0, 0, *w_refs):
            copy.start()
        expert_bases(base, total, chunks_ref, n_src, n_local)

    @pl.when(step < n_src)
    def _():
        length = fill_onehot(hot, pos_ref, None, chunks_ref, step, n_local)
        dispatch(pack, hot, tok_ref, wide_x, base, chunks_ref, step, n_local, cap, length)
        fill_onehot(hot, pos_ref, gate_ref, chunks_ref, step, n_local)
        dispatch(pack, hot, grad_ref, wide_q, base, chunks_ref, step, n_local, cap, length)

    @pl.when((step >= n_src) & (step < n_src + n_local))
    def _():
        expert = step - n_src
        slot = next_weights(expert, n_local, *w_refs)
        zero_tail(wide_x, expert * cap, total[expert], SMALL_TILE)
        zero_tail(wide_q, expert * cap, total[expert], SMALL_TILE)
        dwg_ref[...] = jnp.zeros_like(dwg_ref)
        dwu_ref[...] = jnp.zeros_like(dwu_ref)
        dwd_ref[...] = jnp.zeros_like(dwd_ref)

        def rows_step(rows):
            x_rows = wide_x[rows, :]
            q_rows = wide_q[rows, :]
            pre = dot_nn(x_rows, gu_buf[slot])
            gate, up = pre[:, :ff], pre[:, ff:]
            sig = jax.nn.sigmoid(gate)
            silu = gate * sig
            act = (silu * up).astype(BF16)
            grad_act = dot_nt(q_rows, dn_buf[slot]).astype(BF16).astype(F32)
            grad_gate = (grad_act * up * (sig * (1.0 + gate * (1.0 - sig)))).astype(BF16)
            grad_up = (grad_act * silu).astype(BF16)
            grad_pre = jnp.concatenate([grad_gate, grad_up], axis=1)
            dwd_ref[0] += dot_tn(act, q_rows)
            dw_pre = dot_tn(x_rows, grad_pre)
            dwg_ref[0] += dw_pre[:, :ff]
            dwu_ref[0] += dw_pre[:, ff:]
            wide_x[rows, :] = dot_nt(grad_pre, gu_buf[slot]).astype(BF16)

        tiled_rows(expert * cap, total[expert], rows_step)

    @pl.when(step >= n_src + n_local)
    def _():
        src = step - n_src - n_local
        length = fill_onehot(hot, pos_ref, None, chunks_ref, src, n_local)
        combine(out_ref, pack, hot, wide_x, base, chunks_ref, src, n_local, cap, length, ROW_TILE)


def expert_call(backward, chunks, tables, pos, gate, w_gate, w_up, w_down):
    n_src, n_local, _, tok_rows = pos.shape
    hidden, ff = w_gate.shape[1:]
    cap = n_src * 128 + BLOCK
    pack_rows = n_local * 128 + BLOCK
    steps = 2 * n_src + n_local

    def src_in(i, *_):
        return (jnp.minimum(i, n_src - 1), 0)

    def src_out(i, *_):
        return (jnp.clip(i - n_src - n_local, 0, n_src - 1), 0)

    def weight_out(i, *_):
        return (jnp.clip(i - n_src, 0, n_local - 1), 0, 0)

    table_spec = pl.BlockSpec((tok_rows, hidden), src_in)

    def route_in(i, *_):
        return (jnp.where(i < n_src, i, jnp.clip(i - n_src - n_local, 0, n_src - 1)), 0, 0, 0)

    route_spec = pl.BlockSpec((1,) + pos.shape[1:], route_in)
    raw = pl.BlockSpec(memory_space=pl.ANY)
    out_shape = [jax.ShapeDtypeStruct((n_src * tok_rows, hidden), F32)]
    out_specs = [pl.BlockSpec((tok_rows, hidden), src_out)]
    wide = pltpu.VMEM((n_local * cap, hidden), BF16)
    scratch = [wide]
    if backward:
        out_shape += [jax.ShapeDtypeStruct(w.shape, F32) for w in (w_gate, w_up, w_down)]
        out_specs += [pl.BlockSpec((1,) + w.shape[1:], weight_out) for w in (w_gate, w_up, w_down)]
        scratch += [wide]
    scratch += [
        pltpu.VMEM((pack_rows, tok_rows), BF16),
        pltpu.VMEM((pack_rows, hidden), BF16),
        pltpu.VMEM((2, hidden, 2 * ff), BF16),
        pltpu.VMEM((2, ff, hidden), BF16),
        pltpu.SMEM((n_src, n_local), jnp.int32),
        pltpu.SMEM((n_local,), jnp.int32),
        pltpu.SemaphoreType.DMA((2, 3)),
    ]
    body = backward_kernel if backward else forward_kernel
    flops = (100 if backward else 60) * 10 ** 9
    return pl.pallas_call(
        functools.partial(body, n_src, n_local, cap),
        grid_spec=pltpu.PrefetchScalarGridSpec(
            num_scalar_prefetch=1,
            grid=(steps,),
            in_specs=[table_spec] * len(tables) + [route_spec, route_spec, raw, raw, raw],
            out_specs=out_specs,
            scratch_shapes=scratch,
        ),
        out_shape=out_shape,
        compiler_params=pltpu.CompilerParams(dimension_semantics=("arbitrary",), vmem_limit_bytes=VMEM_BYTES),
        cost_estimate=pl.CostEstimate(flops=flops, bytes_accessed=60 * 10 ** 6, transcendentals=0),
        name="expert_backward" if backward else "expert_forward",
    )(chunks, *tables, pos, gate, w_gate, w_up, w_down)


def route_tables(ids, gates, first, n_local):
    tok_rows = ids.shape[2]
    experts = (first + jnp.arange(n_local)).astype(F32)
    match = ids[:, None] == experts[None, :, None, None]
    kept = jnp.any(match, axis=2)
    gate = jnp.sum(jnp.where(match, gates[:, None], 0.0), axis=2)
    upper = (jnp.arange(tok_rows)[:, None] <= jnp.arange(tok_rows)[None, :]).astype(BF16)
    rank = jnp.einsum("set,tu->seu", kept.astype(BF16), upper, preferred_element_type=F32)
    pos = jnp.where(kept, rank - 1.0, -1.0).astype(BF16)
    chunks = (rank[:, :, -1].astype(jnp.int32) + CHUNK - 1) // CHUNK
    shape = pos.shape[:2] + (CHUNK, tok_rows)
    return jnp.broadcast_to(pos[:, :, None], shape), jnp.broadcast_to(gate.astype(BF16)[:, :, None], shape), chunks


def solution(mesh):
    stages = mesh.shape["pp"]
    ep_size = mesh.shape["ep"]
    next_perm = [(stage_idx, (stage_idx + 1) % stages) for stage_idx in range(stages)]
    prev_perm = [(stage_idx, (stage_idx - 1) % stages) for stage_idx in range(stages)]
    tok_spec = P("pp", "ep", None)
    dense_spec = P("pp", None, None)
    expert_spec = P("pp", "ep", None, None)

    def device_step(x_fwd, ids_fwd, slots_fwd, gates_fwd, x_saved, grad_in, ids_bwd, slots_bwd, gates_bwd, w_one, w_two, w_gate, w_up, w_down):
        x_fwd, ids_fwd, slots_fwd, gates_fwd = x_fwd[0], ids_fwd[0], slots_fwd[0], gates_fwd[0]
        x_saved, grad_in, ids_bwd, slots_bwd, gates_bwd = x_saved[0], grad_in[0], ids_bwd[0], slots_bwd[0], gates_bwd[0]
        w_one, w_two, w_gate, w_up, w_down = w_one[0], w_two[0], w_gate[0], w_up[0], w_down[0]
        top_k = ids_fwd.shape[1]
        n_local = w_gate.shape[0]
        first = lax.axis_index("ep") * n_local

        h_fwd, _ = dense_forward(x_fwd, w_one, w_two)
        xn_fwd = rms_norm(h_fwd.astype(F32)).astype(BF16)
        all_fwd = lax.all_gather(xn_fwd, "ep", axis=0, tiled=True)

        xn_fwd, x_saved, grad_in = lax.optimization_barrier((xn_fwd, x_saved, grad_in))
        all_grad = lax.all_gather(grad_in, "ep", axis=0, tiled=True)
        routes = jnp.concatenate([
            jnp.where(slots_fwd >= 0, ids_fwd, -1).astype(BF16), gates_fwd,
            jnp.where(slots_bwd >= 0, ids_bwd, -1).astype(BF16), gates_bwd,
        ], axis=1).T
        routes = lax.all_gather(routes, "ep", axis=0, tiled=False).astype(F32)
        id_f, gate_f, id_b, gate_b = (routes[:, i * top_k:(i + 1) * top_k] for i in range(4))
        pos_f, gate_f, chunks_f = route_tables(id_f, gate_f, first, n_local)
        pos_b, gate_b, chunks_b = route_tables(id_b, gate_b, first, n_local)
        h_bwd, hidden_pre = dense_forward(x_saved, w_one, w_two)
        xn_bwd = rms_norm(h_bwd.astype(F32)).astype(BF16)
        all_bwd = lax.all_gather(xn_bwd, "ep", axis=0, tiled=True)

        (part_fwd,) = expert_call(False, chunks_f, (all_fwd,), pos_f, gate_f, w_gate, w_up, w_down)
        mix_sum = lax.psum_scatter(part_fwd, "ep", scatter_dimension=0, tiled=True)
        y_out = (h_fwd.astype(F32) + mix_sum).astype(BF16)

        chunks_b, _ = lax.optimization_barrier((chunks_b, part_fwd))
        part_bwd, dw_gate, dw_up, dw_down = expert_call(True, chunks_b, (all_bwd, all_grad), pos_b, gate_b, w_gate, w_up, w_down)
        grad_xn = lax.psum_scatter(part_bwd, "ep", scatter_dimension=0, tiled=True)
        _, rms_vjp = jax.vjp(rms_norm, h_bwd.astype(F32))
        grad_h = grad_in.astype(F32) + rms_vjp(grad_xn)[0]
        grad_x = dense_backward(x_saved, hidden_pre, w_one, w_two, grad_h).astype(BF16)

        y_next = lax.ppermute(y_out, "pp", next_perm)
        dx_prev = lax.ppermute(grad_x, "pp", prev_perm)
        return y_next[None], dx_prev[None], dw_gate[None], dw_up[None], dw_down[None]

    in_specs = (tok_spec,) * 9 + (dense_spec, dense_spec, expert_spec, expert_spec, expert_spec)
    out_specs = (tok_spec, tok_spec, expert_spec, expert_spec, expert_spec)
    return jax.shard_map(device_step, mesh=mesh, in_specs=in_specs, out_specs=out_specs, check_vma=False)
```

```python
import functools

import jax
import jax.numpy as jnp
from jax import lax
from jax.experimental import pallas as pl
from jax.experimental.pallas import tpu as pltpu
from jax.sharding import PartitionSpec as P

NORM_EPS = 1e-6
CHUNK = 16
BLOCK = 64
ROW_TILE = 512
BIG_TILE = 512
SMALL_TILE = 256
VMEM_BYTES = 66_500_000
BF16 = jnp.bfloat16
F32 = jnp.float32


def rms_norm(values):
    return values * lax.rsqrt(jnp.mean(values * values, axis=-1, keepdims=True) + NORM_EPS)


def silu_grad(values):
    sigmoid_vals = jax.nn.sigmoid(values)
    return sigmoid_vals * (1.0 + values * (1.0 - sigmoid_vals))


def dense_forward(x_rows, w_one, w_two):
    normed = rms_norm(x_rows.astype(F32)).astype(BF16)
    hidden_pre = jnp.dot(normed, w_one, preferred_element_type=F32)
    dense_act = jax.nn.silu(hidden_pre).astype(BF16)
    dense_out = jnp.dot(dense_act, w_two, preferred_element_type=F32)
    return (x_rows.astype(F32) + dense_out).astype(BF16), hidden_pre


def dot_nn(lhs, rhs):
    return jnp.dot(lhs, rhs, preferred_element_type=F32)


def dot_nt(lhs, rhs):
    return lax.dot_general(lhs, rhs, (((1,), (1,)), ((), ())), preferred_element_type=F32)


def dot_tn(lhs, rhs):
    return lax.dot_general(lhs, rhs, (((0,), (0,)), ((), ())), preferred_element_type=F32)


def rows_at(index, count):
    return pl.ds(pl.multiple_of(index, CHUNK), count)


def fill_onehot(hot_ref, pos_ref, gate_ref, chunks_ref, src, n_local):
    tok_rows = pos_ref.shape[3]
    iota = lax.broadcasted_iota(jnp.int32, (CHUNK, tok_rows), 0).astype(F32).astype(BF16)

    def body(expert, start):
        n_chunks = chunks_ref[src, expert]

        def block(first):
            pos_rows = pos_ref[0, expert]
            value = jnp.ones((CHUNK, tok_rows), BF16) if gate_ref is None else gate_ref[0, expert]
            for c in range(first, first + BLOCK // CHUNK):
                hot = jnp.where(iota + jnp.bfloat16(c * CHUNK) == pos_rows, value, jnp.zeros_like(value))
                hot_ref[rows_at(start + c * CHUNK, CHUNK), :] = hot

        block(0)
        pl.when(n_chunks > BLOCK // CHUNK)(functools.partial(block, BLOCK // CHUNK))
        return start + n_chunks * CHUNK

    return lax.fori_loop(0, n_local, body, jnp.int32(0))


def zero_tail(ref, offset, length, tile):
    n_tiles = (length + tile - 1) // tile

    def body(c, carry):
        ref[rows_at(offset + c * CHUNK, CHUNK), :] = jnp.zeros((CHUNK, ref.shape[1]), ref.dtype)
        return carry

    lax.fori_loop(length // CHUNK, n_tiles * (tile // CHUNK), body, 0)
    return n_tiles


def move_segments(pack_ref, wide_ref, base_ref, chunks_ref, src, n_local, cap, to_wide):
    def body(expert, start):
        n_chunks = chunks_ref[src, expert]
        base = expert * cap + base_ref[src, expert]

        def block(first):
            pack_rows = rows_at(start + first, BLOCK)
            wide_rows = rows_at(base + first, BLOCK)
            if to_wide:
                wide_ref[wide_rows, :] = pack_ref[pack_rows, :]
            else:
                pack_ref[pack_rows, :] = wide_ref[wide_rows, :]

        block(0)
        pl.when(n_chunks > BLOCK // CHUNK)(functools.partial(block, BLOCK))
        return start + n_chunks * CHUNK

    lax.fori_loop(0, n_local, body, jnp.int32(0))


def expert_bases(base_ref, total_ref, chunks_ref, n_src, n_local):
    for expert in range(n_local):
        total_ref[expert] = 0

    def body(src, carry):
        for expert in range(n_local):
            base_ref[src, expert] = total_ref[expert]
            total_ref[expert] = total_ref[expert] + chunks_ref[src, expert] * CHUNK
        return carry

    lax.fori_loop(0, n_src, body, 0)


def dispatch(pack_ref, hot_ref, table_ref, wide_ref, base_ref, chunks_ref, src, n_local, cap, length):
    def body(tile, carry):
        rows = rows_at(tile * ROW_TILE, ROW_TILE)
        pack_ref[rows, :] = dot_nn(hot_ref[rows, :], table_ref[...]).astype(BF16)
        return carry

    lax.fori_loop(0, (length + ROW_TILE - 1) // ROW_TILE, body, 0)
    move_segments(pack_ref, wide_ref, base_ref, chunks_ref, src, n_local, cap, True)


def combine(out_ref, pack_ref, hot_ref, wide_ref, base_ref, chunks_ref, src, n_local, cap, length, tile):
    move_segments(pack_ref, wide_ref, base_ref, chunks_ref, src, n_local, cap, False)
    n_tiles = zero_tail(pack_ref, 0, length, tile)
    zero_tail(hot_ref, 0, length, tile)
    out_ref[...] = jnp.zeros_like(out_ref)

    def body(step, carry):
        rows = rows_at(step * tile, tile)
        out_ref[...] += dot_tn(hot_ref[rows, :], pack_ref[rows, :])
        return carry

    lax.fori_loop(0, n_tiles, body, 0)


def tiled_rows(first, count, step):
    n_small = (count + SMALL_TILE - 1) // SMALL_TILE
    per_big = BIG_TILE // SMALL_TILE
    n_big = n_small // per_big

    def big(tile, carry):
        step(rows_at(first + tile * BIG_TILE, BIG_TILE))
        return carry

    def small(tile, carry):
        step(rows_at(first + n_big * BIG_TILE + tile * SMALL_TILE, SMALL_TILE))
        return carry

    lax.fori_loop(0, n_big, big, 0)
    if per_big > 1:
        lax.fori_loop(0, n_small - n_big * per_big, small, 0)


def weight_copies(expert, slot, wg_ref, wu_ref, wd_ref, gu_buf, dn_buf, sems):
    ff = wg_ref.shape[2]
    return (
        pltpu.make_async_copy(wg_ref.at[expert], gu_buf.at[slot, :, pl.ds(0, ff)], sems.at[slot, 0]),
        pltpu.make_async_copy(wu_ref.at[expert], gu_buf.at[slot, :, pl.ds(ff, ff)], sems.at[slot, 1]),
        pltpu.make_async_copy(wd_ref.at[expert], dn_buf.at[slot], sems.at[slot, 2]),
    )


def next_weights(expert, n_local, *refs):
    slot = lax.rem(expert, 2)

    @pl.when(expert + 1 < n_local)
    def _():
        for copy in weight_copies(expert + 1, lax.rem(expert + 1, 2), *refs):
            copy.start()

    for copy in weight_copies(expert, slot, *refs):
        copy.wait()
    return slot


def forward_kernel(n_src, n_local, cap, chunks_ref, tok_ref, pos_ref, gate_ref, wg_ref, wu_ref, wd_ref, out_ref,
                   wide, hot, pack, gu_buf, dn_buf, base, total, sems):
    step = pl.program_id(0)
    ff = wg_ref.shape[2]
    w_refs = (wg_ref, wu_ref, wd_ref, gu_buf, dn_buf, sems)

    @pl.when(step == 0)
    def _():
        for copy in weight_copies(0, 0, *w_refs):
            copy.start()
        expert_bases(base, total, chunks_ref, n_src, n_local)

    @pl.when(step < n_src)
    def _():
        length = fill_onehot(hot, pos_ref, None, chunks_ref, step, n_local)
        dispatch(pack, hot, tok_ref, wide, base, chunks_ref, step, n_local, cap, length)

    @pl.when((step >= n_src) & (step < n_src + n_local))
    def _():
        expert = step - n_src
        slot = next_weights(expert, n_local, *w_refs)

        def rows_step(rows):
            pre = dot_nn(wide[rows, :], gu_buf[slot])
            gate = pre[:, :ff]
            act = (gate * jax.nn.sigmoid(gate) * pre[:, ff:]).astype(BF16)
            wide[rows, :] = dot_nn(act, dn_buf[slot]).astype(BF16)

        tiled_rows(expert * cap, total[expert], rows_step)

    @pl.when(step >= n_src + n_local)
    def _():
        src = step - n_src - n_local
        length = fill_onehot(hot, pos_ref, gate_ref, chunks_ref, src, n_local)
        combine(out_ref, pack, hot, wide, base, chunks_ref, src, n_local, cap, length, ROW_TILE)


def backward_kernel(n_src, n_local, cap, chunks_ref, tok_ref, grad_ref, pos_ref, gate_ref, wg_ref, wu_ref, wd_ref,
                    out_ref, dwg_ref, dwu_ref, dwd_ref,
                    wide_x, wide_q, hot, pack, gu_buf, dn_buf, base, total, sems):
    step = pl.program_id(0)
    ff = wg_ref.shape[2]
    w_refs = (wg_ref, wu_ref, wd_ref, gu_buf, dn_buf, sems)

    @pl.when(step == 0)
    def _():
        for copy in weight_copies(0, 0, *w_refs):
            copy.start()
        expert_bases(base, total, chunks_ref, n_src, n_local)

    @pl.when(step < n_src)
    def _():
        length = fill_onehot(hot, pos_ref, None, chunks_ref, step, n_local)
        dispatch(pack, hot, tok_ref, wide_x, base, chunks_ref, step, n_local, cap, length)
        fill_onehot(hot, pos_ref, gate_ref, chunks_ref, step, n_local)
        dispatch(pack, hot, grad_ref, wide_q, base, chunks_ref, step, n_local, cap, length)

    @pl.when((step >= n_src) & (step < n_src + n_local))
    def _():
        expert = step - n_src
        slot = next_weights(expert, n_local, *w_refs)
        zero_tail(wide_x, expert * cap, total[expert], SMALL_TILE)
        zero_tail(wide_q, expert * cap, total[expert], SMALL_TILE)
        dwg_ref[...] = jnp.zeros_like(dwg_ref)
        dwu_ref[...] = jnp.zeros_like(dwu_ref)
        dwd_ref[...] = jnp.zeros_like(dwd_ref)

        def rows_step(rows):
            x_rows = wide_x[rows, :]
            q_rows = wide_q[rows, :]
            pre = dot_nn(x_rows, gu_buf[slot])
            gate, up = pre[:, :ff], pre[:, ff:]
            sig = jax.nn.sigmoid(gate)
            silu = gate * sig
            act = (silu * up).astype(BF16)
            grad_act = dot_nt(q_rows, dn_buf[slot]).astype(BF16).astype(F32)
            grad_gate = (grad_act * up * (sig * (1.0 + gate * (1.0 - sig)))).astype(BF16)
            grad_up = (grad_act * silu).astype(BF16)
            grad_pre = jnp.concatenate([grad_gate, grad_up], axis=1)
            dwd_ref[0] += dot_tn(act, q_rows)
            dw_pre = dot_tn(x_rows, grad_pre)
            dwg_ref[0] += dw_pre[:, :ff]
            dwu_ref[0] += dw_pre[:, ff:]
            wide_x[rows, :] = dot_nt(grad_pre, gu_buf[slot]).astype(BF16)

        tiled_rows(expert * cap, total[expert], rows_step)

    @pl.when(step >= n_src + n_local)
    def _():
        src = step - n_src - n_local
        length = fill_onehot(hot, pos_ref, None, chunks_ref, src, n_local)
        combine(out_ref, pack, hot, wide_x, base, chunks_ref, src, n_local, cap, length, ROW_TILE)


def expert_call(backward, chunks, tables, pos, gate, w_gate, w_up, w_down):
    n_src, n_local, _, tok_rows = pos.shape
    hidden, ff = w_gate.shape[1:]
    cap = n_src * 128 + BLOCK
    pack_rows = n_local * 128 + BLOCK
    steps = 2 * n_src + n_local

    def src_in(i, *_):
        return (jnp.minimum(i, n_src - 1), 0)

    def src_out(i, *_):
        return (jnp.clip(i - n_src - n_local, 0, n_src - 1), 0)

    def weight_out(i, *_):
        return (jnp.clip(i - n_src, 0, n_local - 1), 0, 0)

    table_spec = pl.BlockSpec((tok_rows, hidden), src_in)

    def route_in(i, *_):
        return (jnp.where(i < n_src, i, jnp.clip(i - n_src - n_local, 0, n_src - 1)), 0, 0, 0)

    route_spec = pl.BlockSpec((1,) + pos.shape[1:], route_in)
    raw = pl.BlockSpec(memory_space=pl.ANY)
    out_shape = [jax.ShapeDtypeStruct((n_src * tok_rows, hidden), F32)]
    out_specs = [pl.BlockSpec((tok_rows, hidden), src_out)]
    wide = pltpu.VMEM((n_local * cap, hidden), BF16)
    scratch = [wide]
    if backward:
        out_shape += [jax.ShapeDtypeStruct(w.shape, F32) for w in (w_gate, w_up, w_down)]
        out_specs += [pl.BlockSpec((1,) + w.shape[1:], weight_out) for w in (w_gate, w_up, w_down)]
        scratch += [wide]
    scratch += [
        pltpu.VMEM((pack_rows, tok_rows), BF16),
        pltpu.VMEM((pack_rows, hidden), BF16),
        pltpu.VMEM((2, hidden, 2 * ff), BF16),
        pltpu.VMEM((2, ff, hidden), BF16),
        pltpu.SMEM((n_src, n_local), jnp.int32),
        pltpu.SMEM((n_local,), jnp.int32),
        pltpu.SemaphoreType.DMA((2, 3)),
    ]
    body = backward_kernel if backward else forward_kernel
    flops = (100 if backward else 60) * 10 ** 9
    return pl.pallas_call(
        functools.partial(body, n_src, n_local, cap),
        grid_spec=pltpu.PrefetchScalarGridSpec(
            num_scalar_prefetch=1,
            grid=(steps,),
            in_specs=[table_spec] * len(tables) + [route_spec, route_spec, raw, raw, raw],
            out_specs=out_specs,
            scratch_shapes=scratch,
        ),
        out_shape=out_shape,
        compiler_params=pltpu.CompilerParams(dimension_semantics=("arbitrary",), vmem_limit_bytes=VMEM_BYTES),
        cost_estimate=pl.CostEstimate(flops=flops, bytes_accessed=60 * 10 ** 6, transcendentals=0),
        name="expert_backward" if backward else "expert_forward",
    )(chunks, *tables, pos, gate, w_gate, w_up, w_down)


def reduce_tail_kernel(part_ref, h_ref, x_ref, grad_ref, pre_ref, w1_ref, w2_ref, out_ref,
                       sums, core_in, x_in, y_in, x_last, y_last, dx_buf, h_buf, x_buf, grad_buf, pre_buf, w1_buf, w2_buf,
                       load_sem, row_sem, weight_sem, core_send, core_recv, hop_send, hop_recv, last_send, last_recv, dx_send, dx_recv):
    n_chunks, half = x_in.shape[0], x_in.shape[2]
    chunk = 2 * half
    tok_rows = n_chunks * chunk
    me = lax.axis_index("ep")
    core, x_pos, y_pos = lax.rem(me, 2), lax.rem(me // 2, 2), me // 4
    x_step, y_step = 2 - 4 * x_pos, 4 - 8 * y_pos
    partner = me + 1 - 2 * core
    x_peer, y_peer = me + x_step, me + y_step
    pp_peer = 1 - lax.axis_index("pp")
    offsets = (0, x_step, y_step, x_step + y_step)
    mesh_id = pl.DeviceIdType.MESH

    barrier = pltpu.get_barrier_semaphore()
    for peer in ({"ep": partner}, {"ep": x_peer}, {"ep": y_peer}, {"pp": pp_peer}):
        pl.semaphore_signal(barrier, inc=1, device_id=peer, device_id_type=mesh_id)
    pl.semaphore_wait(barrier, 4)

    def part_rows(dest, k):
        return part_ref.at[pl.ds(pl.multiple_of(dest * tok_rows + k * chunk, chunk), chunk)]

    def core_copy(k, i):
        return pltpu.make_async_remote_copy(part_rows(partner + offsets[i], k), core_in.at[k, i], core_send.at[k, i], core_recv.at[k, i],
                                            device_id={"ep": partner}, device_id_type=mesh_id)

    def load_copy(k, i):
        return pltpu.make_async_copy(part_rows(me + offsets[i], k), sums.at[k, i], load_sem.at[k, i])

    def hop_copies(k):
        top, low = pl.ds(0, half), pl.ds(half, half)
        return [
            pltpu.make_async_remote_copy(sums.at[k, i, rows], land.at[k, j], hop_send.at[k, n], hop_recv.at[k, n],
                                         device_id={"ep": peer}, device_id_type=mesh_id)
            for n, (i, rows, land, j, peer) in enumerate((
                (3, top, x_in, 1, x_peer), (3, low, y_in, 1, y_peer), (1, top, x_in, 0, x_peer), (2, low, y_in, 0, y_peer)))
        ]

    def last_copies(k):
        top, low = pl.ds(0, half), pl.ds(half, half)
        return [
            pltpu.make_async_remote_copy(sums.at[k, 2, top], y_last.at[k], last_send.at[k, 0], last_recv.at[k, 0],
                                         device_id={"ep": y_peer}, device_id_type=mesh_id),
            pltpu.make_async_remote_copy(sums.at[k, 1, low], x_last.at[k], last_send.at[k, 1], last_recv.at[k, 1],
                                         device_id={"ep": x_peer}, device_id_type=mesh_id),
        ]

    def chunk_rows(k):
        return pl.ds(pl.multiple_of(k * chunk, chunk), chunk)

    def row_copies(k):
        return [pltpu.make_async_copy(src.at[chunk_rows(k)], buf.at[chunk_rows(k)], row_sem.at[k, n])
                for n, (src, buf) in enumerate(((h_ref, h_buf), (x_ref, x_buf), (grad_ref, grad_buf), (pre_ref, pre_buf)))]

    def weight_loads():
        return [pltpu.make_async_copy(w1_ref, w1_buf, weight_sem.at[0]), pltpu.make_async_copy(w2_ref, w2_buf, weight_sem.at[1])]

    def dx_copy(k):
        return pltpu.make_async_remote_copy(dx_buf.at[chunk_rows(k)], out_ref.at[chunk_rows(k)], dx_send.at[k], dx_recv.at[k],
                                            device_id={"pp": pp_peer}, device_id_type=mesh_id)

    def start_chunk(k, carry):
        for i in (3, 1, 2, 0):
            core_copy(k, i).start()
            load_copy(k, i).start()
        return carry

    lax.fori_loop(0, n_chunks, start_chunk, 0)

    def add_cores(k, carry):
        hops = hop_copies(k)
        for i, ready in ((3, (0, 1)), (1, (2,)), (2, (3,)), (0, ())):
            load_copy(k, i).wait()
            core_copy(k, i).wait_recv()
            sums[k, i] = sums[k, i] + core_in[k, i]
            for n in ready:
                hops[n].start()
        return carry

    lax.fori_loop(0, n_chunks, add_cores, 0)

    for copy in weight_loads():
        copy.start()

    def start_rows(k, carry):
        for copy in row_copies(k):
            copy.start()
        return carry

    lax.fori_loop(0, n_chunks, start_rows, 0)

    def relay(k, carry):
        hops, lasts = hop_copies(k), last_copies(k)
        hops[0].wait_recv()
        sums[k, 2, :half] = sums[k, 2, :half] + x_in[k, 1]
        lasts[0].start()
        hops[1].wait_recv()
        sums[k, 1, half:] = sums[k, 1, half:] + y_in[k, 1]
        lasts[1].start()
        return carry

    lax.fori_loop(0, n_chunks, relay, 0)

    for copy in weight_loads():
        copy.wait()

    def norm_grad(values, grads):
        scale = lax.rsqrt(jnp.mean(values * values, axis=-1, keepdims=True) + NORM_EPS)
        return scale * grads - values * (scale * scale * scale * jnp.mean(grads * values, axis=-1, keepdims=True))

    def finish(k, carry):
        rows = chunk_rows(k)
        hops, lasts = hop_copies(k), last_copies(k)
        for copy in row_copies(k):
            copy.wait()
        for copy in hops[2:]:
            copy.wait_recv()
        for copy in lasts:
            copy.wait_recv()
        sums[k, 0, :half] = sums[k, 0, :half] + x_in[k, 0] + y_last[k]
        sums[k, 0, half:] = sums[k, 0, half:] + y_in[k, 0] + x_last[k]
        grad_h = grad_buf[rows, :].astype(F32) + norm_grad(h_buf[rows, :].astype(F32), sums[k, 0])
        grad_act = dot_nt(grad_h.astype(BF16), w2_buf[...])
        grad_pre = (grad_act * silu_grad(pre_buf[rows, :])).astype(BF16)
        grad_norm = dot_nt(grad_pre, w1_buf[...])
        dx_buf[rows, :] = (grad_h + norm_grad(x_buf[rows, :].astype(F32), grad_norm)).astype(BF16)
        dx_copy(k).start()
        return carry

    lax.fori_loop(0, n_chunks, finish, 0)

    def drain(k, carry):
        for i in range(4):
            core_copy(k, i).wait_send()
        for copy in hop_copies(k) + last_copies(k):
            copy.wait_send()
        dx_copy(k).wait()
        return carry

    lax.fori_loop(0, n_chunks, drain, 0)


def reduce_tail(part, h_rows, x_rows, grad_rows, hidden_pre, w_one, w_two):
    tok_rows, hidden = x_rows.shape
    ff = w_one.shape[1]
    n_chunks = 4
    half = tok_rows // (2 * n_chunks)
    raw = pl.BlockSpec(memory_space=pl.ANY)
    dma = pltpu.SemaphoreType.DMA
    rows_buf = pltpu.VMEM((tok_rows, hidden), BF16)
    return pl.pallas_call(
        reduce_tail_kernel,
        out_shape=jax.ShapeDtypeStruct((tok_rows, hidden), BF16),
        in_specs=[raw] * 7,
        out_specs=raw,
        scratch_shapes=[
            pltpu.VMEM((n_chunks, 4, 2 * half, hidden), F32),
            pltpu.VMEM((n_chunks, 4, 2 * half, hidden), F32),
            pltpu.VMEM((n_chunks, 2, half, hidden), F32),
            pltpu.VMEM((n_chunks, 2, half, hidden), F32),
            pltpu.VMEM((n_chunks, half, hidden), F32),
            pltpu.VMEM((n_chunks, half, hidden), F32),
            rows_buf, rows_buf, rows_buf, rows_buf,
            pltpu.VMEM((tok_rows, ff), F32),
            pltpu.VMEM(w_one.shape, BF16),
            pltpu.VMEM(w_two.shape, BF16),
            dma((n_chunks, 4)), dma((n_chunks, 4)), dma((2,)),
            dma((n_chunks, 4)), dma((n_chunks, 4)), dma((n_chunks, 4)), dma((n_chunks, 4)),
            dma((n_chunks, 2)), dma((n_chunks, 2)), dma((n_chunks,)), dma((n_chunks,)),
        ],
        compiler_params=pltpu.CompilerParams(collective_id=0, has_side_effects=True, vmem_limit_bytes=VMEM_BYTES),
        cost_estimate=pl.CostEstimate(flops=60 * 10 ** 9, bytes_accessed=40 * 10 ** 6, transcendentals=0),
        name="reduce_tail",
    )(part, h_rows, x_rows, grad_rows, hidden_pre, w_one, w_two)


def route_tables(ids, gates, first, n_local):
    tok_rows = ids.shape[2]
    experts = (first + jnp.arange(n_local)).astype(F32)
    match = ids[:, None] == experts[None, :, None, None]
    kept = jnp.any(match, axis=2)
    gate = jnp.sum(jnp.where(match, gates[:, None], 0.0), axis=2)
    upper = (jnp.arange(tok_rows)[:, None] <= jnp.arange(tok_rows)[None, :]).astype(BF16)
    rank = jnp.einsum("set,tu->seu", kept.astype(BF16), upper, preferred_element_type=F32)
    pos = jnp.where(kept, rank - 1.0, -1.0).astype(BF16)
    chunks = (rank[:, :, -1].astype(jnp.int32) + CHUNK - 1) // CHUNK
    shape = pos.shape[:2] + (CHUNK, tok_rows)
    return jnp.broadcast_to(pos[:, :, None], shape), jnp.broadcast_to(gate.astype(BF16)[:, :, None], shape), chunks


def solution(mesh):
    stages = mesh.shape["pp"]
    ep_size = mesh.shape["ep"]
    next_perm = [(stage_idx, (stage_idx + 1) % stages) for stage_idx in range(stages)]
    assert (stages, ep_size) == (2, 8)
    tok_spec = P("pp", "ep", None)
    dense_spec = P("pp", None, None)
    expert_spec = P("pp", "ep", None, None)

    def device_step(x_fwd, ids_fwd, slots_fwd, gates_fwd, x_saved, grad_in, ids_bwd, slots_bwd, gates_bwd, w_one, w_two, w_gate, w_up, w_down):
        x_fwd, ids_fwd, slots_fwd, gates_fwd = x_fwd[0], ids_fwd[0], slots_fwd[0], gates_fwd[0]
        x_saved, grad_in, ids_bwd, slots_bwd, gates_bwd = x_saved[0], grad_in[0], ids_bwd[0], slots_bwd[0], gates_bwd[0]
        w_one, w_two, w_gate, w_up, w_down = w_one[0], w_two[0], w_gate[0], w_up[0], w_down[0]
        top_k = ids_fwd.shape[1]
        n_local = w_gate.shape[0]
        first = lax.axis_index("ep") * n_local

        h_fwd, _ = dense_forward(x_fwd, w_one, w_two)
        xn_fwd = rms_norm(h_fwd.astype(F32)).astype(BF16)
        all_fwd = lax.all_gather(xn_fwd, "ep", axis=0, tiled=True)

        xn_fwd, x_saved, grad_in = lax.optimization_barrier((xn_fwd, x_saved, grad_in))
        all_grad = lax.all_gather(grad_in, "ep", axis=0, tiled=True)
        routes = jnp.concatenate([
            jnp.where(slots_fwd >= 0, ids_fwd, -1).astype(BF16), gates_fwd,
            jnp.where(slots_bwd >= 0, ids_bwd, -1).astype(BF16), gates_bwd,
        ], axis=1).T
        routes = lax.all_gather(routes, "ep", axis=0, tiled=False).astype(F32)
        id_f, gate_f, id_b, gate_b = (routes[:, i * top_k:(i + 1) * top_k] for i in range(4))
        pos_f, gate_f, chunks_f = route_tables(id_f, gate_f, first, n_local)
        pos_b, gate_b, chunks_b = route_tables(id_b, gate_b, first, n_local)
        h_bwd, hidden_pre = dense_forward(x_saved, w_one, w_two)
        xn_bwd = rms_norm(h_bwd.astype(F32)).astype(BF16)
        all_bwd = lax.all_gather(xn_bwd, "ep", axis=0, tiled=True)

        (part_fwd,) = expert_call(False, chunks_f, (all_fwd,), pos_f, gate_f, w_gate, w_up, w_down)
        mix_sum = lax.psum_scatter(part_fwd, "ep", scatter_dimension=0, tiled=True)
        y_out = (h_fwd.astype(F32) + mix_sum).astype(BF16)

        chunks_b, _ = lax.optimization_barrier((chunks_b, part_fwd))
        part_bwd, dw_gate, dw_up, dw_down = expert_call(True, chunks_b, (all_bwd, all_grad), pos_b, gate_b, w_gate, w_up, w_down)
        y_next = lax.ppermute(y_out, "pp", next_perm)
        dx_prev = reduce_tail(part_bwd, h_bwd, x_saved, grad_in, hidden_pre, w_one, w_two)
        return y_next[None], dx_prev[None], dw_gate[None], dw_up[None], dw_down[None]

    in_specs = (tok_spec,) * 9 + (dense_spec, dense_spec, expert_spec, expert_spec, expert_spec)
    out_specs = (tok_spec, tok_spec, expert_spec, expert_spec, expert_spec)
    return jax.shard_map(device_step, mesh=mesh, in_specs=in_specs, out_specs=out_specs, check_vma=False)
```

```python
import functools

import jax
import jax.numpy as jnp
from jax import lax
from jax.experimental import pallas as pl
from jax.experimental.pallas import tpu as pltpu
from jax.sharding import PartitionSpec as P

NORM_EPS = 1e-6
CHUNK = 16
BLOCK = 64
UNROLL = 4
ROW_TILE = 1024
COMB_TILE = 512
BIG_TILE = 512
SMALL_TILE = 256
VMEM_BYTES = 66_500_000
BF16 = jnp.bfloat16
F32 = jnp.float32


def rms_norm(values):
    return values * lax.rsqrt(jnp.mean(values * values, axis=-1, keepdims=True) + NORM_EPS)


def silu_grad(values):
    sigmoid_vals = jax.nn.sigmoid(values)
    return sigmoid_vals * (1.0 + values * (1.0 - sigmoid_vals))


def dense_forward(x_rows, w_one, w_two):
    normed = rms_norm(x_rows.astype(F32)).astype(BF16)
    hidden_pre = jnp.dot(normed, w_one, preferred_element_type=F32)
    dense_act = jax.nn.silu(hidden_pre).astype(BF16)
    dense_out = jnp.dot(dense_act, w_two, preferred_element_type=F32)
    return (x_rows.astype(F32) + dense_out).astype(BF16), hidden_pre


def dot_nn(lhs, rhs):
    return jnp.dot(lhs, rhs, preferred_element_type=F32)


def dot_nt(lhs, rhs):
    return lax.dot_general(lhs, rhs, (((1,), (1,)), ((), ())), preferred_element_type=F32)


def dot_tn(lhs, rhs):
    return lax.dot_general(lhs, rhs, (((0,), (0,)), ((), ())), preferred_element_type=F32)


def rows_at(index, count):
    return pl.ds(pl.multiple_of(index, CHUNK), count)


def fill_onehot(hot_ref, rep, pos_ref, gate_ref, chunks_ref, src, n_local):
    tok_rows = pos_ref.shape[2]
    iota = lax.broadcasted_iota(jnp.int32, (CHUNK, tok_rows), 0).astype(F32).astype(BF16)
    ones = jnp.ones((CHUNK, tok_rows), BF16)
    for expert in range(n_local):
        rep[0, expert] = jnp.broadcast_to(pos_ref[0, expert:expert + 1, :], (CHUNK, tok_rows)).astype(BF16)
        if gate_ref is not None:
            rep[1, expert] = jnp.broadcast_to(gate_ref[0, expert:expert + 1, :], (CHUNK, tok_rows)).astype(BF16)

    def one(expert, start):
        n_chunks = chunks_ref[src, expert]

        def block(first):
            pos_rows = rep[0, expert]
            value = ones if gate_ref is None else rep[1, expert]
            for c in range(first, first + BLOCK // CHUNK):
                hot = jnp.where(iota + jnp.bfloat16(c * CHUNK) == pos_rows, value, jnp.zeros_like(value))
                hot_ref[rows_at(start + c * CHUNK, CHUNK), :] = hot

        block(0)
        pl.when(n_chunks > BLOCK // CHUNK)(functools.partial(block, BLOCK // CHUNK))
        return start + n_chunks * CHUNK

    return expert_loop(n_local, one)


def expert_loop(n_local, one):
    def body(group, start):
        for i in range(UNROLL):
            start = one(group * UNROLL + i, start)
        return start

    return lax.fori_loop(0, n_local // UNROLL, body, jnp.int32(0))


def zero_tail(ref, offset, length, tile):
    n_tiles = (length + tile - 1) // tile

    def body(c, carry):
        ref[rows_at(offset + c * CHUNK, CHUNK), :] = jnp.zeros((CHUNK, ref.shape[1]), ref.dtype)
        return carry

    lax.fori_loop(length // CHUNK, n_tiles * (tile // CHUNK), body, 0)


def move_segments(pack_ref, wide_ref, base_ref, chunks_ref, src, n_local, cap, to_wide):
    def one(expert, start):
        n_chunks = chunks_ref[src, expert]
        base = expert * cap + base_ref[src, expert]

        def block(first):
            pack_rows = rows_at(start + first, BLOCK)
            wide_rows = rows_at(base + first, BLOCK)
            if to_wide:
                wide_ref[wide_rows, :] = pack_ref[pack_rows, :]
            else:
                pack_ref[pack_rows, :] = wide_ref[wide_rows, :]

        block(0)
        pl.when(n_chunks > BLOCK // CHUNK)(functools.partial(block, BLOCK))
        return start + n_chunks * CHUNK

    expert_loop(n_local, one)


def expert_bases(base_ref, total_ref, chunks_ref, n_src, n_local):
    for expert in range(n_local):
        total_ref[expert] = 0

    def body(src, carry):
        for expert in range(n_local):
            base_ref[src, expert] = total_ref[expert]
            total_ref[expert] = total_ref[expert] + chunks_ref[src, expert] * CHUNK
        return carry

    lax.fori_loop(0, n_src, body, 0)


def dispatch(pack_ref, hot_ref, table_ref, columns, wide_ref, base_ref, chunks_ref, src, n_local, cap, length):
    def step(rows):
        pack_ref[rows, :] = dot_nn(hot_ref[rows, :], table_ref[:, columns]).astype(BF16)

    tiled_rows(0, length, step, ROW_TILE, SMALL_TILE)
    move_segments(pack_ref, wide_ref, base_ref, chunks_ref, src, n_local, cap, True)


def combine(out_ref, pack_ref, hot_ref, wide_ref, base_ref, chunks_ref, src, n_local, cap, length):
    move_segments(pack_ref, wide_ref, base_ref, chunks_ref, src, n_local, cap, False)
    zero_tail(pack_ref, 0, length, COMB_TILE)
    zero_tail(hot_ref, 0, length, COMB_TILE)
    out_ref[...] = jnp.zeros_like(out_ref)

    def step(rows):
        out_ref[...] += dot_tn(hot_ref[rows, :], pack_ref[rows, :])

    tiled_rows(0, length, step, ROW_TILE, COMB_TILE)


def tiled_rows(first, count, step, big_tile, small_tile):
    n_small = (count + small_tile - 1) // small_tile
    per_big = big_tile // small_tile
    n_big = n_small // per_big

    def big(tile, carry):
        step(rows_at(first + tile * big_tile, big_tile))
        return carry

    lax.fori_loop(0, n_big, big, 0)
    for left in range(1, per_big):
        pl.when(n_small - n_big * per_big == left)(
            functools.partial(step, rows_at(first + n_big * big_tile, left * small_tile)))


def weight_copies(expert, slot, wg_ref, wu_ref, wd_ref, gu_buf, dn_buf, sems):
    ff = wg_ref.shape[2]
    return (
        pltpu.make_async_copy(wg_ref.at[expert], gu_buf.at[slot, :, pl.ds(0, ff)], sems.at[slot, 0]),
        pltpu.make_async_copy(wu_ref.at[expert], gu_buf.at[slot, :, pl.ds(ff, ff)], sems.at[slot, 1]),
        pltpu.make_async_copy(wd_ref.at[expert], dn_buf.at[slot], sems.at[slot, 2]),
    )


def next_weights(expert, n_local, *refs):
    slot = lax.rem(expert, 2)

    @pl.when(expert + 1 < n_local)
    def _():
        for copy in weight_copies(expert + 1, lax.rem(expert + 1, 2), *refs):
            copy.start()

    for copy in weight_copies(expert, slot, *refs):
        copy.wait()
    return slot


def forward_kernel(n_src, n_local, cap, chunks_ref, tok_ref, pos_ref, gate_ref, wg_ref, wu_ref, wd_ref, out_ref,
                   wide, hot, rep, pack, gu_buf, dn_buf, base, total, sems):
    step = pl.program_id(0)
    hidden, ff = wg_ref.shape[1:]
    w_refs = (wg_ref, wu_ref, wd_ref, gu_buf, dn_buf, sems)

    @pl.when(step == 0)
    def _():
        for copy in weight_copies(0, 0, *w_refs):
            copy.start()
        expert_bases(base, total, chunks_ref, n_src, n_local)

    @pl.when(step < n_src)
    def _():
        length = fill_onehot(hot, rep, pos_ref, None, chunks_ref, step, n_local)
        dispatch(pack, hot, tok_ref, pl.ds(0, hidden), wide, base, chunks_ref, step, n_local, cap, length)

    @pl.when((step >= n_src) & (step < n_src + n_local))
    def _():
        expert = step - n_src
        slot = next_weights(expert, n_local, *w_refs)

        def rows_step(rows):
            pre = dot_nn(wide[rows, :], gu_buf[slot])
            gate = pre[:, :ff]
            act = (gate * jax.nn.sigmoid(gate) * pre[:, ff:]).astype(BF16)
            wide[rows, :] = dot_nn(act, dn_buf[slot]).astype(BF16)

        tiled_rows(expert * cap, total[expert], rows_step, BIG_TILE, SMALL_TILE)

    @pl.when(step >= n_src + n_local)
    def _():
        src = step - n_src - n_local
        length = fill_onehot(hot, rep, pos_ref, gate_ref, chunks_ref, src, n_local)
        combine(out_ref, pack, hot, wide, base, chunks_ref, src, n_local, cap, length)


def backward_kernel(n_src, n_local, cap, chunks_ref, tok_ref, pos_ref, gate_ref, wg_ref, wu_ref, wd_ref,
                    out_ref, dwg_ref, dwu_ref, dwd_ref,
                    wide_x, wide_q, hot, rep, pack, gu_buf, dn_buf, base, total, sems):
    step = pl.program_id(0)
    hidden, ff = wg_ref.shape[1:]
    w_refs = (wg_ref, wu_ref, wd_ref, gu_buf, dn_buf, sems)

    @pl.when(step == 0)
    def _():
        for copy in weight_copies(0, 0, *w_refs):
            copy.start()
        expert_bases(base, total, chunks_ref, n_src, n_local)

    @pl.when(step < n_src)
    def _():
        length = fill_onehot(hot, rep, pos_ref, None, chunks_ref, step, n_local)
        dispatch(pack, hot, tok_ref, pl.ds(0, hidden), wide_x, base, chunks_ref, step, n_local, cap, length)
        fill_onehot(hot, rep, pos_ref, gate_ref, chunks_ref, step, n_local)
        dispatch(pack, hot, tok_ref, pl.ds(hidden, hidden), wide_q, base, chunks_ref, step, n_local, cap, length)

    @pl.when((step >= n_src) & (step < n_src + n_local))
    def _():
        expert = step - n_src
        slot = next_weights(expert, n_local, *w_refs)
        zero_tail(wide_x, expert * cap, total[expert], SMALL_TILE)
        zero_tail(wide_q, expert * cap, total[expert], SMALL_TILE)
        dwg_ref[...] = jnp.zeros_like(dwg_ref)
        dwu_ref[...] = jnp.zeros_like(dwu_ref)
        dwd_ref[...] = jnp.zeros_like(dwd_ref)

        def rows_step(rows):
            x_rows = wide_x[rows, :]
            q_rows = wide_q[rows, :]
            pre = dot_nn(x_rows, gu_buf[slot])
            gate, up = pre[:, :ff], pre[:, ff:]
            sig = jax.nn.sigmoid(gate)
            silu = gate * sig
            act = (silu * up).astype(BF16)
            grad_act = dot_nt(q_rows, dn_buf[slot]).astype(BF16).astype(F32)
            grad_gate = (grad_act * up * (sig * (1.0 + gate * (1.0 - sig)))).astype(BF16)
            grad_up = (grad_act * silu).astype(BF16)
            grad_pre = jnp.concatenate([grad_gate, grad_up], axis=1)
            dwd_ref[0] += dot_tn(act, q_rows)
            dw_pre = dot_tn(x_rows, grad_pre)
            dwg_ref[0] += dw_pre[:, :ff]
            dwu_ref[0] += dw_pre[:, ff:]
            wide_x[rows, :] = dot_nt(grad_pre, gu_buf[slot]).astype(BF16)

        tiled_rows(expert * cap, total[expert], rows_step, BIG_TILE, SMALL_TILE)

    @pl.when(step >= n_src + n_local)
    def _():
        src = step - n_src - n_local
        length = fill_onehot(hot, rep, pos_ref, None, chunks_ref, src, n_local)
        combine(out_ref, pack, hot, wide_x, base, chunks_ref, src, n_local, cap, length)


def expert_call(backward, chunks, table, pos, gate, w_gate, w_up, w_down):
    n_src, n_local, tok_rows = pos.shape
    hidden, ff = w_gate.shape[1:]
    cap = n_src * 128 + BLOCK
    pack_rows = n_local * 128 + BLOCK
    steps = 2 * n_src + n_local

    def src_in(i, *_):
        return (jnp.minimum(i, n_src - 1), 0)

    def src_out(i, *_):
        return (jnp.clip(i - n_src - n_local, 0, n_src - 1), 0)

    def weight_out(i, *_):
        return (jnp.clip(i - n_src, 0, n_local - 1), 0, 0)

    table_spec = pl.BlockSpec((tok_rows, table.shape[1]), src_in)

    def route_in(i, *_):
        return (jnp.where(i < n_src, i, jnp.clip(i - n_src - n_local, 0, n_src - 1)), 0, 0)

    route_spec = pl.BlockSpec((1,) + pos.shape[1:], route_in)
    raw = pl.BlockSpec(memory_space=pl.ANY)
    out_shape = [jax.ShapeDtypeStruct((n_src * tok_rows, hidden), F32)]
    out_specs = [pl.BlockSpec((tok_rows, hidden), src_out)]
    wide = pltpu.VMEM((n_local * cap, hidden), BF16)
    scratch = [wide]
    if backward:
        out_shape += [jax.ShapeDtypeStruct(w.shape, F32) for w in (w_gate, w_up, w_down)]
        out_specs += [pl.BlockSpec((1,) + w.shape[1:], weight_out) for w in (w_gate, w_up, w_down)]
        scratch += [wide]
    scratch += [
        pltpu.VMEM((pack_rows, tok_rows), BF16),
        pltpu.VMEM((2, n_local, CHUNK, tok_rows), BF16),
        pltpu.VMEM((pack_rows, hidden), BF16),
        pltpu.VMEM((2, hidden, 2 * ff), BF16),
        pltpu.VMEM((2, ff, hidden), BF16),
        pltpu.SMEM((n_src, n_local), jnp.int32),
        pltpu.SMEM((n_local,), jnp.int32),
        pltpu.SemaphoreType.DMA((2, 3)),
    ]
    body = backward_kernel if backward else forward_kernel
    flops = (100 if backward else 60) * 10 ** 9
    return pl.pallas_call(
        functools.partial(body, n_src, n_local, cap),
        grid_spec=pltpu.PrefetchScalarGridSpec(
            num_scalar_prefetch=1,
            grid=(steps,),
            in_specs=[table_spec] + [route_spec, route_spec, raw, raw, raw],
            out_specs=out_specs,
            scratch_shapes=scratch,
        ),
        out_shape=out_shape,
        compiler_params=pltpu.CompilerParams(dimension_semantics=("arbitrary",), vmem_limit_bytes=VMEM_BYTES),
        cost_estimate=pl.CostEstimate(flops=flops, bytes_accessed=60 * 10 ** 6, transcendentals=0),
        name="expert_backward" if backward else "expert_forward",
    )(chunks, table, pos, gate, w_gate, w_up, w_down)


def reduce_tail_kernel(part_ref, h_ref, x_ref, grad_ref, pre_ref, w1_ref, w2_ref, out_ref,
                       sums, core_in, x_in, y_in, x_last, y_last, dx_buf, h_buf, x_buf, grad_buf, pre_buf, w1_buf, w2_buf,
                       load_sem, row_sem, weight_sem, core_send, core_recv, hop_send, hop_recv, last_send, last_recv, dx_send, dx_recv):
    n_chunks, half = x_in.shape[0], x_in.shape[2]
    chunk = 2 * half
    tok_rows = n_chunks * chunk
    me = lax.axis_index("ep")
    core, x_pos, y_pos = lax.rem(me, 2), lax.rem(me // 2, 2), me // 4
    x_step, y_step = 2 - 4 * x_pos, 4 - 8 * y_pos
    partner = me + 1 - 2 * core
    x_peer, y_peer = me + x_step, me + y_step
    pp_peer = 1 - lax.axis_index("pp")
    offsets = (0, x_step, y_step, x_step + y_step)
    mesh_id = pl.DeviceIdType.MESH

    barrier = pltpu.get_barrier_semaphore()
    for peer in ({"ep": partner}, {"ep": x_peer}, {"ep": y_peer}, {"pp": pp_peer}):
        pl.semaphore_signal(barrier, inc=1, device_id=peer, device_id_type=mesh_id)
    pl.semaphore_wait(barrier, 4)

    def part_rows(dest, k):
        return part_ref.at[pl.ds(pl.multiple_of(dest * tok_rows + k * chunk, chunk), chunk)]

    def core_copy(k, i):
        return pltpu.make_async_remote_copy(part_rows(partner + offsets[i], k), core_in.at[k, i], core_send.at[k, i], core_recv.at[k, i],
                                            device_id={"ep": partner}, device_id_type=mesh_id)

    def load_copy(k, i):
        return pltpu.make_async_copy(part_rows(me + offsets[i], k), sums.at[k, i], load_sem.at[k, i])

    def hop_copies(k):
        top, low = pl.ds(0, half), pl.ds(half, half)
        return [
            pltpu.make_async_remote_copy(sums.at[k, i, rows], land.at[k, j], hop_send.at[k, n], hop_recv.at[k, n],
                                         device_id={"ep": peer}, device_id_type=mesh_id)
            for n, (i, rows, land, j, peer) in enumerate((
                (3, top, x_in, 1, x_peer), (3, low, y_in, 1, y_peer), (1, top, x_in, 0, x_peer), (2, low, y_in, 0, y_peer)))
        ]

    def last_copies(k):
        top, low = pl.ds(0, half), pl.ds(half, half)
        return [
            pltpu.make_async_remote_copy(sums.at[k, 2, top], y_last.at[k], last_send.at[k, 0], last_recv.at[k, 0],
                                         device_id={"ep": y_peer}, device_id_type=mesh_id),
            pltpu.make_async_remote_copy(sums.at[k, 1, low], x_last.at[k], last_send.at[k, 1], last_recv.at[k, 1],
                                         device_id={"ep": x_peer}, device_id_type=mesh_id),
        ]

    def chunk_rows(k):
        return pl.ds(pl.multiple_of(k * chunk, chunk), chunk)

    def row_copies(k):
        return [pltpu.make_async_copy(src.at[chunk_rows(k)], buf.at[chunk_rows(k)], row_sem.at[k, n])
                for n, (src, buf) in enumerate(((h_ref, h_buf), (x_ref, x_buf), (grad_ref, grad_buf), (pre_ref, pre_buf)))]

    def weight_loads():
        return [pltpu.make_async_copy(w1_ref, w1_buf, weight_sem.at[0]), pltpu.make_async_copy(w2_ref, w2_buf, weight_sem.at[1])]

    def dx_copy(k):
        return pltpu.make_async_remote_copy(dx_buf.at[chunk_rows(k)], out_ref.at[chunk_rows(k)], dx_send.at[k], dx_recv.at[k],
                                            device_id={"pp": pp_peer}, device_id_type=mesh_id)

    def start_chunk(k, carry):
        for i in (3, 1, 2, 0):
            core_copy(k, i).start()
            load_copy(k, i).start()
        return carry

    lax.fori_loop(0, n_chunks, start_chunk, 0)

    def add_cores(k, carry):
        hops = hop_copies(k)
        for i, ready in ((3, (0, 1)), (1, (2,)), (2, (3,)), (0, ())):
            load_copy(k, i).wait()
            core_copy(k, i).wait_recv()
            sums[k, i] = sums[k, i] + core_in[k, i]
            for n in ready:
                hops[n].start()
        return carry

    lax.fori_loop(0, n_chunks, add_cores, 0)

    for copy in weight_loads():
        copy.start()

    def start_rows(k, carry):
        for copy in row_copies(k):
            copy.start()
        return carry

    lax.fori_loop(0, n_chunks, start_rows, 0)

    def relay(k, carry):
        hops, lasts = hop_copies(k), last_copies(k)
        hops[0].wait_recv()
        sums[k, 2, :half] = sums[k, 2, :half] + x_in[k, 1]
        lasts[0].start()
        hops[1].wait_recv()
        sums[k, 1, half:] = sums[k, 1, half:] + y_in[k, 1]
        lasts[1].start()
        return carry

    lax.fori_loop(0, n_chunks, relay, 0)

    for copy in weight_loads():
        copy.wait()

    def norm_grad(values, grads):
        scale = lax.rsqrt(jnp.mean(values * values, axis=-1, keepdims=True) + NORM_EPS)
        return scale * grads - values * (scale * scale * scale * jnp.mean(grads * values, axis=-1, keepdims=True))

    def finish(k, carry):
        rows = chunk_rows(k)
        hops, lasts = hop_copies(k), last_copies(k)
        for copy in row_copies(k):
            copy.wait()
        for copy in hops[2:]:
            copy.wait_recv()
        for copy in lasts:
            copy.wait_recv()
        sums[k, 0, :half] = sums[k, 0, :half] + x_in[k, 0] + y_last[k]
        sums[k, 0, half:] = sums[k, 0, half:] + y_in[k, 0] + x_last[k]
        grad_h = grad_buf[rows, :].astype(F32) + norm_grad(h_buf[rows, :].astype(F32), sums[k, 0])
        grad_act = dot_nt(grad_h.astype(BF16), w2_buf[...])
        grad_pre = (grad_act * silu_grad(pre_buf[rows, :])).astype(BF16)
        grad_norm = dot_nt(grad_pre, w1_buf[...])
        dx_buf[rows, :] = (grad_h + norm_grad(x_buf[rows, :].astype(F32), grad_norm)).astype(BF16)
        dx_copy(k).start()
        return carry

    lax.fori_loop(0, n_chunks, finish, 0)

    def drain(k, carry):
        for i in range(4):
            core_copy(k, i).wait_send()
        for copy in hop_copies(k) + last_copies(k):
            copy.wait_send()
        dx_copy(k).wait()
        return carry

    lax.fori_loop(0, n_chunks, drain, 0)


def reduce_tail(part, h_rows, x_rows, grad_rows, hidden_pre, w_one, w_two):
    tok_rows, hidden = x_rows.shape
    ff = w_one.shape[1]
    n_chunks = 4
    half = tok_rows // (2 * n_chunks)
    raw = pl.BlockSpec(memory_space=pl.ANY)
    dma = pltpu.SemaphoreType.DMA
    rows_buf = pltpu.VMEM((tok_rows, hidden), BF16)
    return pl.pallas_call(
        reduce_tail_kernel,
        out_shape=jax.ShapeDtypeStruct((tok_rows, hidden), BF16),
        in_specs=[raw] * 7,
        out_specs=raw,
        scratch_shapes=[
            pltpu.VMEM((n_chunks, 4, 2 * half, hidden), F32),
            pltpu.VMEM((n_chunks, 4, 2 * half, hidden), F32),
            pltpu.VMEM((n_chunks, 2, half, hidden), F32),
            pltpu.VMEM((n_chunks, 2, half, hidden), F32),
            pltpu.VMEM((n_chunks, half, hidden), F32),
            pltpu.VMEM((n_chunks, half, hidden), F32),
            rows_buf, rows_buf, rows_buf, rows_buf,
            pltpu.VMEM((tok_rows, ff), F32),
            pltpu.VMEM(w_one.shape, BF16),
            pltpu.VMEM(w_two.shape, BF16),
            dma((n_chunks, 4)), dma((n_chunks, 4)), dma((2,)),
            dma((n_chunks, 4)), dma((n_chunks, 4)), dma((n_chunks, 4)), dma((n_chunks, 4)),
            dma((n_chunks, 2)), dma((n_chunks, 2)), dma((n_chunks,)), dma((n_chunks,)),
        ],
        compiler_params=pltpu.CompilerParams(collective_id=0, has_side_effects=True, vmem_limit_bytes=VMEM_BYTES),
        cost_estimate=pl.CostEstimate(flops=60 * 10 ** 9, bytes_accessed=40 * 10 ** 6, transcendentals=0),
        name="reduce_tail",
    )(part, h_rows, x_rows, grad_rows, hidden_pre, w_one, w_two)


def route_tables(ids, gates, first, n_local):
    tok_rows = ids.shape[2]
    experts = (first + jnp.arange(n_local)).astype(F32)
    match = ids[:, None] == experts[None, :, None, None]
    kept = jnp.any(match, axis=2)
    gate = jnp.sum(jnp.where(match, gates[:, None], 0.0), axis=2)
    upper = (jnp.arange(tok_rows)[:, None] <= jnp.arange(tok_rows)[None, :]).astype(BF16)
    rank = jnp.einsum("set,tu->seu", kept.astype(BF16), upper, preferred_element_type=F32)
    pos = jnp.where(kept, rank - 1.0, -1.0)
    chunks = (rank[:, :, -1].astype(jnp.int32) + CHUNK - 1) // CHUNK
    return pos, gate, chunks


def solution(mesh):
    stages = mesh.shape["pp"]
    ep_size = mesh.shape["ep"]
    next_perm = [(stage_idx, (stage_idx + 1) % stages) for stage_idx in range(stages)]
    assert (stages, ep_size) == (2, 8)
    tok_spec = P("pp", "ep", None)
    dense_spec = P("pp", None, None)
    expert_spec = P("pp", "ep", None, None)

    def device_step(x_fwd, ids_fwd, slots_fwd, gates_fwd, x_saved, grad_in, ids_bwd, slots_bwd, gates_bwd, w_one, w_two, w_gate, w_up, w_down):
        x_fwd, ids_fwd, slots_fwd, gates_fwd = x_fwd[0], ids_fwd[0], slots_fwd[0], gates_fwd[0]
        x_saved, grad_in, ids_bwd, slots_bwd, gates_bwd = x_saved[0], grad_in[0], ids_bwd[0], slots_bwd[0], gates_bwd[0]
        w_one, w_two, w_gate, w_up, w_down = w_one[0], w_two[0], w_gate[0], w_up[0], w_down[0]
        top_k = ids_fwd.shape[1]
        n_local = w_gate.shape[0]
        first = lax.axis_index("ep") * n_local

        h_fwd, _ = dense_forward(x_fwd, w_one, w_two)
        xn_fwd = rms_norm(h_fwd.astype(F32)).astype(BF16)
        all_fwd = lax.all_gather(xn_fwd, "ep", axis=0, tiled=True)

        xn_fwd, x_saved, grad_in = lax.optimization_barrier((xn_fwd, x_saved, grad_in))
        routes = jnp.concatenate([
            jnp.where(slots_fwd >= 0, ids_fwd, -1).astype(BF16), gates_fwd,
            jnp.where(slots_bwd >= 0, ids_bwd, -1).astype(BF16), gates_bwd,
        ], axis=1).T
        routes = lax.all_gather(routes, "ep", axis=0, tiled=False).astype(F32)
        id_f, gate_f, id_b, gate_b = (routes[:, i * top_k:(i + 1) * top_k] for i in range(4))
        pos_f, gate_f, chunks_f = route_tables(id_f, gate_f, first, n_local)
        pos_b, gate_b, chunks_b = route_tables(id_b, gate_b, first, n_local)
        h_bwd, hidden_pre = dense_forward(x_saved, w_one, w_two)
        xn_bwd = rms_norm(h_bwd.astype(F32)).astype(BF16)
        all_bwd = lax.all_gather(jnp.concatenate([xn_bwd, grad_in], axis=1), "ep", axis=0, tiled=True)

        (part_fwd,) = expert_call(False, chunks_f, all_fwd, pos_f, gate_f, w_gate, w_up, w_down)
        mix_sum = lax.psum_scatter(part_fwd, "ep", scatter_dimension=0, tiled=True)
        y_out = (h_fwd.astype(F32) + mix_sum).astype(BF16)

        chunks_b, _ = lax.optimization_barrier((chunks_b, part_fwd))
        part_bwd, dw_gate, dw_up, dw_down = expert_call(True, chunks_b, all_bwd, pos_b, gate_b, w_gate, w_up, w_down)
        y_next = lax.ppermute(y_out, "pp", next_perm)
        dx_prev = reduce_tail(part_bwd, h_bwd, x_saved, grad_in, hidden_pre, w_one, w_two)
        return y_next[None], dx_prev[None], dw_gate[None], dw_up[None], dw_down[None]

    in_specs = (tok_spec,) * 9 + (dense_spec, dense_spec, expert_spec, expert_spec, expert_spec)
    out_specs = (tok_spec, tok_spec, expert_spec, expert_spec, expert_spec)
    return jax.shard_map(device_step, mesh=mesh, in_specs=in_specs, out_specs=out_specs, check_vma=False)
```

```python
import functools

import jax
import jax.numpy as jnp
from jax import lax
from jax.experimental import pallas as pl
from jax.experimental.pallas import tpu as pltpu
from jax.sharding import PartitionSpec as P

NORM_EPS = 1e-6
CHUNK = 16
BLOCK = 64
UNROLL = 4
ROW_TILE = 1024
COMB_TILE = 512
BIG_TILE = 512
SMALL_TILE = 256
VMEM_BYTES = 66_500_000
BF16 = jnp.bfloat16
F32 = jnp.float32


def rms_norm(values):
    return values * lax.rsqrt(jnp.mean(values * values, axis=-1, keepdims=True) + NORM_EPS)


def silu_grad(values):
    sigmoid_vals = jax.nn.sigmoid(values)
    return sigmoid_vals * (1.0 + values * (1.0 - sigmoid_vals))


def dot_nn(lhs, rhs):
    return jnp.dot(lhs, rhs, preferred_element_type=F32)


def dot_nt(lhs, rhs):
    return lax.dot_general(lhs, rhs, (((1,), (1,)), ((), ())), preferred_element_type=F32)


def dot_tn(lhs, rhs):
    return lax.dot_general(lhs, rhs, (((0,), (0,)), ((), ())), preferred_element_type=F32)


def rows_at(index, count):
    return pl.ds(pl.multiple_of(index, CHUNK), count)


def fill_onehot(hot_ref, rep, pos_ref, gate_ref, chunks_ref, src, n_local):
    tok_rows = pos_ref.shape[2]
    iota = lax.broadcasted_iota(jnp.int32, (CHUNK, tok_rows), 0).astype(F32).astype(BF16)
    ones = jnp.ones((CHUNK, tok_rows), BF16)
    for expert in range(n_local):
        rep[0, expert] = jnp.broadcast_to(pos_ref[0, expert:expert + 1, :], (CHUNK, tok_rows)).astype(BF16)
        if gate_ref is not None:
            rep[1, expert] = jnp.broadcast_to(gate_ref[0, expert:expert + 1, :], (CHUNK, tok_rows)).astype(BF16)

    def one(expert, start):
        n_chunks = chunks_ref[src, expert]

        def block(first):
            pos_rows = rep[0, expert]
            value = ones if gate_ref is None else rep[1, expert]
            for c in range(first, first + BLOCK // CHUNK):
                hot = jnp.where(iota + jnp.bfloat16(c * CHUNK) == pos_rows, value, jnp.zeros_like(value))
                hot_ref[rows_at(start + c * CHUNK, CHUNK), :] = hot

        block(0)
        pl.when(n_chunks > BLOCK // CHUNK)(functools.partial(block, BLOCK // CHUNK))
        return start + n_chunks * CHUNK

    return expert_loop(n_local, one)


def expert_loop(n_local, one):
    def body(group, start):
        for i in range(UNROLL):
            start = one(group * UNROLL + i, start)
        return start

    return lax.fori_loop(0, n_local // UNROLL, body, jnp.int32(0))


def zero_tail(ref, offset, length, tile):
    n_tiles = (length + tile - 1) // tile

    def body(c, carry):
        ref[rows_at(offset + c * CHUNK, CHUNK), :] = jnp.zeros((CHUNK, ref.shape[1]), ref.dtype)
        return carry

    lax.fori_loop(length // CHUNK, n_tiles * (tile // CHUNK), body, 0)


def move_segments(pack_ref, wide_ref, base_ref, chunks_ref, src, n_local, cap, to_wide):
    def one(expert, start):
        n_chunks = chunks_ref[src, expert]
        base = expert * cap + base_ref[src, expert]

        def block(first):
            pack_rows = rows_at(start + first, BLOCK)
            wide_rows = rows_at(base + first, BLOCK)
            if to_wide:
                wide_ref[wide_rows, :] = pack_ref[pack_rows, :]
            else:
                pack_ref[pack_rows, :] = wide_ref[wide_rows, :]

        block(0)
        pl.when(n_chunks > BLOCK // CHUNK)(functools.partial(block, BLOCK))
        return start + n_chunks * CHUNK

    expert_loop(n_local, one)


def expert_bases(base_ref, total_ref, chunks_ref, n_src, n_local):
    for expert in range(n_local):
        total_ref[expert] = 0

    def body(src, carry):
        for expert in range(n_local):
            base_ref[src, expert] = total_ref[expert]
            total_ref[expert] = total_ref[expert] + chunks_ref[src, expert] * CHUNK
        return carry

    lax.fori_loop(0, n_src, body, 0)


def dispatch(pack_ref, hot_ref, table_ref, columns, wide_ref, base_ref, chunks_ref, src, n_local, cap, length):
    def step(rows):
        pack_ref[rows, :] = dot_nn(hot_ref[rows, :], table_ref[:, columns]).astype(BF16)

    tiled_rows(0, length, step, ROW_TILE, SMALL_TILE)
    move_segments(pack_ref, wide_ref, base_ref, chunks_ref, src, n_local, cap, True)


def combine(out_ref, pack_ref, hot_ref, wide_ref, base_ref, chunks_ref, src, n_local, cap, length):
    move_segments(pack_ref, wide_ref, base_ref, chunks_ref, src, n_local, cap, False)
    zero_tail(pack_ref, 0, length, COMB_TILE)
    zero_tail(hot_ref, 0, length, COMB_TILE)
    out_ref[...] = jnp.zeros_like(out_ref)

    def step(rows):
        out_ref[...] += dot_tn(hot_ref[rows, :], pack_ref[rows, :])

    tiled_rows(0, length, step, ROW_TILE, COMB_TILE)


def tiled_rows(first, count, step, big_tile, small_tile):
    n_small = (count + small_tile - 1) // small_tile
    per_big = big_tile // small_tile
    n_big = n_small // per_big

    def big(tile, carry):
        step(rows_at(first + tile * big_tile, big_tile))
        return carry

    lax.fori_loop(0, n_big, big, 0)
    for left in range(1, per_big):
        pl.when(n_small - n_big * per_big == left)(
            functools.partial(step, rows_at(first + n_big * big_tile, left * small_tile)))


def weight_copies(expert, slot, wg_ref, wu_ref, wd_ref, gu_buf, dn_buf, sems):
    ff = wg_ref.shape[2]
    return (
        pltpu.make_async_copy(wg_ref.at[expert], gu_buf.at[slot, :, pl.ds(0, ff)], sems.at[slot, 0]),
        pltpu.make_async_copy(wu_ref.at[expert], gu_buf.at[slot, :, pl.ds(ff, ff)], sems.at[slot, 1]),
        pltpu.make_async_copy(wd_ref.at[expert], dn_buf.at[slot], sems.at[slot, 2]),
    )


def next_weights(expert, n_local, *refs):
    slot = lax.rem(expert, 2)

    @pl.when(expert + 1 < n_local)
    def _():
        for copy in weight_copies(expert + 1, lax.rem(expert + 1, 2), *refs):
            copy.start()

    for copy in weight_copies(expert, slot, *refs):
        copy.wait()
    return slot


def forward_kernel(n_src, n_local, cap, chunks_ref, tok_ref, pos_ref, gate_ref, wg_ref, wu_ref, wd_ref, out_ref,
                   wide, hot, rep, pack, gu_buf, dn_buf, base, total, sems):
    step = pl.program_id(0)
    hidden, ff = wg_ref.shape[1:]
    w_refs = (wg_ref, wu_ref, wd_ref, gu_buf, dn_buf, sems)

    @pl.when(step == 0)
    def _():
        for copy in weight_copies(0, 0, *w_refs):
            copy.start()
        expert_bases(base, total, chunks_ref, n_src, n_local)

    @pl.when(step < n_src)
    def _():
        length = fill_onehot(hot, rep, pos_ref, None, chunks_ref, step, n_local)
        dispatch(pack, hot, tok_ref, pl.ds(0, hidden), wide, base, chunks_ref, step, n_local, cap, length)

    @pl.when((step >= n_src) & (step < n_src + n_local))
    def _():
        expert = step - n_src
        slot = next_weights(expert, n_local, *w_refs)

        def rows_step(rows):
            pre = dot_nn(wide[rows, :], gu_buf[slot])
            gate = pre[:, :ff]
            act = (gate * jax.nn.sigmoid(gate) * pre[:, ff:]).astype(BF16)
            wide[rows, :] = dot_nn(act, dn_buf[slot]).astype(BF16)

        tiled_rows(expert * cap, total[expert], rows_step, BIG_TILE, SMALL_TILE)

    @pl.when(step >= n_src + n_local)
    def _():
        src = step - n_src - n_local
        length = fill_onehot(hot, rep, pos_ref, gate_ref, chunks_ref, src, n_local)
        combine(out_ref, pack, hot, wide, base, chunks_ref, src, n_local, cap, length)


def backward_kernel(n_src, n_local, cap, chunks_ref, tok_ref, pos_ref, gate_ref, wg_ref, wu_ref, wd_ref,
                    out_ref, dwg_ref, dwu_ref, dwd_ref,
                    wide_x, wide_q, hot, rep, pack, gu_buf, dn_buf, base, total, sems):
    step = pl.program_id(0)
    hidden, ff = wg_ref.shape[1:]
    w_refs = (wg_ref, wu_ref, wd_ref, gu_buf, dn_buf, sems)

    @pl.when(step == 0)
    def _():
        for copy in weight_copies(0, 0, *w_refs):
            copy.start()
        expert_bases(base, total, chunks_ref, n_src, n_local)

    @pl.when(step < n_src)
    def _():
        length = fill_onehot(hot, rep, pos_ref, None, chunks_ref, step, n_local)
        dispatch(pack, hot, tok_ref, pl.ds(0, hidden), wide_x, base, chunks_ref, step, n_local, cap, length)
        fill_onehot(hot, rep, pos_ref, gate_ref, chunks_ref, step, n_local)
        dispatch(pack, hot, tok_ref, pl.ds(hidden, hidden), wide_q, base, chunks_ref, step, n_local, cap, length)

    @pl.when((step >= n_src) & (step < n_src + n_local))
    def _():
        expert = step - n_src
        slot = next_weights(expert, n_local, *w_refs)
        zero_tail(wide_x, expert * cap, total[expert], SMALL_TILE)
        zero_tail(wide_q, expert * cap, total[expert], SMALL_TILE)
        dwg_ref[...] = jnp.zeros_like(dwg_ref)
        dwu_ref[...] = jnp.zeros_like(dwu_ref)
        dwd_ref[...] = jnp.zeros_like(dwd_ref)

        def rows_step(rows):
            x_rows = wide_x[rows, :]
            q_rows = wide_q[rows, :]
            pre = dot_nn(x_rows, gu_buf[slot])
            gate, up = pre[:, :ff], pre[:, ff:]
            sig = jax.nn.sigmoid(gate)
            silu = gate * sig
            act = (silu * up).astype(BF16)
            grad_act = dot_nt(q_rows, dn_buf[slot]).astype(BF16).astype(F32)
            grad_gate = (grad_act * up * (sig * (1.0 + gate * (1.0 - sig)))).astype(BF16)
            grad_up = (grad_act * silu).astype(BF16)
            grad_pre = jnp.concatenate([grad_gate, grad_up], axis=1)
            dwd_ref[0] += dot_tn(act, q_rows)
            dw_pre = dot_tn(x_rows, grad_pre)
            dwg_ref[0] += dw_pre[:, :ff]
            dwu_ref[0] += dw_pre[:, ff:]
            wide_x[rows, :] = dot_nt(grad_pre, gu_buf[slot]).astype(BF16)

        tiled_rows(expert * cap, total[expert], rows_step, BIG_TILE, SMALL_TILE)

    @pl.when(step >= n_src + n_local)
    def _():
        src = step - n_src - n_local
        length = fill_onehot(hot, rep, pos_ref, None, chunks_ref, src, n_local)
        combine(out_ref, pack, hot, wide_x, base, chunks_ref, src, n_local, cap, length)


def expert_call(backward, chunks, table, pos, gate, w_gate, w_up, w_down):
    n_src, n_local, tok_rows = pos.shape
    hidden, ff = w_gate.shape[1:]
    cap = n_src * 128 + BLOCK
    pack_rows = n_local * 128 + BLOCK
    steps = 2 * n_src + n_local

    def src_in(i, *_):
        return (jnp.minimum(i, n_src - 1), 0)

    def src_out(i, *_):
        return (jnp.clip(i - n_src - n_local, 0, n_src - 1), 0)

    def weight_out(i, *_):
        return (jnp.clip(i - n_src, 0, n_local - 1), 0, 0)

    table_spec = pl.BlockSpec((tok_rows, table.shape[1]), src_in)

    def route_in(i, *_):
        return (jnp.where(i < n_src, i, jnp.clip(i - n_src - n_local, 0, n_src - 1)), 0, 0)

    route_spec = pl.BlockSpec((1,) + pos.shape[1:], route_in)
    raw = pl.BlockSpec(memory_space=pl.ANY)
    out_shape = [jax.ShapeDtypeStruct((n_src * tok_rows, hidden), F32)]
    out_specs = [pl.BlockSpec((tok_rows, hidden), src_out)]
    wide = pltpu.VMEM((n_local * cap, hidden), BF16)
    scratch = [wide]
    if backward:
        out_shape += [jax.ShapeDtypeStruct(w.shape, F32) for w in (w_gate, w_up, w_down)]
        out_specs += [pl.BlockSpec((1,) + w.shape[1:], weight_out) for w in (w_gate, w_up, w_down)]
        scratch += [wide]
    scratch += [
        pltpu.VMEM((pack_rows, tok_rows), BF16),
        pltpu.VMEM((2, n_local, CHUNK, tok_rows), BF16),
        pltpu.VMEM((pack_rows, hidden), BF16),
        pltpu.VMEM((2, hidden, 2 * ff), BF16),
        pltpu.VMEM((2, ff, hidden), BF16),
        pltpu.SMEM((n_src, n_local), jnp.int32),
        pltpu.SMEM((n_local,), jnp.int32),
        pltpu.SemaphoreType.DMA((2, 3)),
    ]
    body = backward_kernel if backward else forward_kernel
    flops = (100 if backward else 60) * 10 ** 9
    return pl.pallas_call(
        functools.partial(body, n_src, n_local, cap),
        grid_spec=pltpu.PrefetchScalarGridSpec(
            num_scalar_prefetch=1,
            grid=(steps,),
            in_specs=[table_spec] + [route_spec, route_spec, raw, raw, raw],
            out_specs=out_specs,
            scratch_shapes=scratch,
        ),
        out_shape=out_shape,
        compiler_params=pltpu.CompilerParams(dimension_semantics=("arbitrary",), vmem_limit_bytes=VMEM_BYTES),
        cost_estimate=pl.CostEstimate(flops=flops, bytes_accessed=60 * 10 ** 6, transcendentals=0),
        name="expert_backward" if backward else "expert_forward",
    )(chunks, table, pos, gate, w_gate, w_up, w_down)


def reduce_tail_kernel(part_ref, h_ref, x_ref, grad_ref, pre_ref, w1_ref, w2_ref, out_ref,
                       sums, core_in, x_in, y_in, x_last, y_last, dx_buf, h_buf, x_buf, grad_buf, pre_buf, w1_buf, w2_buf,
                       load_sem, row_sem, weight_sem, core_send, core_recv, hop_send, hop_recv, last_send, last_recv, dx_send, dx_recv):
    n_chunks, half = x_in.shape[0], x_in.shape[2]
    chunk = 2 * half
    tok_rows = n_chunks * chunk
    me = lax.axis_index("ep")
    core, x_pos, y_pos = lax.rem(me, 2), lax.rem(me // 2, 2), me // 4
    x_step, y_step = 2 - 4 * x_pos, 4 - 8 * y_pos
    partner = me + 1 - 2 * core
    x_peer, y_peer = me + x_step, me + y_step
    pp_peer = 1 - lax.axis_index("pp")
    offsets = (0, x_step, y_step, x_step + y_step)
    mesh_id = pl.DeviceIdType.MESH

    barrier = pltpu.get_barrier_semaphore()
    for peer in ({"ep": partner}, {"ep": x_peer}, {"ep": y_peer}, {"pp": pp_peer}):
        pl.semaphore_signal(barrier, inc=1, device_id=peer, device_id_type=mesh_id)
    pl.semaphore_wait(barrier, 4)

    def part_rows(dest, k):
        return part_ref.at[pl.ds(pl.multiple_of(dest * tok_rows + k * chunk, chunk), chunk)]

    def core_copy(k, i):
        return pltpu.make_async_remote_copy(part_rows(partner + offsets[i], k), core_in.at[k, i], core_send.at[k, i], core_recv.at[k, i],
                                            device_id={"ep": partner}, device_id_type=mesh_id)

    def load_copy(k, i):
        return pltpu.make_async_copy(part_rows(me + offsets[i], k), sums.at[k, i], load_sem.at[k, i])

    def hop_copies(k):
        top, low = pl.ds(0, half), pl.ds(half, half)
        return [
            pltpu.make_async_remote_copy(sums.at[k, i, rows], land.at[k, j], hop_send.at[k, n], hop_recv.at[k, n],
                                         device_id={"ep": peer}, device_id_type=mesh_id)
            for n, (i, rows, land, j, peer) in enumerate((
                (3, top, x_in, 1, x_peer), (3, low, y_in, 1, y_peer), (1, top, x_in, 0, x_peer), (2, low, y_in, 0, y_peer)))
        ]

    def last_copies(k):
        top, low = pl.ds(0, half), pl.ds(half, half)
        return [
            pltpu.make_async_remote_copy(sums.at[k, 2, top], y_last.at[k], last_send.at[k, 0], last_recv.at[k, 0],
                                         device_id={"ep": y_peer}, device_id_type=mesh_id),
            pltpu.make_async_remote_copy(sums.at[k, 1, low], x_last.at[k], last_send.at[k, 1], last_recv.at[k, 1],
                                         device_id={"ep": x_peer}, device_id_type=mesh_id),
        ]

    def chunk_rows(k):
        return pl.ds(pl.multiple_of(k * chunk, chunk), chunk)

    def row_copies(k):
        return [pltpu.make_async_copy(src.at[chunk_rows(k)], buf.at[chunk_rows(k)], row_sem.at[k, n])
                for n, (src, buf) in enumerate(((h_ref, h_buf), (x_ref, x_buf), (grad_ref, grad_buf), (pre_ref, pre_buf)))]

    def weight_loads():
        return [pltpu.make_async_copy(w1_ref, w1_buf, weight_sem.at[0]), pltpu.make_async_copy(w2_ref, w2_buf, weight_sem.at[1])]

    def dx_copy(k):
        return pltpu.make_async_remote_copy(dx_buf.at[chunk_rows(k)], out_ref.at[chunk_rows(k)], dx_send.at[k], dx_recv.at[k],
                                            device_id={"pp": pp_peer}, device_id_type=mesh_id)

    def start_chunk(k, carry):
        for i in (3, 1, 2, 0):
            core_copy(k, i).start()
            load_copy(k, i).start()
        return carry

    lax.fori_loop(0, n_chunks, start_chunk, 0)

    def add_cores(k, carry):
        hops = hop_copies(k)
        for i, ready in ((3, (0, 1)), (1, (2,)), (2, (3,)), (0, ())):
            load_copy(k, i).wait()
            core_copy(k, i).wait_recv()
            sums[k, i] = sums[k, i] + core_in[k, i]
            for n in ready:
                hops[n].start()
        return carry

    lax.fori_loop(0, n_chunks, add_cores, 0)

    for copy in weight_loads():
        copy.start()

    def start_rows(k, carry):
        for copy in row_copies(k):
            copy.start()
        return carry

    lax.fori_loop(0, n_chunks, start_rows, 0)

    def relay(k, carry):
        hops, lasts = hop_copies(k), last_copies(k)
        hops[0].wait_recv()
        sums[k, 2, :half] = sums[k, 2, :half] + x_in[k, 1]
        lasts[0].start()
        hops[1].wait_recv()
        sums[k, 1, half:] = sums[k, 1, half:] + y_in[k, 1]
        lasts[1].start()
        return carry

    lax.fori_loop(0, n_chunks, relay, 0)

    for copy in weight_loads():
        copy.wait()

    def norm_grad(values, grads):
        scale = lax.rsqrt(jnp.mean(values * values, axis=-1, keepdims=True) + NORM_EPS)
        return scale * grads - values * (scale * scale * scale * jnp.mean(grads * values, axis=-1, keepdims=True))

    def finish(k, carry):
        rows = chunk_rows(k)
        hops, lasts = hop_copies(k), last_copies(k)
        for copy in row_copies(k):
            copy.wait()
        for copy in hops[2:]:
            copy.wait_recv()
        for copy in lasts:
            copy.wait_recv()
        sums[k, 0, :half] = sums[k, 0, :half] + x_in[k, 0] + y_last[k]
        sums[k, 0, half:] = sums[k, 0, half:] + y_in[k, 0] + x_last[k]
        grad_h = grad_buf[rows, :].astype(F32) + norm_grad(h_buf[rows, :].astype(F32), sums[k, 0])
        grad_act = dot_nt(grad_h.astype(BF16), w2_buf[...])
        grad_pre = (grad_act * silu_grad(pre_buf[rows, :])).astype(BF16)
        grad_norm = dot_nt(grad_pre, w1_buf[...])
        dx_buf[rows, :] = (grad_h + norm_grad(x_buf[rows, :].astype(F32), grad_norm)).astype(BF16)
        dx_copy(k).start()
        return carry

    lax.fori_loop(0, n_chunks, finish, 0)

    def drain(k, carry):
        for i in range(4):
            core_copy(k, i).wait_send()
        for copy in hop_copies(k) + last_copies(k):
            copy.wait_send()
        dx_copy(k).wait()
        return carry

    lax.fori_loop(0, n_chunks, drain, 0)


def reduce_tail(part, h_rows, x_rows, grad_rows, hidden_pre, w_one, w_two):
    tok_rows, hidden = x_rows.shape
    ff = w_one.shape[1]
    n_chunks = 4
    half = tok_rows // (2 * n_chunks)
    raw = pl.BlockSpec(memory_space=pl.ANY)
    dma = pltpu.SemaphoreType.DMA
    rows_buf = pltpu.VMEM((tok_rows, hidden), BF16)
    return pl.pallas_call(
        reduce_tail_kernel,
        out_shape=jax.ShapeDtypeStruct((tok_rows, hidden), BF16),
        in_specs=[raw] * 7,
        out_specs=raw,
        scratch_shapes=[
            pltpu.VMEM((n_chunks, 4, 2 * half, hidden), F32),
            pltpu.VMEM((n_chunks, 4, 2 * half, hidden), F32),
            pltpu.VMEM((n_chunks, 2, half, hidden), F32),
            pltpu.VMEM((n_chunks, 2, half, hidden), F32),
            pltpu.VMEM((n_chunks, half, hidden), F32),
            pltpu.VMEM((n_chunks, half, hidden), F32),
            rows_buf, rows_buf, rows_buf, rows_buf,
            pltpu.VMEM((tok_rows, ff), F32),
            pltpu.VMEM(w_one.shape, BF16),
            pltpu.VMEM(w_two.shape, BF16),
            dma((n_chunks, 4)), dma((n_chunks, 4)), dma((2,)),
            dma((n_chunks, 4)), dma((n_chunks, 4)), dma((n_chunks, 4)), dma((n_chunks, 4)),
            dma((n_chunks, 2)), dma((n_chunks, 2)), dma((n_chunks,)), dma((n_chunks,)),
        ],
        compiler_params=pltpu.CompilerParams(collective_id=0, has_side_effects=True, vmem_limit_bytes=VMEM_BYTES),
        cost_estimate=pl.CostEstimate(flops=60 * 10 ** 9, bytes_accessed=40 * 10 ** 6, transcendentals=0),
        name="reduce_tail",
    )(part, h_rows, x_rows, grad_rows, hidden_pre, w_one, w_two)


def head_kernel(x_ref, saved_ref, grad_ref, w1_ref, w2_ref, routes_ref,
                all_ref, h_ref, saved_h_ref, pre_ref, pair_ref, pos_f_ref, gate_f_ref, pos_b_ref, gate_b_ref, count_ref,
                normed, pre_buf, routes, kept, own_sem, pre_sem, first_send, first_recv, hop_send, hop_recv, core_send, core_recv):
    tok_rows = x_ref.shape[0]
    n_chunks = first_send.shape[0] - 1
    n_src = routes.shape[0]
    n_local = kept.shape[0] // (2 * n_src)
    top_k = routes_ref.shape[0] // 4
    chunk = tok_rows // n_chunks
    me = lax.axis_index("ep")
    core, x_pos, y_pos = lax.rem(me, 2), lax.rem(me // 2, 2), me // 4
    x_step, y_step = 2 - 4 * x_pos, 4 - 8 * y_pos
    partner = me + 1 - 2 * core
    x_peer, y_peer, far_peer = me + x_step, me + y_step, me + x_step + y_step
    mesh_id = pl.DeviceIdType.MESH

    barrier = pltpu.get_barrier_semaphore()
    for peer in (partner, x_peer, y_peer):
        pl.semaphore_signal(barrier, inc=1, device_id={"ep": peer}, device_id_type=mesh_id)
    pl.semaphore_wait(barrier, 3)

    def chunk_rows(c):
        return pl.ds(pl.multiple_of(c * chunk, chunk), chunk)

    def view(c, src, part):
        if isinstance(c, int) and c == n_chunks:
            size = routes.shape[1] // 2
            return routes.at[src] if part is None else routes.at[src, pl.ds(part * size, size)]
        first = src * tok_rows + c * chunk
        if part is None:
            return all_ref.at[pl.ds(pl.multiple_of(first, chunk), chunk)]
        return all_ref.at[pl.ds(pl.multiple_of(first + part * (chunk // 2), chunk // 2), chunk // 2)]

    def remote(src, dst, send, recv, peer):
        return pltpu.make_async_remote_copy(src, dst, send, recv, device_id={"ep": peer}, device_id_type=mesh_id)

    def first_copy(c, n):
        own = routes_ref if isinstance(c, int) and c == n_chunks else normed.at[chunk_rows(c)]
        return remote(own, view(c, me, None), first_send.at[c, n], first_recv.at[c, n], (partner, x_peer, y_peer)[n])

    def hop_copy(c, n):
        piece = view(c, (x_peer, y_peer)[n], n)
        return remote(piece, piece, hop_send.at[c, n], hop_recv.at[c, n], (y_peer, x_peer)[n])

    def core_copy(c, n):
        piece = view(c, *((x_peer, None), (y_peer, None), (far_peer, 0), (far_peer, 1))[n])
        return remote(piece, piece, core_send.at[c, n], core_recv.at[c, n], partner)

    def own_copy(c):
        return pltpu.make_async_copy(normed.at[chunk_rows(c)], view(c, me, None), own_sem.at[c])

    def pass_on(c):
        for n in range(2):
            first_copy(c, n + 1).wait_recv()
            hop_copy(c, n).start()
            core_copy(c, n).start()

    def pass_far(c):
        for n in range(2):
            hop_copy(c, n).wait_recv()
            core_copy(c, n + 2).start()

    def arrive(c):
        first_copy(c, 0).wait_recv()
        for n in range(4):
            core_copy(c, n).wait_recv()

    def drain(c):
        for n in range(3):
            first_copy(c, n).wait_send()
        for n in range(2):
            hop_copy(c, n).wait_send()
        for n in range(4):
            core_copy(c, n).wait_send()

    def dense_rows(x_rows):
        pre = dot_nn(rms_norm(x_rows).astype(BF16), w1_ref[...])
        act = (pre * jax.nn.sigmoid(pre)).astype(BF16)
        hidden = (x_rows + dot_nn(act, w2_ref[...])).astype(BF16)
        return pre, hidden, rms_norm(hidden.astype(F32)).astype(BF16)

    def dense(c):
        rows = chunk_rows(c)
        _, h_ref[rows, :], normed[rows, :] = dense_rows(x_ref[rows, :].astype(F32))

    def pre_copy(c):
        return pltpu.make_async_copy(pre_buf.at[chunk_rows(c)], pre_ref.at[chunk_rows(c)], pre_sem.at[c])

    def dense_saved(c):
        rows = chunk_rows(c)
        width = grad_ref.shape[1]
        pre_buf[rows, :], saved_h_ref[rows, :], pair_ref[rows, :width] = dense_rows(saved_ref[rows, :].astype(F32))
        pair_ref[rows, width:] = grad_ref[rows, :]
        pre_copy(c).start()

    def send(c):
        for n in (1, 2, 0):
            first_copy(c, n).start()
        own_copy(c).start()

    def tables(src):
        pieces = [routes[src, pl.ds(i * top_k, top_k), :].astype(F32) for i in range(4)] if top_k % CHUNK == 0 else None
        whole = routes[src].astype(F32) if pieces is None else None
        if pieces is None:
            pieces = [whole[i * top_k:(i + 1) * top_k] for i in range(4)]
        lines = lax.broadcasted_iota(jnp.int32, (n_local, tok_rows), 0)

        def body(expert, carry):
            wanted = (me * n_local + expert).astype(F32)
            out = []
            for batch in range(2):
                match = pieces[2 * batch] == wanted
                here = lines == expert
                hit = jnp.max(jnp.where(match, 1.0, 0.0), axis=0, keepdims=True)
                gate = jnp.sum(jnp.where(match, pieces[2 * batch + 1], 0.0), axis=0, keepdims=True)
                out += [jnp.where(here, hit, carry[2 * batch]), jnp.where(here, gate, carry[2 * batch + 1])]
            return tuple(out)

        zero = jnp.zeros((n_local, tok_rows), F32)
        hit_f, gate_f, hit_b, gate_b = lax.fori_loop(0, n_local, body, (zero,) * 4)
        rows = pl.ds(pl.multiple_of(src * n_local, n_local), n_local)
        low_rows = pl.ds(pl.multiple_of((n_src + src) * n_local, n_local), n_local)
        gate_f_ref[rows, :] = gate_f
        gate_b_ref[rows, :] = gate_b
        kept[rows, :] = hit_f.astype(BF16)
        kept[low_rows, :] = hit_b.astype(BF16)

    def ranks():
        width = 256
        hits = kept[...]
        half = n_src * n_local
        for first in range(0, tok_rows, width):
            upto = lax.broadcasted_iota(jnp.int32, (tok_rows, width), 1) + first
            upper = jnp.where(lax.broadcasted_iota(jnp.int32, (tok_rows, width), 0) <= upto, 1.0, 0.0).astype(BF16)
            rank = dot_nn(hits, upper)
            pos = jnp.where(kept[:, first:first + width].astype(F32) > 0.0, rank - 1.0, -1.0)
            pos_f_ref[:, first:first + width] = pos[:half]
            pos_b_ref[:, first:first + width] = pos[half:]
            if first + width == tok_rows:
                count_ref[...] = rank[:, width - 128:]

    routes[me] = routes_ref[...]
    for n in (1, 2, 0):
        first_copy(n_chunks, n).start()
    dense(0)
    pass_on(n_chunks)
    send(0)

    def dense_send(c, carry):
        dense(c)
        send(c)
        return carry

    lax.fori_loop(1, n_chunks, dense_send, 0)
    pass_far(n_chunks)
    arrive(n_chunks)

    def forward(c, carry):
        pass_on(c)
        for i in range(n_src // n_chunks):
            tables(c * (n_src // n_chunks) + i)
        dense_saved(c)
        return carry

    lax.fori_loop(0, n_chunks, forward, 0)

    def far(c, carry):
        pass_far(c)
        return carry

    lax.fori_loop(0, n_chunks - 1, far, 0)
    ranks()
    lax.fori_loop(n_chunks - 1, n_chunks, far, 0)

    def finish(c, carry):
        arrive(c)
        own_copy(c).wait()
        pre_copy(c).wait()
        drain(c)
        return carry

    lax.fori_loop(0, n_chunks, finish, 0)
    drain(n_chunks)


def head(x_rows, saved_rows, grad_rows, w_one, w_two, routes, n_src, n_local):
    tok_rows, hidden = x_rows.shape
    ff = w_one.shape[1]
    n_chunks = 4
    dma = pltpu.SemaphoreType.DMA
    vmem = pl.BlockSpec(memory_space=pltpu.VMEM)
    raw = pl.BlockSpec(memory_space=pl.ANY)
    table = jax.ShapeDtypeStruct((n_src * n_local, tok_rows), F32)
    return pl.pallas_call(
        head_kernel,
        out_shape=[
            jax.ShapeDtypeStruct((n_src * tok_rows, hidden), BF16), jax.ShapeDtypeStruct((tok_rows, hidden), BF16),
            jax.ShapeDtypeStruct((tok_rows, hidden), BF16), jax.ShapeDtypeStruct((tok_rows, ff), F32),
            jax.ShapeDtypeStruct((tok_rows, 2 * hidden), BF16),
            table, table, table, table, jax.ShapeDtypeStruct((2 * n_src * n_local, 128), F32),
        ],
        in_specs=[vmem] * 6,
        out_specs=[raw, vmem, vmem, raw] + [vmem] * 6,
        scratch_shapes=[
            pltpu.VMEM((tok_rows, hidden), BF16),
            pltpu.VMEM((tok_rows, ff), F32),
            pltpu.VMEM((n_src,) + routes.shape, BF16),
            pltpu.VMEM((2 * n_src * n_local, tok_rows), BF16),
            dma((n_chunks,)), dma((n_chunks,)),
            dma((n_chunks + 1, 3)), dma((n_chunks + 1, 3)),
            dma((n_chunks + 1, 2)), dma((n_chunks + 1, 2)),
            dma((n_chunks + 1, 4)), dma((n_chunks + 1, 4)),
        ],
        compiler_params=pltpu.CompilerParams(collective_id=1, has_side_effects=True, vmem_limit_bytes=VMEM_BYTES),
        cost_estimate=pl.CostEstimate(flops=30 * 10 ** 9, bytes_accessed=20 * 10 ** 6, transcendentals=0),
        name="head",
    )(x_rows, saved_rows, grad_rows, w_one, w_two, routes)


def solution(mesh):
    stages = mesh.shape["pp"]
    ep_size = mesh.shape["ep"]
    next_perm = [(stage_idx, (stage_idx + 1) % stages) for stage_idx in range(stages)]
    assert (stages, ep_size) == (2, 8)
    tok_spec = P("pp", "ep", None)
    dense_spec = P("pp", None, None)
    expert_spec = P("pp", "ep", None, None)

    def device_step(x_fwd, ids_fwd, slots_fwd, gates_fwd, x_saved, grad_in, ids_bwd, slots_bwd, gates_bwd, w_one, w_two, w_gate, w_up, w_down):
        x_fwd, ids_fwd, slots_fwd, gates_fwd = x_fwd[0], ids_fwd[0], slots_fwd[0], gates_fwd[0]
        x_saved, grad_in, ids_bwd, slots_bwd, gates_bwd = x_saved[0], grad_in[0], ids_bwd[0], slots_bwd[0], gates_bwd[0]
        w_one, w_two, w_gate, w_up, w_down = w_one[0], w_two[0], w_gate[0], w_up[0], w_down[0]
        n_local = w_gate.shape[0]

        routes = jnp.concatenate([
            jnp.where(slots_fwd >= 0, ids_fwd, -1).astype(BF16), gates_fwd,
            jnp.where(slots_bwd >= 0, ids_bwd, -1).astype(BF16), gates_bwd,
        ], axis=1).T
        all_fwd, h_fwd, h_bwd, hidden_pre, pair, pos_f, gate_f, pos_b, gate_b, counts = head(
            x_fwd, x_saved, grad_in, w_one, w_two, routes, ep_size, n_local)
        all_bwd = lax.all_gather(pair, "ep", axis=0, tiled=True)
        pos_f, gate_f, pos_b, gate_b = (t.reshape(ep_size, n_local, -1) for t in (pos_f, gate_f, pos_b, gate_b))
        chunks = (counts[:, -1].reshape(2, ep_size, n_local).astype(jnp.int32) + CHUNK - 1) // CHUNK
        chunks_f, chunks_b = chunks[0], chunks[1]

        (part_fwd,) = expert_call(False, chunks_f, all_fwd, pos_f, gate_f, w_gate, w_up, w_down)
        part_fwd, all_bwd = lax.optimization_barrier((part_fwd, all_bwd))
        mix_sum = lax.psum_scatter(part_fwd, "ep", scatter_dimension=0, tiled=True)
        y_out = (h_fwd.astype(F32) + mix_sum).astype(BF16)

        part_bwd, dw_gate, dw_up, dw_down = expert_call(True, chunks_b, all_bwd, pos_b, gate_b, w_gate, w_up, w_down)
        y_next = lax.ppermute(y_out, "pp", next_perm)
        dx_prev = reduce_tail(part_bwd, h_bwd, x_saved, grad_in, hidden_pre, w_one, w_two)
        return y_next[None], dx_prev[None], dw_gate[None], dw_up[None], dw_down[None]

    in_specs = (tok_spec,) * 9 + (dense_spec, dense_spec, expert_spec, expert_spec, expert_spec)
    out_specs = (tok_spec, tok_spec, expert_spec, expert_spec, expert_spec)
    return jax.shard_map(device_step, mesh=mesh, in_specs=in_specs, out_specs=out_specs, check_vma=False)
```

```python
import functools

import jax
import jax.numpy as jnp
from jax import lax
from jax.experimental import pallas as pl
from jax.experimental.pallas import tpu as pltpu
from jax.sharding import PartitionSpec as P

NORM_EPS = 1e-6
CHUNK = 16
BLOCK = 64
UNROLL = 8
ROW_TILE = 1024
COMB_TILE = 256
BIG_TILE = 1024
SMALL_TILE = 256
VMEM_BYTES = 66_500_000
BF16 = jnp.bfloat16
F32 = jnp.float32


def rms_norm(values):
    return values * lax.rsqrt(jnp.mean(values * values, axis=-1, keepdims=True) + NORM_EPS)


def silu_grad(values):
    sigmoid_vals = jax.nn.sigmoid(values)
    return sigmoid_vals * (1.0 + values * (1.0 - sigmoid_vals))


def dot_nn(lhs, rhs):
    return jnp.dot(lhs, rhs, preferred_element_type=F32)


def dot_nt(lhs, rhs):
    return lax.dot_general(lhs, rhs, (((1,), (1,)), ((), ())), preferred_element_type=F32)


def dot_tn(lhs, rhs):
    return lax.dot_general(lhs, rhs, (((0,), (0,)), ((), ())), preferred_element_type=F32)


def rows_at(index, count):
    return pl.ds(pl.multiple_of(index, CHUNK), count)


def fill_onehot(hot_ref, rep, pos_ref, gate_ref, chunks_ref, src, n_local):
    tok_rows = pos_ref.shape[2]
    iota = lax.broadcasted_iota(jnp.int32, (CHUNK, tok_rows), 0).astype(F32).astype(BF16)
    ones = jnp.ones((CHUNK, tok_rows), BF16)
    for expert in range(n_local):
        rep[0, expert] = jnp.broadcast_to(pos_ref[0, expert:expert + 1, :], (CHUNK, tok_rows)).astype(BF16)
        if gate_ref is not None:
            rep[1, expert] = jnp.broadcast_to(gate_ref[0, expert:expert + 1, :], (CHUNK, tok_rows)).astype(BF16)

    def one(expert, start):
        n_chunks = chunks_ref[src, expert]

        def block(first):
            pos_rows = rep[0, expert]
            value = ones if gate_ref is None else rep[1, expert]
            for c in range(first, first + BLOCK // CHUNK):
                hot = jnp.where(iota + jnp.bfloat16(c * CHUNK) == pos_rows, value, jnp.zeros_like(value))
                hot_ref[rows_at(start + c * CHUNK, CHUNK), :] = hot

        block(0)
        pl.when(n_chunks > BLOCK // CHUNK)(functools.partial(block, BLOCK // CHUNK))
        return start + n_chunks * CHUNK

    return expert_loop(n_local, one)


def expert_loop(n_local, one):
    def body(group, start):
        for i in range(UNROLL):
            start = one(group * UNROLL + i, start)
        return start

    return lax.fori_loop(0, n_local // UNROLL, body, jnp.int32(0))


def zero_tail(ref, offset, length, tile):
    n_tiles = (length + tile - 1) // tile

    def body(c, carry):
        ref[rows_at(offset + c * CHUNK, CHUNK), :] = jnp.zeros((CHUNK, ref.shape[1]), ref.dtype)
        return carry

    lax.fori_loop(length // CHUNK, n_tiles * (tile // CHUNK), body, 0)


def move_segments(pack_ref, wide_ref, base_ref, chunks_ref, src, n_local, cap, to_wide):
    def one(expert, start):
        n_chunks = chunks_ref[src, expert]
        base = expert * cap + base_ref[src, expert]

        def block(first):
            pack_rows = rows_at(start + first, BLOCK)
            wide_rows = rows_at(base + first, BLOCK)
            if to_wide:
                wide_ref[wide_rows, :] = pack_ref[pack_rows, :]
            else:
                pack_ref[pack_rows, :] = wide_ref[wide_rows, :]

        block(0)
        pl.when(n_chunks > BLOCK // CHUNK)(functools.partial(block, BLOCK))
        return start + n_chunks * CHUNK

    expert_loop(n_local, one)


def expert_bases(base_ref, total_ref, chunks_ref, n_src, n_local):
    for expert in range(n_local):
        total_ref[expert] = 0

    def body(src, carry):
        for expert in range(n_local):
            base_ref[src, expert] = total_ref[expert]
            total_ref[expert] = total_ref[expert] + chunks_ref[src, expert] * CHUNK
        return carry

    lax.fori_loop(0, n_src, body, 0)


def dispatch(pack_ref, hot_ref, table_ref, columns, wide_ref, base_ref, chunks_ref, src, n_local, cap, length):
    def step(rows):
        pack_ref[rows, :] = dot_nn(hot_ref[rows, :], table_ref[:, columns]).astype(BF16)

    tiled_rows(0, length, step, ROW_TILE, SMALL_TILE)
    move_segments(pack_ref, wide_ref, base_ref, chunks_ref, src, n_local, cap, True)


def combine(out_ref, pack_ref, hot_ref, wide_ref, base_ref, chunks_ref, src, n_local, cap, length):
    move_segments(pack_ref, wide_ref, base_ref, chunks_ref, src, n_local, cap, False)
    zero_tail(pack_ref, 0, length, COMB_TILE)
    zero_tail(hot_ref, 0, length, COMB_TILE)
    out_ref[...] = jnp.zeros_like(out_ref)

    def step(rows):
        out_ref[...] += dot_tn(hot_ref[rows, :], pack_ref[rows, :])

    tiled_rows(0, length, step, ROW_TILE, COMB_TILE)


def tiled_rows(first, count, step, big_tile, small_tile):
    n_small = (count + small_tile - 1) // small_tile
    per_big = big_tile // small_tile
    n_big = n_small // per_big

    def big(tile, carry):
        step(rows_at(first + tile * big_tile, big_tile))
        return carry

    lax.fori_loop(0, n_big, big, 0)
    for left in range(1, per_big):
        pl.when(n_small - n_big * per_big == left)(
            functools.partial(step, rows_at(first + n_big * big_tile, left * small_tile)))


def weight_copies(expert, slot, wg_ref, wu_ref, wd_ref, gu_buf, dn_buf, sems):
    ff = wg_ref.shape[2]
    return (
        pltpu.make_async_copy(wg_ref.at[expert], gu_buf.at[slot, :, pl.ds(0, ff)], sems.at[slot, 0]),
        pltpu.make_async_copy(wu_ref.at[expert], gu_buf.at[slot, :, pl.ds(ff, ff)], sems.at[slot, 1]),
        pltpu.make_async_copy(wd_ref.at[expert], dn_buf.at[slot], sems.at[slot, 2]),
    )


def next_weights(expert, n_local, *refs):
    slot = lax.rem(expert, 2)

    @pl.when(expert + 1 < n_local)
    def _():
        for copy in weight_copies(expert + 1, lax.rem(expert + 1, 2), *refs):
            copy.start()

    for copy in weight_copies(expert, slot, *refs):
        copy.wait()
    return slot


def forward_kernel(n_src, n_local, cap, chunks_ref, tok_ref, pos_ref, gate_ref, wg_ref, wu_ref, wd_ref, out_ref,
                   wide, hot, rep, pack, gu_buf, dn_buf, base, total, sems):
    step = pl.program_id(0)
    hidden, ff = wg_ref.shape[1:]
    w_refs = (wg_ref, wu_ref, wd_ref, gu_buf, dn_buf, sems)

    @pl.when(step == 0)
    def _():
        for copy in weight_copies(0, 0, *w_refs):
            copy.start()
        expert_bases(base, total, chunks_ref, n_src, n_local)

    @pl.when(step < n_src)
    def _():
        length = fill_onehot(hot, rep, pos_ref, None, chunks_ref, step, n_local)
        dispatch(pack, hot, tok_ref, pl.ds(0, hidden), wide, base, chunks_ref, step, n_local, cap, length)

    @pl.when((step >= n_src) & (step < n_src + n_local))
    def _():
        expert = step - n_src
        slot = next_weights(expert, n_local, *w_refs)

        def rows_step(rows):
            pre = dot_nn(wide[rows, :], gu_buf[slot])
            gate = pre[:, :ff]
            act = (gate * jax.nn.sigmoid(gate) * pre[:, ff:]).astype(BF16)
            wide[rows, :] = dot_nn(act, dn_buf[slot]).astype(BF16)

        tiled_rows(expert * cap, total[expert], rows_step, BIG_TILE, SMALL_TILE)

    @pl.when(step >= n_src + n_local)
    def _():
        src = step - n_src - n_local
        length = fill_onehot(hot, rep, pos_ref, gate_ref, chunks_ref, src, n_local)
        combine(out_ref, pack, hot, wide, base, chunks_ref, src, n_local, cap, length)


def backward_kernel(n_src, n_local, cap, chunks_ref, tok_ref, pos_ref, gate_ref, wg_ref, wu_ref, wd_ref,
                    rows_ref, dwg_ref, dwu_ref, dwd_ref,
                    wide_x, wide_q, hot, rep, pack, gu_buf, dn_buf, base, total, sems):
    step = pl.program_id(0)
    hidden, ff = wg_ref.shape[1:]
    w_refs = (wg_ref, wu_ref, wd_ref, gu_buf, dn_buf, sems)

    @pl.when(step == 0)
    def _():
        for copy in weight_copies(0, 0, *w_refs):
            copy.start()
        expert_bases(base, total, chunks_ref, n_src, n_local)

    @pl.when(step < n_src)
    def _():
        length = fill_onehot(hot, rep, pos_ref, None, chunks_ref, step, n_local)
        dispatch(pack, hot, tok_ref, pl.ds(0, hidden), wide_x, base, chunks_ref, step, n_local, cap, length)
        fill_onehot(hot, rep, pos_ref, gate_ref, chunks_ref, step, n_local)
        dispatch(pack, hot, tok_ref, pl.ds(hidden, hidden), wide_q, base, chunks_ref, step, n_local, cap, length)

    @pl.when((step >= n_src) & (step < n_src + n_local))
    def _():
        expert = step - n_src
        slot = next_weights(expert, n_local, *w_refs)
        zero_tail(wide_x, expert * cap, total[expert], SMALL_TILE)
        zero_tail(wide_q, expert * cap, total[expert], SMALL_TILE)
        dwg_ref[...] = jnp.zeros_like(dwg_ref)
        dwu_ref[...] = jnp.zeros_like(dwu_ref)
        dwd_ref[...] = jnp.zeros_like(dwd_ref)

        def rows_step(rows):
            x_rows = wide_x[rows, :]
            q_rows = wide_q[rows, :]
            pre = dot_nn(x_rows, gu_buf[slot])
            gate, up = pre[:, :ff], pre[:, ff:]
            sig = jax.nn.sigmoid(gate)
            silu = gate * sig
            act = (silu * up).astype(BF16)
            grad_act = dot_nt(q_rows, dn_buf[slot]).astype(BF16).astype(F32)
            grad_gate = (grad_act * up * (sig * (1.0 + gate * (1.0 - sig)))).astype(BF16)
            grad_up = (grad_act * silu).astype(BF16)
            grad_pre = jnp.concatenate([grad_gate, grad_up], axis=1)
            dwd_ref[0] += dot_tn(act, q_rows)
            dw_pre = dot_tn(x_rows, grad_pre)
            dwg_ref[0] += dw_pre[:, :ff]
            dwu_ref[0] += dw_pre[:, ff:]
            rows_ref[0, rows_at(rows.start - expert * cap, rows.size), :] = dot_nt(grad_pre, gu_buf[slot]).astype(BF16)

        tiled_rows(expert * cap, total[expert], rows_step, BIG_TILE, SMALL_TILE)

        done = (total[expert] + SMALL_TILE - 1) // SMALL_TILE * (SMALL_TILE // CHUNK)
        end = jnp.minimum(total[expert] // CHUNK + 128 // CHUNK, cap // CHUNK)

        def clear(c, carry):
            rows_ref[0, rows_at(c * CHUNK, CHUNK), :] = jnp.zeros((CHUNK, hidden), BF16)
            return carry

        lax.fori_loop(done, jnp.maximum(done, end), clear, 0)


def expert_call(backward, chunks, table, pos, gate, w_gate, w_up, w_down):
    n_src, n_local, tok_rows = pos.shape
    hidden, ff = w_gate.shape[1:]
    cap = n_src * 128 + BLOCK
    pack_rows = n_local * 128 + BLOCK
    steps = n_src + n_local if backward else 2 * n_src + n_local

    def src_in(i, *_):
        return (jnp.minimum(i, n_src - 1), 0)

    def src_out(i, *_):
        return (jnp.clip(i - n_src - n_local, 0, n_src - 1), 0)

    def weight_out(i, *_):
        return (jnp.clip(i - n_src, 0, n_local - 1), 0, 0)

    table_spec = pl.BlockSpec((tok_rows, table.shape[1]), src_in)

    def route_in(i, *_):
        return (jnp.where(i < n_src, i, jnp.clip(i - n_src - n_local, 0, n_src - 1)), 0, 0)

    route_spec = pl.BlockSpec((1,) + pos.shape[1:], route_in)
    raw = pl.BlockSpec(memory_space=pl.ANY)
    out_shape = [jax.ShapeDtypeStruct((n_src * tok_rows, hidden), F32)]
    out_specs = [pl.BlockSpec((tok_rows, hidden), src_out)]
    wide = pltpu.VMEM((n_local * cap, hidden), BF16)
    scratch = [wide]
    if backward:
        out_shape = [jax.ShapeDtypeStruct((n_local, cap, hidden), BF16)]
        out_specs = [pl.BlockSpec((1, cap, hidden), weight_out)]
        out_shape += [jax.ShapeDtypeStruct(w.shape, F32) for w in (w_gate, w_up, w_down)]
        out_specs += [pl.BlockSpec((1,) + w.shape[1:], weight_out) for w in (w_gate, w_up, w_down)]
        scratch += [wide]
    scratch += [
        pltpu.VMEM((pack_rows, tok_rows), BF16),
        pltpu.VMEM((2, n_local, CHUNK, tok_rows), BF16),
        pltpu.VMEM((pack_rows, hidden), BF16),
        pltpu.VMEM((2, hidden, 2 * ff), BF16),
        pltpu.VMEM((2, ff, hidden), BF16),
        pltpu.SMEM((n_src, n_local), jnp.int32),
        pltpu.SMEM((n_local,), jnp.int32),
        pltpu.SemaphoreType.DMA((2, 3)),
    ]
    body = backward_kernel if backward else forward_kernel
    flops = (100 if backward else 60) * 10 ** 9
    return pl.pallas_call(
        functools.partial(body, n_src, n_local, cap),
        grid_spec=pltpu.PrefetchScalarGridSpec(
            num_scalar_prefetch=1,
            grid=(steps,),
            in_specs=[table_spec] + [route_spec, route_spec, raw, raw, raw],
            out_specs=out_specs,
            scratch_shapes=scratch,
        ),
        out_shape=out_shape,
        compiler_params=pltpu.CompilerParams(dimension_semantics=("arbitrary",), vmem_limit_bytes=VMEM_BYTES),
        cost_estimate=pl.CostEstimate(flops=flops, bytes_accessed=60 * 10 ** 6, transcendentals=0),
        name="expert_backward" if backward else "expert_forward",
    )(chunks, table, pos, gate, w_gate, w_up, w_down)


def reduce_tail_kernel(base_ref, rows_ref, pos_ref, h_ref, x_ref, grad_ref, pre_ref, w1_ref, w2_ref, out_ref,
                       rows_buf, hot, pack, rep, work, sums, core_in, x_in, y_in, x_last, y_last,
                       dx_buf, h_buf, x_buf, grad_buf, pre_buf, w1_buf, w2_buf,
                       rows_sem, load_sem, pre_sem, core_send, core_recv, hop_send, hop_recv, last_send, last_recv, dx_send, dx_recv):
    n_chunks, half = x_in.shape[0], x_in.shape[2]
    chunk = 2 * half
    n_local, cap = rows_ref.shape[:2]
    tok_rows = n_chunks * chunk
    group = hot.shape[0] // 128
    far, near_x, near_y, own = range(4)
    me = lax.axis_index("ep")
    core, x_pos, y_pos = lax.rem(me, 2), lax.rem(me // 2, 2), me // 4
    x_step, y_step = 2 - 4 * x_pos, 4 - 8 * y_pos
    partner = me + 1 - 2 * core
    x_peer, y_peer = me + x_step, me + y_step
    pp_peer = 1 - lax.axis_index("pp")
    mesh_id = pl.DeviceIdType.MESH

    barrier = pltpu.get_barrier_semaphore()
    for peer in ({"ep": partner}, {"ep": x_peer}, {"ep": y_peer}, {"pp": pp_peer}):
        pl.semaphore_signal(barrier, inc=1, device_id=peer, device_id_type=mesh_id)

    def expert_rows(e):
        return pltpu.make_async_copy(rows_ref.at[e], rows_buf.at[pl.ds(e * cap, cap)], rows_sem.at[e])

    def start_rows(e, carry):
        expert_rows(e).start()
        return carry

    lax.fori_loop(0, n_local, start_rows, 0)
    rows_buf[n_local * cap:] = jnp.zeros((rows_buf.shape[0] - n_local * cap,) + rows_buf.shape[1:], BF16)

    def loads():
        pairs = ((h_ref, h_buf), (x_ref, x_buf), (grad_ref, grad_buf), (w1_ref, w1_buf), (w2_ref, w2_buf))
        return [pltpu.make_async_copy(src, dst, load_sem.at[n]) for n, (src, dst) in enumerate(pairs)]

    def chunk_rows(k):
        return pl.ds(pl.multiple_of(k * chunk, chunk), chunk)

    def half_rows(k, low):
        return pl.ds(pl.multiple_of(k * chunk + low * half, half), half)

    def pre_copy(k):
        return pltpu.make_async_copy(pre_ref.at[chunk_rows(k)], pre_buf.at[lax.rem(k, 2)], pre_sem.at[k])

    def core_copy(t):
        return pltpu.make_async_remote_copy(work.at[0], core_in.at[t], core_send.at[t], core_recv.at[t],
                                            device_id={"ep": partner}, device_id_type=mesh_id)

    def hop_copy(k, n):
        t, low, land, j, peer = ((far, 0, x_in, 1, x_peer), (far, 1, y_in, 1, y_peer), (near_x, 0, x_in, 0, x_peer), (near_y, 1, y_in, 0, y_peer))[n]
        return pltpu.make_async_remote_copy(sums.at[t, half_rows(k, low)], land.at[k, j], hop_send.at[k, n], hop_recv.at[k, n],
                                            device_id={"ep": peer}, device_id_type=mesh_id)

    def last_copy(k, n):
        t, low, land, peer = ((near_y, 0, y_last, y_peer), (near_x, 1, x_last, x_peer))[n]
        return pltpu.make_async_remote_copy(sums.at[t, half_rows(k, low)], land.at[k], last_send.at[k, n], last_recv.at[k, n],
                                            device_id={"ep": peer}, device_id_type=mesh_id)

    def dx_copy(k):
        return pltpu.make_async_remote_copy(dx_buf.at[chunk_rows(k)], out_ref.at[chunk_rows(k)], dx_send.at[k], dx_recv.at[k],
                                            device_id={"pp": pp_peer}, device_id_type=mesh_id)

    iota = lax.broadcasted_iota(jnp.int32, (CHUNK, tok_rows), 0).astype(F32).astype(BF16)
    ones = jnp.ones((CHUNK, tok_rows), BF16)

    def combine_dest(dest, slot):
        for expert in range(n_local):
            rep[expert] = jnp.broadcast_to(pos_ref[dest, expert:expert + 1, :], (CHUNK, tok_rows)).astype(BF16)
        work[slot] = jnp.zeros(work.shape[1:], F32)

        def part(g, carry):
            for i in range(group):
                expert = g * group + i
                pos_rows = rep[expert]
                for c in range(128 // CHUNK):
                    line = i * 128 + c * CHUNK
                    hot[line:line + CHUNK, :] = jnp.where(iota + jnp.bfloat16(c * CHUNK) == pos_rows, ones, jnp.zeros_like(ones))
                pack[i * 128:(i + 1) * 128, :] = rows_buf[pl.ds(expert * cap + base_ref[dest, expert], 128 // CHUNK)].reshape(128, pack.shape[1])
            work[slot] += dot_tn(hot[...], pack[...])
            return carry

        lax.fori_loop(0, n_local // group, part, 0)

    def wait_rows(e, carry):
        expert_rows(e).wait()
        return carry

    lax.fori_loop(0, n_local, wait_rows, 0)
    for copy in loads():
        copy.start()
    for k in range(2):
        pre_copy(k).start()
    pl.semaphore_wait(barrier, 4)

    def start_hops(*which):
        def body(k, carry):
            for n in which:
                hop_copy(k, n).start()
            return carry

        lax.fori_loop(0, n_chunks, body, 0)

    def one_chip(t, carry):
        shift = x_step * (1 - t // 2) + y_step * (1 - lax.rem(t, 2))

        @pl.when(t > 0)
        def _():
            core_copy(t - 1).wait_send()

        combine_dest(partner + shift, 0)
        core_copy(t).start()
        combine_dest(me + shift, 1)
        core_copy(t).wait_recv()
        sums[t] = work[1] + core_in[t]
        pl.when(t == far)(functools.partial(start_hops, 0, 1))
        pl.when(t == near_x)(functools.partial(start_hops, 2))
        pl.when(t == near_y)(functools.partial(start_hops, 3))
        return carry

    lax.fori_loop(0, 4, one_chip, 0)
    core_copy(3).wait_send()

    def relay(k, carry):
        for n, (t, low, land) in enumerate(((near_y, 0, x_in), (near_x, 1, y_in))):
            hop_copy(k, n).wait_recv()
            sums[t, half_rows(k, low), :] = sums[t, half_rows(k, low), :] + land[k, 1]
            last_copy(k, n).start()
        return carry

    lax.fori_loop(0, n_chunks, relay, 0)

    for copy in loads():
        copy.wait()

    def norm_grad(values, grads):
        scale = lax.rsqrt(jnp.mean(values * values, axis=-1, keepdims=True) + NORM_EPS)
        return scale * grads - values * (scale * scale * scale * jnp.mean(grads * values, axis=-1, keepdims=True))

    def finish(k, carry):
        rows = chunk_rows(k)
        pre_copy(k).wait()
        for n in range(2):
            hop_copy(k, n + 2).wait_recv()
            last_copy(k, n).wait_recv()
        sums[own, half_rows(k, 0), :] = sums[own, half_rows(k, 0), :] + x_in[k, 0] + y_last[k]
        sums[own, half_rows(k, 1), :] = sums[own, half_rows(k, 1), :] + y_in[k, 0] + x_last[k]
        grad_h = grad_buf[rows, :].astype(F32) + norm_grad(h_buf[rows, :].astype(F32), sums[own, rows, :])
        grad_act = dot_nt(grad_h.astype(BF16), w2_buf[...])
        grad_pre = (grad_act * silu_grad(pre_buf[lax.rem(k, 2)])).astype(BF16)

        @pl.when(k + 2 < n_chunks)
        def _():
            pre_copy(k + 2).start()

        grad_norm = dot_nt(grad_pre, w1_buf[...])
        dx_buf[rows, :] = (grad_h + norm_grad(x_buf[rows, :].astype(F32), grad_norm)).astype(BF16)
        dx_copy(k).start()
        return carry

    lax.fori_loop(0, n_chunks, finish, 0)

    def drain(k, carry):
        for n in range(4):
            hop_copy(k, n).wait_send()
        for n in range(2):
            last_copy(k, n).wait_send()
        dx_copy(k).wait()
        return carry

    lax.fori_loop(0, n_chunks, drain, 0)


def reduce_tail(base, expert_out, pos, h_rows, x_rows, grad_rows, hidden_pre, w_one, w_two):
    tok_rows, hidden = x_rows.shape
    n_local, cap = expert_out.shape[0], expert_out.shape[1] // CHUNK
    expert_out = expert_out.reshape(n_local, cap, CHUNK, hidden)
    ff = w_one.shape[1]
    n_chunks = 4
    half = tok_rows // (2 * n_chunks)
    raw = pl.BlockSpec(memory_space=pl.ANY)
    dma = pltpu.SemaphoreType.DMA
    rows_buf = pltpu.VMEM((tok_rows, hidden), BF16)
    group = n_local // 2
    return pl.pallas_call(
        reduce_tail_kernel,
        out_shape=jax.ShapeDtypeStruct((tok_rows, hidden), BF16),
        in_specs=[pl.BlockSpec(memory_space=pltpu.SMEM), raw, pl.BlockSpec(memory_space=pltpu.VMEM)] + [raw] * 6,
        out_specs=raw,
        scratch_shapes=[
            pltpu.VMEM((n_local * cap + (128 - BLOCK) // CHUNK, CHUNK, hidden), BF16),
            pltpu.VMEM((group * 128, tok_rows), BF16),
            pltpu.VMEM((group * 128, hidden), BF16),
            pltpu.VMEM((n_local, CHUNK, tok_rows), BF16),
            pltpu.VMEM((2, tok_rows, hidden), F32),
            pltpu.VMEM((4, tok_rows, hidden), F32),
            pltpu.VMEM((4, tok_rows, hidden), F32),
            pltpu.VMEM((n_chunks, 2, half, hidden), F32),
            pltpu.VMEM((n_chunks, 2, half, hidden), F32),
            pltpu.VMEM((n_chunks, half, hidden), F32),
            pltpu.VMEM((n_chunks, half, hidden), F32),
            rows_buf, rows_buf, rows_buf, rows_buf,
            pltpu.VMEM((2, 2 * half, ff), F32),
            pltpu.VMEM(w_one.shape, BF16),
            pltpu.VMEM(w_two.shape, BF16),
            dma((n_local,)), dma((5,)), dma((n_chunks,)),
            dma((4,)), dma((4,)), dma((n_chunks, 4)), dma((n_chunks, 4)),
            dma((n_chunks, 2)), dma((n_chunks, 2)), dma((n_chunks,)), dma((n_chunks,)),
        ],
        compiler_params=pltpu.CompilerParams(collective_id=0, has_side_effects=True, vmem_limit_bytes=VMEM_BYTES),
        cost_estimate=pl.CostEstimate(flops=60 * 10 ** 9, bytes_accessed=40 * 10 ** 6, transcendentals=0),
        name="reduce_tail",
    )(base, expert_out, pos, h_rows, x_rows, grad_rows, hidden_pre, w_one, w_two)


def head_kernel(x_ref, saved_ref, grad_ref, w1_ref, w2_ref, routes_ref,
                all_ref, h_ref, saved_h_ref, pre_ref, pair_ref, pos_f_ref, gate_f_ref, pos_b_ref, gate_b_ref, count_ref,
                normed, pre_buf, routes, kept, own_sem, pre_sem, first_send, first_recv, hop_send, hop_recv, core_send, core_recv):
    tok_rows = x_ref.shape[0]
    n_chunks = first_send.shape[0] - 1
    n_src = routes.shape[0]
    n_local = kept.shape[0] // (2 * n_src)
    top_k = routes_ref.shape[0] // 4
    chunk = tok_rows // n_chunks
    me = lax.axis_index("ep")
    core, x_pos, y_pos = lax.rem(me, 2), lax.rem(me // 2, 2), me // 4
    x_step, y_step = 2 - 4 * x_pos, 4 - 8 * y_pos
    partner = me + 1 - 2 * core
    x_peer, y_peer, far_peer = me + x_step, me + y_step, me + x_step + y_step
    mesh_id = pl.DeviceIdType.MESH

    barrier = pltpu.get_barrier_semaphore()
    for peer in (partner, x_peer, y_peer):
        pl.semaphore_signal(barrier, inc=1, device_id={"ep": peer}, device_id_type=mesh_id)
    pl.semaphore_wait(barrier, 3)

    def chunk_rows(c):
        return pl.ds(pl.multiple_of(c * chunk, chunk), chunk)

    def view(c, src, part):
        if isinstance(c, int) and c == n_chunks:
            size = routes.shape[1] // 2
            return routes.at[src] if part is None else routes.at[src, pl.ds(part * size, size)]
        first = src * tok_rows + c * chunk
        if part is None:
            return all_ref.at[pl.ds(pl.multiple_of(first, chunk), chunk)]
        return all_ref.at[pl.ds(pl.multiple_of(first + part * (chunk // 2), chunk // 2), chunk // 2)]

    def remote(src, dst, send, recv, peer):
        return pltpu.make_async_remote_copy(src, dst, send, recv, device_id={"ep": peer}, device_id_type=mesh_id)

    def first_copy(c, n):
        own = routes_ref if isinstance(c, int) and c == n_chunks else normed.at[chunk_rows(c)]
        return remote(own, view(c, me, None), first_send.at[c, n], first_recv.at[c, n], (partner, x_peer, y_peer)[n])

    def hop_copy(c, n):
        piece = view(c, (x_peer, y_peer)[n], n)
        return remote(piece, piece, hop_send.at[c, n], hop_recv.at[c, n], (y_peer, x_peer)[n])

    def core_copy(c, n):
        piece = view(c, *((x_peer, None), (y_peer, None), (far_peer, 0), (far_peer, 1))[n])
        return remote(piece, piece, core_send.at[c, n], core_recv.at[c, n], partner)

    def own_copy(c):
        return pltpu.make_async_copy(normed.at[chunk_rows(c)], view(c, me, None), own_sem.at[c])

    def pass_on(c):
        for n in range(2):
            first_copy(c, n + 1).wait_recv()
            hop_copy(c, n).start()
            core_copy(c, n).start()

    def pass_far(c):
        for n in range(2):
            hop_copy(c, n).wait_recv()
            core_copy(c, n + 2).start()

    def arrive(c):
        first_copy(c, 0).wait_recv()
        for n in range(4):
            core_copy(c, n).wait_recv()

    def drain(c):
        for n in range(3):
            first_copy(c, n).wait_send()
        for n in range(2):
            hop_copy(c, n).wait_send()
        for n in range(4):
            core_copy(c, n).wait_send()

    def dense_rows(x_rows):
        pre = dot_nn(rms_norm(x_rows).astype(BF16), w1_ref[...])
        act = (pre * jax.nn.sigmoid(pre)).astype(BF16)
        hidden = (x_rows + dot_nn(act, w2_ref[...])).astype(BF16)
        return pre, hidden, rms_norm(hidden.astype(F32)).astype(BF16)

    def dense(c):
        rows = chunk_rows(c)
        _, h_ref[rows, :], normed[rows, :] = dense_rows(x_ref[rows, :].astype(F32))

    def pre_copy(c):
        return pltpu.make_async_copy(pre_buf.at[chunk_rows(c)], pre_ref.at[chunk_rows(c)], pre_sem.at[c])

    def dense_saved(c):
        rows = chunk_rows(c)
        width = grad_ref.shape[1]
        pre_buf[rows, :], saved_h_ref[rows, :], pair_ref[rows, :width] = dense_rows(saved_ref[rows, :].astype(F32))
        pair_ref[rows, width:] = grad_ref[rows, :]
        pre_copy(c).start()

    def send(c):
        for n in (1, 2, 0):
            first_copy(c, n).start()
        own_copy(c).start()

    def tables(src):
        pieces = [routes[src, pl.ds(i * top_k, top_k), :].astype(F32) for i in range(4)] if top_k % CHUNK == 0 else None
        whole = routes[src].astype(F32) if pieces is None else None
        if pieces is None:
            pieces = [whole[i * top_k:(i + 1) * top_k] for i in range(4)]
        lines = lax.broadcasted_iota(jnp.int32, (n_local, tok_rows), 0)

        def body(expert, carry):
            wanted = (me * n_local + expert).astype(F32)
            out = []
            for batch in range(2):
                match = pieces[2 * batch] == wanted
                here = lines == expert
                hit = jnp.max(jnp.where(match, 1.0, 0.0), axis=0, keepdims=True)
                gate = jnp.sum(jnp.where(match, pieces[2 * batch + 1], 0.0), axis=0, keepdims=True)
                out += [jnp.where(here, hit, carry[2 * batch]), jnp.where(here, gate, carry[2 * batch + 1])]
            return tuple(out)

        zero = jnp.zeros((n_local, tok_rows), F32)
        hit_f, gate_f, hit_b, gate_b = lax.fori_loop(0, n_local, body, (zero,) * 4)
        rows = pl.ds(pl.multiple_of(src * n_local, n_local), n_local)
        low_rows = pl.ds(pl.multiple_of((n_src + src) * n_local, n_local), n_local)
        gate_f_ref[rows, :] = gate_f
        gate_b_ref[rows, :] = gate_b
        kept[rows, :] = hit_f.astype(BF16)
        kept[low_rows, :] = hit_b.astype(BF16)

    def ranks():
        width = 256
        hits = kept[...]
        half = n_src * n_local
        for first in range(0, tok_rows, width):
            upto = lax.broadcasted_iota(jnp.int32, (tok_rows, width), 1) + first
            upper = jnp.where(lax.broadcasted_iota(jnp.int32, (tok_rows, width), 0) <= upto, 1.0, 0.0).astype(BF16)
            rank = dot_nn(hits, upper)
            pos = jnp.where(kept[:, first:first + width].astype(F32) > 0.0, rank - 1.0, -1.0)
            pos_f_ref[:, first:first + width] = pos[:half]
            pos_b_ref[:, first:first + width] = pos[half:]
            if first + width == tok_rows:
                count_ref[...] = rank[:, width - 128:]

    routes[me] = routes_ref[...]
    for n in (1, 2, 0):
        first_copy(n_chunks, n).start()
    dense(0)
    pass_on(n_chunks)
    send(0)

    def dense_send(c, carry):
        dense(c)
        send(c)
        return carry

    lax.fori_loop(1, n_chunks, dense_send, 0)
    pass_far(n_chunks)
    arrive(n_chunks)

    def forward(c, carry):
        pass_on(c)
        for i in range(n_src // n_chunks):
            tables(c * (n_src // n_chunks) + i)
        dense_saved(c)
        return carry

    lax.fori_loop(0, n_chunks, forward, 0)

    def far(c, carry):
        pass_far(c)
        return carry

    lax.fori_loop(0, n_chunks - 1, far, 0)
    ranks()
    lax.fori_loop(n_chunks - 1, n_chunks, far, 0)

    def finish(c, carry):
        arrive(c)
        own_copy(c).wait()
        pre_copy(c).wait()
        drain(c)
        return carry

    lax.fori_loop(0, n_chunks, finish, 0)
    drain(n_chunks)


def head(x_rows, saved_rows, grad_rows, w_one, w_two, routes, n_src, n_local):
    tok_rows, hidden = x_rows.shape
    ff = w_one.shape[1]
    n_chunks = 4
    dma = pltpu.SemaphoreType.DMA
    vmem = pl.BlockSpec(memory_space=pltpu.VMEM)
    raw = pl.BlockSpec(memory_space=pl.ANY)
    table = jax.ShapeDtypeStruct((n_src * n_local, tok_rows), F32)
    return pl.pallas_call(
        head_kernel,
        out_shape=[
            jax.ShapeDtypeStruct((n_src * tok_rows, hidden), BF16), jax.ShapeDtypeStruct((tok_rows, hidden), BF16),
            jax.ShapeDtypeStruct((tok_rows, hidden), BF16), jax.ShapeDtypeStruct((tok_rows, ff), F32),
            jax.ShapeDtypeStruct((tok_rows, 2 * hidden), BF16),
            table, table, table, table, jax.ShapeDtypeStruct((2 * n_src * n_local, 128), F32),
        ],
        in_specs=[vmem] * 6,
        out_specs=[raw, vmem, vmem, raw] + [vmem] * 6,
        scratch_shapes=[
            pltpu.VMEM((tok_rows, hidden), BF16),
            pltpu.VMEM((tok_rows, ff), F32),
            pltpu.VMEM((n_src,) + routes.shape, BF16),
            pltpu.VMEM((2 * n_src * n_local, tok_rows), BF16),
            dma((n_chunks,)), dma((n_chunks,)),
            dma((n_chunks + 1, 3)), dma((n_chunks + 1, 3)),
            dma((n_chunks + 1, 2)), dma((n_chunks + 1, 2)),
            dma((n_chunks + 1, 4)), dma((n_chunks + 1, 4)),
        ],
        compiler_params=pltpu.CompilerParams(collective_id=1, has_side_effects=True, vmem_limit_bytes=VMEM_BYTES),
        cost_estimate=pl.CostEstimate(flops=30 * 10 ** 9, bytes_accessed=20 * 10 ** 6, transcendentals=0),
        name="head",
    )(x_rows, saved_rows, grad_rows, w_one, w_two, routes)


def solution(mesh):
    stages = mesh.shape["pp"]
    ep_size = mesh.shape["ep"]
    next_perm = [(stage_idx, (stage_idx + 1) % stages) for stage_idx in range(stages)]
    assert (stages, ep_size) == (2, 8)
    tok_spec = P("pp", "ep", None)
    dense_spec = P("pp", None, None)
    expert_spec = P("pp", "ep", None, None)

    def device_step(x_fwd, ids_fwd, slots_fwd, gates_fwd, x_saved, grad_in, ids_bwd, slots_bwd, gates_bwd, w_one, w_two, w_gate, w_up, w_down):
        x_fwd, ids_fwd, slots_fwd, gates_fwd = x_fwd[0], ids_fwd[0], slots_fwd[0], gates_fwd[0]
        x_saved, grad_in, ids_bwd, slots_bwd, gates_bwd = x_saved[0], grad_in[0], ids_bwd[0], slots_bwd[0], gates_bwd[0]
        w_one, w_two, w_gate, w_up, w_down = w_one[0], w_two[0], w_gate[0], w_up[0], w_down[0]
        n_local = w_gate.shape[0]

        routes = jnp.concatenate([
            jnp.where(slots_fwd >= 0, ids_fwd, -1).astype(BF16), gates_fwd,
            jnp.where(slots_bwd >= 0, ids_bwd, -1).astype(BF16), gates_bwd,
        ], axis=1).T
        all_fwd, h_fwd, h_bwd, hidden_pre, pair, pos_f, gate_f, pos_b, gate_b, counts = head(
            x_fwd, x_saved, grad_in, w_one, w_two, routes, ep_size, n_local)
        all_bwd = lax.all_gather(pair, "ep", axis=0, tiled=True)
        pos_f, gate_f, pos_b, gate_b = (t.reshape(ep_size, n_local, -1) for t in (pos_f, gate_f, pos_b, gate_b))
        chunks = (counts[:, -1].reshape(2, ep_size, n_local).astype(jnp.int32) + CHUNK - 1) // CHUNK
        chunks_f, chunks_b = chunks[0], chunks[1]

        (part_fwd,) = expert_call(False, chunks_f, all_fwd, pos_f, gate_f, w_gate, w_up, w_down)
        part_fwd, all_bwd = lax.optimization_barrier((part_fwd, all_bwd))
        mix_sum = lax.psum_scatter(part_fwd, "ep", scatter_dimension=0, tiled=True)
        y_out = (h_fwd.astype(F32) + mix_sum).astype(BF16)

        earlier = (jnp.arange(ep_size)[:, None] > jnp.arange(ep_size)[None, :]).astype(jnp.int32)
        base_b = jnp.sum(earlier[:, :, None] * chunks_b[None], axis=1)
        rows_bwd, dw_gate, dw_up, dw_down = expert_call(True, chunks_b, all_bwd, pos_b, gate_b, w_gate, w_up, w_down)
        y_next = lax.ppermute(y_out, "pp", next_perm)
        dx_prev = reduce_tail(base_b, rows_bwd, pos_b, h_bwd, x_saved, grad_in, hidden_pre, w_one, w_two)
        return y_next[None], dx_prev[None], dw_gate[None], dw_up[None], dw_down[None]

    in_specs = (tok_spec,) * 9 + (dense_spec, dense_spec, expert_spec, expert_spec, expert_spec)
    out_specs = (tok_spec, tok_spec, expert_spec, expert_spec, expert_spec)
    return jax.shard_map(device_step, mesh=mesh, in_specs=in_specs, out_specs=out_specs, check_vma=False)
```

```python
import functools

import jax
import jax.numpy as jnp
from jax import lax
from jax.experimental import pallas as pl
from jax.experimental.pallas import tpu as pltpu
from jax.sharding import PartitionSpec as P

NORM_EPS = 1e-6
CHUNK = 16
BLOCK = 64
UNROLL = 8
ROW_TILE = 1024
COMB_TILE = 256
BIG_TILE = 1024
SMALL_TILE = 256
VMEM_BYTES = 66_500_000
BF16 = jnp.bfloat16
F32 = jnp.float32


def rms_norm(values):
    return values * lax.rsqrt(jnp.mean(values * values, axis=-1, keepdims=True) + NORM_EPS)


def silu_grad(values):
    sigmoid_vals = jax.nn.sigmoid(values)
    return sigmoid_vals * (1.0 + values * (1.0 - sigmoid_vals))


def dot_nn(lhs, rhs):
    return jnp.dot(lhs, rhs, preferred_element_type=F32)


def dot_nt(lhs, rhs):
    return lax.dot_general(lhs, rhs, (((1,), (1,)), ((), ())), preferred_element_type=F32)


def dot_tn(lhs, rhs):
    return lax.dot_general(lhs, rhs, (((0,), (0,)), ((), ())), preferred_element_type=F32)


def rows_at(index, count):
    return pl.ds(pl.multiple_of(index, CHUNK), count)


def fill_onehot(hot_ref, rep, pos_ref, gate_ref, chunks_ref, src, n_local):
    tok_rows = pos_ref.shape[2]
    iota = lax.broadcasted_iota(jnp.int32, (CHUNK, tok_rows), 0).astype(F32).astype(BF16)
    ones = jnp.ones((CHUNK, tok_rows), BF16)
    for expert in range(n_local):
        rep[0, expert] = jnp.broadcast_to(pos_ref[0, expert:expert + 1, :], (CHUNK, tok_rows)).astype(BF16)
        if gate_ref is not None:
            rep[1, expert] = jnp.broadcast_to(gate_ref[0, expert:expert + 1, :], (CHUNK, tok_rows)).astype(BF16)

    def one(expert, start):
        n_chunks = chunks_ref[src, expert]

        def block(first):
            pos_rows = rep[0, expert]
            value = ones if gate_ref is None else rep[1, expert]
            for c in range(first, first + BLOCK // CHUNK):
                hot = jnp.where(iota + jnp.bfloat16(c * CHUNK) == pos_rows, value, jnp.zeros_like(value))
                hot_ref[rows_at(start + c * CHUNK, CHUNK), :] = hot

        block(0)
        pl.when(n_chunks > BLOCK // CHUNK)(functools.partial(block, BLOCK // CHUNK))
        return start + n_chunks * CHUNK

    return expert_loop(n_local, one)


def expert_loop(n_local, one):
    def body(group, start):
        for i in range(UNROLL):
            start = one(group * UNROLL + i, start)
        return start

    return lax.fori_loop(0, n_local // UNROLL, body, jnp.int32(0))


def zero_tail(ref, offset, length, tile):
    n_tiles = (length + tile - 1) // tile

    def body(c, carry):
        ref[rows_at(offset + c * CHUNK, CHUNK), :] = jnp.zeros((CHUNK, ref.shape[1]), ref.dtype)
        return carry

    lax.fori_loop(length // CHUNK, n_tiles * (tile // CHUNK), body, 0)


def move_segments(pack_ref, wide_ref, base_ref, chunks_ref, src, n_local, cap, to_wide):
    def one(expert, start):
        n_chunks = chunks_ref[src, expert]
        base = expert * cap + base_ref[src, expert]

        def block(first):
            pack_rows = rows_at(start + first, BLOCK)
            wide_rows = rows_at(base + first, BLOCK)
            if to_wide:
                wide_ref[wide_rows, :] = pack_ref[pack_rows, :]
            else:
                pack_ref[pack_rows, :] = wide_ref[wide_rows, :]

        block(0)
        pl.when(n_chunks > BLOCK // CHUNK)(functools.partial(block, BLOCK))
        return start + n_chunks * CHUNK

    expert_loop(n_local, one)


def expert_bases(base_ref, total_ref, chunks_ref, n_src, n_local):
    for expert in range(n_local):
        total_ref[expert] = 0

    def body(src, carry):
        for expert in range(n_local):
            base_ref[src, expert] = total_ref[expert]
            total_ref[expert] = total_ref[expert] + chunks_ref[src, expert] * CHUNK
        return carry

    lax.fori_loop(0, n_src, body, 0)


def dispatch(pack_ref, hot_ref, table_ref, columns, wide_ref, base_ref, chunks_ref, src, n_local, cap, length):
    def step(rows):
        pack_ref[rows, :] = dot_nn(hot_ref[rows, :], table_ref[:, columns]).astype(BF16)

    tiled_rows(0, length, step, ROW_TILE, SMALL_TILE)
    move_segments(pack_ref, wide_ref, base_ref, chunks_ref, src, n_local, cap, True)


def combine(out_ref, pack_ref, hot_ref, wide_ref, base_ref, chunks_ref, src, n_local, cap, length):
    move_segments(pack_ref, wide_ref, base_ref, chunks_ref, src, n_local, cap, False)
    zero_tail(pack_ref, 0, length, COMB_TILE)
    zero_tail(hot_ref, 0, length, COMB_TILE)
    out_ref[...] = jnp.zeros_like(out_ref)

    def step(rows):
        out_ref[...] += dot_tn(hot_ref[rows, :], pack_ref[rows, :])

    tiled_rows(0, length, step, ROW_TILE, COMB_TILE)


def tiled_rows(first, count, step, big_tile, small_tile):
    n_small = (count + small_tile - 1) // small_tile
    per_big = big_tile // small_tile
    n_big = n_small // per_big

    def big(tile, carry):
        step(rows_at(first + tile * big_tile, big_tile))
        return carry

    lax.fori_loop(0, n_big, big, 0)
    for left in range(1, per_big):
        pl.when(n_small - n_big * per_big == left)(
            functools.partial(step, rows_at(first + n_big * big_tile, left * small_tile)))


def weight_copies(expert, slot, wg_ref, wu_ref, wd_ref, gu_buf, dn_buf, sems):
    ff = wg_ref.shape[2]
    return (
        pltpu.make_async_copy(wg_ref.at[expert], gu_buf.at[slot, :, pl.ds(0, ff)], sems.at[slot, 0]),
        pltpu.make_async_copy(wu_ref.at[expert], gu_buf.at[slot, :, pl.ds(ff, ff)], sems.at[slot, 1]),
        pltpu.make_async_copy(wd_ref.at[expert], dn_buf.at[slot], sems.at[slot, 2]),
    )


def next_weights(expert, n_local, *refs):
    slot = lax.rem(expert, 2)

    @pl.when(expert + 1 < n_local)
    def _():
        for copy in weight_copies(expert + 1, lax.rem(expert + 1, 2), *refs):
            copy.start()

    for copy in weight_copies(expert, slot, *refs):
        copy.wait()
    return slot


def forward_kernel(n_src, n_local, cap, chunks_ref, tok_ref, pos_ref, gate_ref, wg_ref, wu_ref, wd_ref, out_ref,
                   wide, hot, rep, pack, gu_buf, dn_buf, base, total, sems):
    step = pl.program_id(0)
    hidden, ff = wg_ref.shape[1:]
    w_refs = (wg_ref, wu_ref, wd_ref, gu_buf, dn_buf, sems)

    @pl.when(step == 0)
    def _():
        for copy in weight_copies(0, 0, *w_refs):
            copy.start()
        expert_bases(base, total, chunks_ref, n_src, n_local)

    @pl.when(step < n_src)
    def _():
        length = fill_onehot(hot, rep, pos_ref, None, chunks_ref, step, n_local)
        dispatch(pack, hot, tok_ref, pl.ds(0, hidden), wide, base, chunks_ref, step, n_local, cap, length)

    @pl.when((step >= n_src) & (step < n_src + n_local))
    def _():
        expert = step - n_src
        slot = next_weights(expert, n_local, *w_refs)

        def rows_step(rows):
            pre = dot_nn(wide[rows, :], gu_buf[slot])
            gate = pre[:, :ff]
            act = (gate * jax.nn.sigmoid(gate) * pre[:, ff:]).astype(BF16)
            wide[rows, :] = dot_nn(act, dn_buf[slot]).astype(BF16)

        tiled_rows(expert * cap, total[expert], rows_step, BIG_TILE, SMALL_TILE)

    @pl.when(step >= n_src + n_local)
    def _():
        src = step - n_src - n_local
        length = fill_onehot(hot, rep, pos_ref, gate_ref, chunks_ref, src, n_local)
        combine(out_ref, pack, hot, wide, base, chunks_ref, src, n_local, cap, length)


def backward_kernel(n_src, n_local, cap, chunks_ref, tok_ref, pos_ref, gate_ref, wg_ref, wu_ref, wd_ref,
                    rows_ref, dwg_ref, dwu_ref, dwd_ref,
                    wide_x, wide_q, hot, rep, pack, gu_buf, dn_buf, base, total, sems):
    step = pl.program_id(0)
    hidden, ff = wg_ref.shape[1:]
    w_refs = (wg_ref, wu_ref, wd_ref, gu_buf, dn_buf, sems)

    @pl.when(step == 0)
    def _():
        for copy in weight_copies(0, 0, *w_refs):
            copy.start()
        expert_bases(base, total, chunks_ref, n_src, n_local)

    @pl.when(step < n_src)
    def _():
        length = fill_onehot(hot, rep, pos_ref, None, chunks_ref, step, n_local)
        dispatch(pack, hot, tok_ref, pl.ds(0, hidden), wide_x, base, chunks_ref, step, n_local, cap, length)
        fill_onehot(hot, rep, pos_ref, gate_ref, chunks_ref, step, n_local)
        dispatch(pack, hot, tok_ref, pl.ds(hidden, hidden), wide_q, base, chunks_ref, step, n_local, cap, length)

    @pl.when((step >= n_src) & (step < n_src + n_local))
    def _():
        expert = step - n_src
        slot = next_weights(expert, n_local, *w_refs)
        zero_tail(wide_x, expert * cap, total[expert], SMALL_TILE)
        zero_tail(wide_q, expert * cap, total[expert], SMALL_TILE)
        dwg_ref[...] = jnp.zeros_like(dwg_ref)
        dwu_ref[...] = jnp.zeros_like(dwu_ref)
        dwd_ref[...] = jnp.zeros_like(dwd_ref)

        def rows_step(rows):
            x_rows = wide_x[rows, :]
            q_rows = wide_q[rows, :]
            pre = dot_nn(x_rows, gu_buf[slot])
            gate, up = pre[:, :ff], pre[:, ff:]
            sig = jax.nn.sigmoid(gate)
            silu = gate * sig
            act = (silu * up).astype(BF16)
            grad_act = dot_nt(q_rows, dn_buf[slot]).astype(BF16).astype(F32)
            grad_gate = (grad_act * up * (sig * (1.0 + gate * (1.0 - sig)))).astype(BF16)
            grad_up = (grad_act * silu).astype(BF16)
            grad_pre = jnp.concatenate([grad_gate, grad_up], axis=1)
            dwd_ref[0] += dot_tn(act, q_rows)
            dw_pre = dot_tn(x_rows, grad_pre)
            dwg_ref[0] += dw_pre[:, :ff]
            dwu_ref[0] += dw_pre[:, ff:]
            rows_ref[0, rows_at(rows.start - expert * cap, rows.size), :] = dot_nt(grad_pre, gu_buf[slot]).astype(BF16)

        tiled_rows(expert * cap, total[expert], rows_step, BIG_TILE, SMALL_TILE)

        done = (total[expert] + SMALL_TILE - 1) // SMALL_TILE * (SMALL_TILE // CHUNK)
        end = jnp.minimum(total[expert] // CHUNK + 128 // CHUNK, cap // CHUNK)

        def clear(c, carry):
            rows_ref[0, rows_at(c * CHUNK, CHUNK), :] = jnp.zeros((CHUNK, hidden), BF16)
            return carry

        lax.fori_loop(done, jnp.maximum(done, end), clear, 0)


def expert_call(backward, chunks, table, pos, gate, w_gate, w_up, w_down):
    n_src, n_local, tok_rows = pos.shape
    hidden, ff = w_gate.shape[1:]
    cap = n_src * 128 + BLOCK
    pack_rows = n_local * 128 + BLOCK
    steps = n_src + n_local if backward else 2 * n_src + n_local

    def src_in(i, *_):
        return (jnp.minimum(i, n_src - 1), 0)

    def src_out(i, *_):
        return (jnp.clip(i - n_src - n_local, 0, n_src - 1), 0)

    def weight_out(i, *_):
        return (jnp.clip(i - n_src, 0, n_local - 1), 0, 0)

    table_spec = pl.BlockSpec((tok_rows, table.shape[1]), src_in)

    def route_in(i, *_):
        return (jnp.where(i < n_src, i, jnp.clip(i - n_src - n_local, 0, n_src - 1)), 0, 0)

    route_spec = pl.BlockSpec((1,) + pos.shape[1:], route_in)
    raw = pl.BlockSpec(memory_space=pl.ANY)
    out_shape = [jax.ShapeDtypeStruct((n_src * tok_rows, hidden), F32)]
    out_specs = [pl.BlockSpec((tok_rows, hidden), src_out)]
    wide = pltpu.VMEM((n_local * cap, hidden), BF16)
    scratch = [wide]
    if backward:
        out_shape = [jax.ShapeDtypeStruct((n_local, cap, hidden), BF16)]
        out_specs = [pl.BlockSpec((1, cap, hidden), weight_out)]
        out_shape += [jax.ShapeDtypeStruct(w.shape, F32) for w in (w_gate, w_up, w_down)]
        out_specs += [pl.BlockSpec((1,) + w.shape[1:], weight_out) for w in (w_gate, w_up, w_down)]
        scratch += [wide]
    scratch += [
        pltpu.VMEM((pack_rows, tok_rows), BF16),
        pltpu.VMEM((2, n_local, CHUNK, tok_rows), BF16),
        pltpu.VMEM((pack_rows, hidden), BF16),
        pltpu.VMEM((2, hidden, 2 * ff), BF16),
        pltpu.VMEM((2, ff, hidden), BF16),
        pltpu.SMEM((n_src, n_local), jnp.int32),
        pltpu.SMEM((n_local,), jnp.int32),
        pltpu.SemaphoreType.DMA((2, 3)),
    ]
    body = backward_kernel if backward else forward_kernel
    flops = (100 if backward else 60) * 10 ** 9
    return pl.pallas_call(
        functools.partial(body, n_src, n_local, cap),
        grid_spec=pltpu.PrefetchScalarGridSpec(
            num_scalar_prefetch=1,
            grid=(steps,),
            in_specs=[table_spec] + [route_spec, route_spec, raw, raw, raw],
            out_specs=out_specs,
            scratch_shapes=scratch,
        ),
        out_shape=out_shape,
        compiler_params=pltpu.CompilerParams(dimension_semantics=("arbitrary",), vmem_limit_bytes=VMEM_BYTES),
        cost_estimate=pl.CostEstimate(flops=flops, bytes_accessed=60 * 10 ** 6, transcendentals=0),
        name="expert_backward" if backward else "expert_forward",
    )(chunks, table, pos, gate, w_gate, w_up, w_down)


def reduce_tail_kernel(base_ref, rows_ref, pos_ref, h_ref, x_ref, grad_ref, pre_ref, w1_ref, w2_ref, out_ref,
                       rows_buf, hot, pack, rep, work, sums, core_in, x_in, y_in, x_last, y_last,
                       dx_buf, h_buf, x_buf, grad_buf, pre_buf, w1_buf, w2_buf,
                       rows_sem, load_sem, pre_sem, core_send, core_recv, hop_send, hop_recv, last_send, last_recv, dx_send, dx_recv):
    n_chunks, half = x_in.shape[0], x_in.shape[2]
    chunk = 2 * half
    n_local, cap = rows_ref.shape[:2]
    tok_rows = n_chunks * chunk
    group = hot.shape[0] // 128
    far, near_x, near_y, own = range(4)
    me = lax.axis_index("ep")
    core, x_pos, y_pos = lax.rem(me, 2), lax.rem(me // 2, 2), me // 4
    x_step, y_step = 2 - 4 * x_pos, 4 - 8 * y_pos
    partner = me + 1 - 2 * core
    x_peer, y_peer = me + x_step, me + y_step
    pp_peer = 1 - lax.axis_index("pp")
    mesh_id = pl.DeviceIdType.MESH

    barrier = pltpu.get_barrier_semaphore()
    for peer in ({"ep": partner}, {"ep": x_peer}, {"ep": y_peer}, {"pp": pp_peer}):
        pl.semaphore_signal(barrier, inc=1, device_id=peer, device_id_type=mesh_id)

    def expert_rows(e):
        return pltpu.make_async_copy(rows_ref.at[e], rows_buf.at[pl.ds(e * cap, cap)], rows_sem.at[e])

    def start_rows(e, carry):
        expert_rows(e).start()
        return carry

    lax.fori_loop(0, n_local, start_rows, 0)
    rows_buf[n_local * cap:] = jnp.zeros((rows_buf.shape[0] - n_local * cap,) + rows_buf.shape[1:], BF16)

    def loads():
        pairs = ((h_ref, h_buf), (x_ref, x_buf), (grad_ref, grad_buf), (w1_ref, w1_buf), (w2_ref, w2_buf))
        return [pltpu.make_async_copy(src, dst, load_sem.at[n]) for n, (src, dst) in enumerate(pairs)]

    def chunk_rows(k):
        return pl.ds(pl.multiple_of(k * chunk, chunk), chunk)

    def half_rows(k, low):
        return pl.ds(pl.multiple_of(k * chunk + low * half, half), half)

    def pre_copy(k):
        return pltpu.make_async_copy(pre_ref.at[chunk_rows(k)], pre_buf.at[lax.rem(k, 2)], pre_sem.at[k])

    def core_copy(t):
        return pltpu.make_async_remote_copy(work.at[0], core_in.at[t], core_send.at[t], core_recv.at[t],
                                            device_id={"ep": partner}, device_id_type=mesh_id)

    def hop_copy(k, n):
        t, low, land, j, peer = ((far, 0, x_in, 1, x_peer), (far, 1, y_in, 1, y_peer), (near_x, 0, x_in, 0, x_peer), (near_y, 1, y_in, 0, y_peer))[n]
        return pltpu.make_async_remote_copy(sums.at[t, half_rows(k, low)], land.at[k, j], hop_send.at[k, n], hop_recv.at[k, n],
                                            device_id={"ep": peer}, device_id_type=mesh_id)

    def last_copy(k, n):
        t, low, land, peer = ((near_y, 0, y_last, y_peer), (near_x, 1, x_last, x_peer))[n]
        return pltpu.make_async_remote_copy(sums.at[t, half_rows(k, low)], land.at[k], last_send.at[k, n], last_recv.at[k, n],
                                            device_id={"ep": peer}, device_id_type=mesh_id)

    def dx_copy(k):
        return pltpu.make_async_remote_copy(dx_buf.at[chunk_rows(k)], out_ref.at[chunk_rows(k)], dx_send.at[k], dx_recv.at[k],
                                            device_id={"pp": pp_peer}, device_id_type=mesh_id)

    iota = lax.broadcasted_iota(jnp.int32, (CHUNK, tok_rows), 0).astype(F32).astype(BF16)
    ones = jnp.ones((CHUNK, tok_rows), BF16)

    def combine_dest(dest, slot):
        for expert in range(n_local):
            rep[expert] = jnp.broadcast_to(pos_ref[dest, expert:expert + 1, :], (CHUNK, tok_rows)).astype(BF16)
        work[slot] = jnp.zeros(work.shape[1:], F32)

        def part(g, carry):
            for i in range(group):
                expert = g * group + i
                pos_rows = rep[expert]
                for c in range(128 // CHUNK):
                    line = i * 128 + c * CHUNK
                    hot[line:line + CHUNK, :] = jnp.where(iota + jnp.bfloat16(c * CHUNK) == pos_rows, ones, jnp.zeros_like(ones))
                pack[i * 128:(i + 1) * 128, :] = rows_buf[pl.ds(expert * cap + base_ref[dest, expert], 128 // CHUNK)].reshape(128, pack.shape[1])
            work[slot] += dot_tn(hot[...], pack[...])
            return carry

        lax.fori_loop(0, n_local // group, part, 0)

    def wait_rows(e, carry):
        expert_rows(e).wait()
        return carry

    lax.fori_loop(0, n_local, wait_rows, 0)
    for copy in loads():
        copy.start()
    for k in range(2):
        pre_copy(k).start()
    pl.semaphore_wait(barrier, 4)

    def start_hops(*which):
        def body(k, carry):
            for n in which:
                hop_copy(k, n).start()
            return carry

        lax.fori_loop(0, n_chunks, body, 0)

    def one_chip(t, carry):
        shift = x_step * (1 - t // 2) + y_step * (1 - lax.rem(t, 2))

        @pl.when(t > 0)
        def _():
            core_copy(t - 1).wait_send()

        combine_dest(partner + shift, 0)
        core_copy(t).start()
        combine_dest(me + shift, 1)
        core_copy(t).wait_recv()
        sums[t] = work[1] + core_in[t]
        pl.when(t == far)(functools.partial(start_hops, 0, 1))
        pl.when(t == near_x)(functools.partial(start_hops, 2))
        pl.when(t == near_y)(functools.partial(start_hops, 3))
        return carry

    lax.fori_loop(0, 4, one_chip, 0)
    core_copy(3).wait_send()

    def relay(k, carry):
        for n, (t, low, land) in enumerate(((near_y, 0, x_in), (near_x, 1, y_in))):
            hop_copy(k, n).wait_recv()
            sums[t, half_rows(k, low), :] = sums[t, half_rows(k, low), :] + land[k, 1]
            last_copy(k, n).start()
        return carry

    lax.fori_loop(0, n_chunks, relay, 0)

    for copy in loads():
        copy.wait()

    def norm_grad(values, grads):
        scale = lax.rsqrt(jnp.mean(values * values, axis=-1, keepdims=True) + NORM_EPS)
        return scale * grads - values * (scale * scale * scale * jnp.mean(grads * values, axis=-1, keepdims=True))

    def finish(k, carry):
        rows = chunk_rows(k)
        pre_copy(k).wait()
        for n in range(2):
            hop_copy(k, n + 2).wait_recv()
            last_copy(k, n).wait_recv()
        sums[own, half_rows(k, 0), :] = sums[own, half_rows(k, 0), :] + x_in[k, 0] + y_last[k]
        sums[own, half_rows(k, 1), :] = sums[own, half_rows(k, 1), :] + y_in[k, 0] + x_last[k]
        grad_h = grad_buf[rows, :].astype(F32) + norm_grad(h_buf[rows, :].astype(F32), sums[own, rows, :])
        grad_act = dot_nt(grad_h.astype(BF16), w2_buf[...])
        grad_pre = (grad_act * silu_grad(pre_buf[lax.rem(k, 2)])).astype(BF16)

        @pl.when(k + 2 < n_chunks)
        def _():
            pre_copy(k + 2).start()

        grad_norm = dot_nt(grad_pre, w1_buf[...])
        dx_buf[rows, :] = (grad_h + norm_grad(x_buf[rows, :].astype(F32), grad_norm)).astype(BF16)
        dx_copy(k).start()
        return carry

    lax.fori_loop(0, n_chunks, finish, 0)

    def drain(k, carry):
        for n in range(4):
            hop_copy(k, n).wait_send()
        for n in range(2):
            last_copy(k, n).wait_send()
        dx_copy(k).wait()
        return carry

    lax.fori_loop(0, n_chunks, drain, 0)


def reduce_tail(base, expert_out, pos, h_rows, x_rows, grad_rows, hidden_pre, w_one, w_two):
    tok_rows, hidden = x_rows.shape
    n_local, cap = expert_out.shape[0], expert_out.shape[1] // CHUNK
    expert_out = expert_out.reshape(n_local, cap, CHUNK, hidden)
    ff = w_one.shape[1]
    n_chunks = 4
    half = tok_rows // (2 * n_chunks)
    raw = pl.BlockSpec(memory_space=pl.ANY)
    dma = pltpu.SemaphoreType.DMA
    rows_buf = pltpu.VMEM((tok_rows, hidden), BF16)
    group = n_local // 2
    return pl.pallas_call(
        reduce_tail_kernel,
        out_shape=jax.ShapeDtypeStruct((tok_rows, hidden), BF16),
        in_specs=[pl.BlockSpec(memory_space=pltpu.SMEM), raw, pl.BlockSpec(memory_space=pltpu.VMEM)] + [raw] * 6,
        out_specs=raw,
        scratch_shapes=[
            pltpu.VMEM((n_local * cap + (128 - BLOCK) // CHUNK, CHUNK, hidden), BF16),
            pltpu.VMEM((group * 128, tok_rows), BF16),
            pltpu.VMEM((group * 128, hidden), BF16),
            pltpu.VMEM((n_local, CHUNK, tok_rows), BF16),
            pltpu.VMEM((2, tok_rows, hidden), F32),
            pltpu.VMEM((4, tok_rows, hidden), F32),
            pltpu.VMEM((4, tok_rows, hidden), F32),
            pltpu.VMEM((n_chunks, 2, half, hidden), F32),
            pltpu.VMEM((n_chunks, 2, half, hidden), F32),
            pltpu.VMEM((n_chunks, half, hidden), F32),
            pltpu.VMEM((n_chunks, half, hidden), F32),
            rows_buf, rows_buf, rows_buf, rows_buf,
            pltpu.VMEM((2, 2 * half, ff), F32),
            pltpu.VMEM(w_one.shape, BF16),
            pltpu.VMEM(w_two.shape, BF16),
            dma((n_local,)), dma((5,)), dma((n_chunks,)),
            dma((4,)), dma((4,)), dma((n_chunks, 4)), dma((n_chunks, 4)),
            dma((n_chunks, 2)), dma((n_chunks, 2)), dma((n_chunks,)), dma((n_chunks,)),
        ],
        compiler_params=pltpu.CompilerParams(collective_id=0, has_side_effects=True, vmem_limit_bytes=VMEM_BYTES),
        cost_estimate=pl.CostEstimate(flops=60 * 10 ** 9, bytes_accessed=40 * 10 ** 6, transcendentals=0),
        name="reduce_tail",
    )(base, expert_out, pos, h_rows, x_rows, grad_rows, hidden_pre, w_one, w_two)


def head_kernel(x_ref, saved_ref, grad_ref, w1_ref, w2_ref, routes_ref,
                all_ref, h_ref, saved_h_ref, pre_ref, pair_ref, pos_f_ref, gate_f_ref, pos_b_ref, gate_b_ref, count_ref,
                normed, pre_buf, routes, kept, own_sem, pre_sem, first_send, first_recv, hop_send, hop_recv, core_send, core_recv):
    tok_rows = x_ref.shape[0]
    n_chunks = first_send.shape[0] - 1
    n_src = routes.shape[0]
    n_local = kept.shape[0] // (2 * n_src)
    top_k = routes_ref.shape[0] // 4
    chunk = tok_rows // n_chunks
    me = lax.axis_index("ep")
    core, x_pos, y_pos = lax.rem(me, 2), lax.rem(me // 2, 2), me // 4
    x_step, y_step = 2 - 4 * x_pos, 4 - 8 * y_pos
    partner = me + 1 - 2 * core
    x_peer, y_peer, far_peer = me + x_step, me + y_step, me + x_step + y_step
    mesh_id = pl.DeviceIdType.MESH

    barrier = pltpu.get_barrier_semaphore()
    for peer in (partner, x_peer, y_peer):
        pl.semaphore_signal(barrier, inc=1, device_id={"ep": peer}, device_id_type=mesh_id)
    pl.semaphore_wait(barrier, 3)

    def chunk_rows(c):
        return pl.ds(pl.multiple_of(c * chunk, chunk), chunk)

    def view(c, src, part):
        if isinstance(c, int) and c == n_chunks:
            size = routes.shape[1] // 2
            return routes.at[src] if part is None else routes.at[src, pl.ds(part * size, size)]
        first = src * tok_rows + c * chunk
        if part is None:
            return all_ref.at[pl.ds(pl.multiple_of(first, chunk), chunk)]
        return all_ref.at[pl.ds(pl.multiple_of(first + part * (chunk // 2), chunk // 2), chunk // 2)]

    def remote(src, dst, send, recv, peer):
        return pltpu.make_async_remote_copy(src, dst, send, recv, device_id={"ep": peer}, device_id_type=mesh_id)

    def first_copy(c, n):
        own = routes_ref if isinstance(c, int) and c == n_chunks else normed.at[chunk_rows(c)]
        return remote(own, view(c, me, None), first_send.at[c, n], first_recv.at[c, n], (partner, x_peer, y_peer)[n])

    def hop_copy(c, n):
        piece = view(c, (x_peer, y_peer)[n], n)
        return remote(piece, piece, hop_send.at[c, n], hop_recv.at[c, n], (y_peer, x_peer)[n])

    def core_copy(c, n):
        piece = view(c, *((x_peer, None), (y_peer, None), (far_peer, 0), (far_peer, 1))[n])
        return remote(piece, piece, core_send.at[c, n], core_recv.at[c, n], partner)

    def own_copy(c):
        return pltpu.make_async_copy(normed.at[chunk_rows(c)], view(c, me, None), own_sem.at[c])

    def pass_on(c):
        for n in range(2):
            first_copy(c, n + 1).wait_recv()
            hop_copy(c, n).start()
            core_copy(c, n).start()

    def pass_far(c):
        for n in range(2):
            hop_copy(c, n).wait_recv()
            core_copy(c, n + 2).start()

    def arrive(c):
        first_copy(c, 0).wait_recv()
        for n in range(4):
            core_copy(c, n).wait_recv()

    def drain(c):
        for n in range(3):
            first_copy(c, n).wait_send()
        for n in range(2):
            hop_copy(c, n).wait_send()
        for n in range(4):
            core_copy(c, n).wait_send()

    def dense_rows(x_rows):
        pre = dot_nn(rms_norm(x_rows).astype(BF16), w1_ref[...])
        act = (pre * jax.nn.sigmoid(pre)).astype(BF16)
        hidden = (x_rows + dot_nn(act, w2_ref[...])).astype(BF16)
        return pre, hidden, rms_norm(hidden.astype(F32)).astype(BF16)

    def dense(c):
        rows = chunk_rows(c)
        _, h_ref[rows, :], normed[rows, :] = dense_rows(x_ref[rows, :].astype(F32))

    def pre_copy(c):
        return pltpu.make_async_copy(pre_buf.at[chunk_rows(c)], pre_ref.at[chunk_rows(c)], pre_sem.at[c])

    def dense_saved(c):
        rows = chunk_rows(c)
        width = grad_ref.shape[1]
        pre_buf[rows, :], saved_h_ref[rows, :], pair_ref[rows, :width] = dense_rows(saved_ref[rows, :].astype(F32))
        pair_ref[rows, width:] = grad_ref[rows, :]
        pre_copy(c).start()

    def send(c):
        for n in (1, 2, 0):
            first_copy(c, n).start()
        own_copy(c).start()

    def tables(src):
        pieces = [routes[src, pl.ds(i * top_k, top_k), :].astype(F32) for i in range(4)] if top_k % CHUNK == 0 else None
        whole = routes[src].astype(F32) if pieces is None else None
        if pieces is None:
            pieces = [whole[i * top_k:(i + 1) * top_k] for i in range(4)]
        lines = lax.broadcasted_iota(jnp.int32, (n_local, tok_rows), 0)

        def body(expert, carry):
            wanted = (me * n_local + expert).astype(F32)
            out = []
            for batch in range(2):
                match = pieces[2 * batch] == wanted
                here = lines == expert
                hit = jnp.max(jnp.where(match, 1.0, 0.0), axis=0, keepdims=True)
                gate = jnp.sum(jnp.where(match, pieces[2 * batch + 1], 0.0), axis=0, keepdims=True)
                out += [jnp.where(here, hit, carry[2 * batch]), jnp.where(here, gate, carry[2 * batch + 1])]
            return tuple(out)

        zero = jnp.zeros((n_local, tok_rows), F32)
        hit_f, gate_f, hit_b, gate_b = lax.fori_loop(0, n_local, body, (zero,) * 4)
        rows = pl.ds(pl.multiple_of(src * n_local, n_local), n_local)
        low_rows = pl.ds(pl.multiple_of((n_src + src) * n_local, n_local), n_local)
        gate_f_ref[rows, :] = gate_f
        gate_b_ref[rows, :] = gate_b
        kept[rows, :] = hit_f.astype(BF16)
        kept[low_rows, :] = hit_b.astype(BF16)

    def ranks():
        width = 256
        hits = kept[...]
        half = n_src * n_local
        for first in range(0, tok_rows, width):
            upto = lax.broadcasted_iota(jnp.int32, (tok_rows, width), 1) + first
            upper = jnp.where(lax.broadcasted_iota(jnp.int32, (tok_rows, width), 0) <= upto, 1.0, 0.0).astype(BF16)
            rank = dot_nn(hits, upper)
            pos = jnp.where(kept[:, first:first + width].astype(F32) > 0.0, rank - 1.0, -1.0)
            pos_f_ref[:, first:first + width] = pos[:half]
            pos_b_ref[:, first:first + width] = pos[half:]
            if first + width == tok_rows:
                count_ref[...] = rank[:, width - 128:]

    routes[me] = routes_ref[...]
    for n in (1, 2, 0):
        first_copy(n_chunks, n).start()
    dense(0)
    pass_on(n_chunks)
    send(0)

    def dense_send(c, carry):
        dense(c)
        send(c)
        return carry

    lax.fori_loop(1, n_chunks, dense_send, 0)
    pass_far(n_chunks)
    arrive(n_chunks)

    def forward(c, carry):
        pass_on(c)
        for i in range(n_src // n_chunks):
            tables(c * (n_src // n_chunks) + i)
        dense_saved(c)
        return carry

    lax.fori_loop(0, n_chunks, forward, 0)

    def far(c, carry):
        pass_far(c)
        return carry

    lax.fori_loop(0, n_chunks - 1, far, 0)
    ranks()
    lax.fori_loop(n_chunks - 1, n_chunks, far, 0)

    def finish(c, carry):
        arrive(c)
        own_copy(c).wait()
        pre_copy(c).wait()
        drain(c)
        return carry

    lax.fori_loop(0, n_chunks, finish, 0)
    drain(n_chunks)


def head(x_rows, saved_rows, grad_rows, w_one, w_two, routes, n_src, n_local):
    tok_rows, hidden = x_rows.shape
    ff = w_one.shape[1]
    n_chunks = 4
    dma = pltpu.SemaphoreType.DMA
    vmem = pl.BlockSpec(memory_space=pltpu.VMEM)
    raw = pl.BlockSpec(memory_space=pl.ANY)
    table = jax.ShapeDtypeStruct((n_src * n_local, tok_rows), F32)
    return pl.pallas_call(
        head_kernel,
        out_shape=[
            jax.ShapeDtypeStruct((n_src * tok_rows, hidden), BF16), jax.ShapeDtypeStruct((tok_rows, hidden), BF16),
            jax.ShapeDtypeStruct((tok_rows, hidden), BF16), jax.ShapeDtypeStruct((tok_rows, ff), F32),
            jax.ShapeDtypeStruct((tok_rows, 2 * hidden), BF16),
            table, table, table, table, jax.ShapeDtypeStruct((2 * n_src * n_local, 128), F32),
        ],
        in_specs=[vmem] * 6,
        out_specs=[raw, vmem, vmem, raw] + [vmem] * 6,
        scratch_shapes=[
            pltpu.VMEM((tok_rows, hidden), BF16),
            pltpu.VMEM((tok_rows, ff), F32),
            pltpu.VMEM((n_src,) + routes.shape, BF16),
            pltpu.VMEM((2 * n_src * n_local, tok_rows), BF16),
            dma((n_chunks,)), dma((n_chunks,)),
            dma((n_chunks + 1, 3)), dma((n_chunks + 1, 3)),
            dma((n_chunks + 1, 2)), dma((n_chunks + 1, 2)),
            dma((n_chunks + 1, 4)), dma((n_chunks + 1, 4)),
        ],
        compiler_params=pltpu.CompilerParams(collective_id=1, has_side_effects=True, vmem_limit_bytes=VMEM_BYTES),
        cost_estimate=pl.CostEstimate(flops=30 * 10 ** 9, bytes_accessed=20 * 10 ** 6, transcendentals=0),
        name="head",
    )(x_rows, saved_rows, grad_rows, w_one, w_two, routes)


def solution(mesh):
    stages = mesh.shape["pp"]
    ep_size = mesh.shape["ep"]
    next_perm = [(stage_idx, (stage_idx + 1) % stages) for stage_idx in range(stages)]
    assert (stages, ep_size) == (2, 8)
    tok_spec = P("pp", "ep", None)
    dense_spec = P("pp", None, None)
    expert_spec = P("pp", "ep", None, None)

    def device_step(x_fwd, ids_fwd, slots_fwd, gates_fwd, x_saved, grad_in, ids_bwd, slots_bwd, gates_bwd, w_one, w_two, w_gate, w_up, w_down):
        x_fwd, ids_fwd, slots_fwd, gates_fwd = x_fwd[0], ids_fwd[0], slots_fwd[0], gates_fwd[0]
        x_saved, grad_in, ids_bwd, slots_bwd, gates_bwd = x_saved[0], grad_in[0], ids_bwd[0], slots_bwd[0], gates_bwd[0]
        w_one, w_two, w_gate, w_up, w_down = w_one[0], w_two[0], w_gate[0], w_up[0], w_down[0]
        n_local = w_gate.shape[0]

        routes = jnp.concatenate([
            jnp.where(slots_fwd >= 0, ids_fwd, -1).astype(BF16), gates_fwd,
            jnp.where(slots_bwd >= 0, ids_bwd, -1).astype(BF16), gates_bwd,
        ], axis=1).T
        all_fwd, h_fwd, h_bwd, hidden_pre, pair, pos_f, gate_f, pos_b, gate_b, counts = head(
            x_fwd, x_saved, grad_in, w_one, w_two, routes, ep_size, n_local)
        all_bwd = lax.all_gather(pair, "ep", axis=0, tiled=True)
        pos_f, gate_f, pos_b, gate_b = (t.reshape(ep_size, n_local, -1) for t in (pos_f, gate_f, pos_b, gate_b))
        chunks = (counts[:, -1].reshape(2, ep_size, n_local).astype(jnp.int32) + CHUNK - 1) // CHUNK
        chunks_f, chunks_b = chunks[0], chunks[1]

        (part_fwd,) = expert_call(False, chunks_f, all_fwd, pos_f, gate_f, w_gate, w_up, w_down)
        part_fwd, all_bwd = lax.optimization_barrier((part_fwd, all_bwd))
        mix_sum = lax.psum_scatter(part_fwd, "ep", scatter_dimension=0, tiled=True)
        mix_sum = lax.ppermute(mix_sum, "pp", next_perm)
        h_fwd = lax.ppermute(h_fwd, "pp", next_perm)

        earlier = (jnp.arange(ep_size)[:, None] > jnp.arange(ep_size)[None, :]).astype(jnp.int32)
        base_b = jnp.sum(earlier[:, :, None] * chunks_b[None], axis=1)
        rows_bwd, dw_gate, dw_up, dw_down = expert_call(True, chunks_b, all_bwd, pos_b, gate_b, w_gate, w_up, w_down)
        dx_prev = reduce_tail(base_b, rows_bwd, pos_b, h_bwd, x_saved, grad_in, hidden_pre, w_one, w_two)
        mix_sum, h_fwd, dx_prev = lax.optimization_barrier((mix_sum, h_fwd, dx_prev))
        y_next = (h_fwd.astype(F32) + mix_sum).astype(BF16)
        return y_next[None], dx_prev[None], dw_gate[None], dw_up[None], dw_down[None]

    in_specs = (tok_spec,) * 9 + (dense_spec, dense_spec, expert_spec, expert_spec, expert_spec)
    out_specs = (tok_spec, tok_spec, expert_spec, expert_spec, expert_spec)
    return jax.shard_map(device_step, mesh=mesh, in_specs=in_specs, out_specs=out_specs, check_vma=False)
```
